128 devices in a mesh: px: 8 (over z_hi, y), py: 16 (over x, z_lo, core).
Axes of the slice: x: 4, y: 4, z: 4 (z_hi: 2, z_lo: 2; z = z_hi * 2 + z_lo), core: 2. Of those that a mesh axis runs over, the one named last changes fastest.
Arguments:
- white_noise: float32 [2, 128, 512, 256], P(None, 'px', 'py'), may hold values from -6 to 6
- spectrum: float32 [128, 512, 256], P('px', 'py'), may hold values from 0.1 to 2, as said below
- group_table: int32 [3, 16], replicated, may hold values from 0 to 15, each once within a row
Outputs:
- modulus: float32 [2, 128, 512, 256], P(None, 'px', 'py')
- level_one: float32 [2, 64, 256, 128], P(None, 'px', 'py')
- level_two: float32 [2, 32, 128, 64], P(None, 'px', 'py')
- level_three: float32 [2, 16, 64, 32], P(None, 'px', 'py')
The draws below stay inside these ranges and needn't reach their ends.
Inputs may be any that keep to these rules, and one draw needn't show every extreme that they name: spectrum[j, m, k] equals spectrum[(128 - j) % 128, (512 - m) % 512, (256 - k) % 256]. `group_table`: each row is a permutation of 0 to 15.
All inputs are finite; a program needn't handle non-finite values.
Results may differ from the reference program's by a relative error of at most 0.000088.
Values sent between devices are 32-bit elements; how exact they have to be, the bound alone decides.
No kernel may reach another device: no remote copies, remote signals or barrier semaphores. Data moves between devices by JAX's collectives and lax.ppermute only.
A program may use at most 192 MiB of HBM per device.

```python
import math
import jax
import jax.numpy as jnp

FIELDS = 2
LEVELS = 3
NZ = 256
NX = 128
NY = 512
N_PY = 16


def draw_spectrum(key, part):
    log_low = math.log(0.1)
    log_high = math.log(2.0)
    rough_part = jnp.exp(jax.random.uniform(key, (NX, NY, NZ), jnp.float32, log_low, log_high))
    mirror = jnp.roll(jnp.flip(rough_part, (0, 1, 2)), 1, (0, 1, 2))
    values = 0.5 * (rough_part + mirror)
    return values


def level_of(stream_key, extent, shards, low, top_value):
    def one(axis_at, blocks):
        draws = jax.random.uniform(jax.random.fold_in(jax.random.fold_in(stream_key, 6), axis_at), (blocks,), jnp.float32, low / len(shards), top_value / len(shards))
        return jnp.repeat(jnp.exp(draws), extent[axis_at] // blocks).reshape((-1,) + (1,) * (len(extent) - axis_at - 1))

    level = one(*shards[0])
    for cut in shards[1:]:
        level = level * one(*cut)
    return level


def normal_values(own_key, shape, deviation, most, split=(), dtype=jnp.bfloat16):
    array = jax.random.normal(own_key, shape, jnp.float32) * deviation
    if len(split) > 0:
        array = level_of(own_key, shape, split, -0.22, 0.18) * array
    return jnp.clip(array, min=-most, max=most).astype(dtype)


def setup_inputs(seed: int = 0) -> dict:
    arg_keys = jax.random.split(jax.random.key(seed), 4)
    white_noise = normal_values(arg_keys[0], (FIELDS, NX, NY, NZ), 1.0, 6.0, ((1, 8), (2, 16)), jnp.float32)
    spectrum = draw_spectrum(jax.random.fold_in(arg_keys[3], 71), 0)
    group_table = jax.vmap(lambda own: jax.random.permutation(own, N_PY))(jax.random.split(arg_keys[2], LEVELS)).reshape((LEVELS, N_PY)).astype(jnp.int32)
    return dict(white_noise=white_noise, spectrum=spectrum, group_table=group_table)


def coarsen(values):
    members, size_x, size_y, size_z = values.shape
    blocks = values.reshape(members, size_x // 2, 2, size_y // 2, 2, size_z // 2, 2)
    return blocks.mean(axis=(2, 4, 6))


def route_blocks(coarse, group_order):
    members, size_x, size_y, size_z = coarse.shape
    blocks = coarse.reshape(members, size_x, N_PY, size_y // N_PY, size_z)
    picked = jnp.take(blocks, group_order, axis=2)
    return picked.reshape(members, size_x, size_y, size_z)


def reference(white_noise, spectrum, group_table):
    spectra = jnp.fft.fftn(white_noise, axes=(1, 2, 3))
    scaled = spectra * spectrum[None]
    fields_real = jnp.real(jnp.fft.ifftn(scaled, axes=(1, 2, 3)))
    modulus = jnp.exp(0.5 * fields_real)
    coarse_one = coarsen(modulus)
    coarse_two = coarsen(coarse_one)
    coarse_three = coarsen(coarse_two)
    level_one = route_blocks(coarse_one, group_table[0])
    level_two = route_blocks(coarse_two, group_table[1])
    level_three = route_blocks(coarse_three, group_table[2])
    return modulus, level_one, level_two, level_three
```

```python
import math

import jax
import jax.numpy as jnp
import ml_dtypes
import numpy as np
from jax import lax
from jax.experimental import pallas as pl
from jax.experimental.pallas import tpu as pltpu
from jax.sharding import PartitionSpec as P

NX, NY, NZ = 128, 512, 256
N_PX, N_PY = 8, 16
DEVICES = N_PX * N_PY
SEND_ROWS = 24
BACK_ROWS = 16
ROUTE_ROWS = 24
F32 = jnp.float32
BF16 = jnp.bfloat16


def halves(table):
    high = table.astype(np.float32).astype(ml_dtypes.bfloat16)
    low = (table - high.astype(np.float64)).astype(np.float32).astype(ml_dtypes.bfloat16)
    return high, low


def angle_tables(rows, columns, length):
    angles = 2.0 * math.pi * ((rows[:, None] * columns[None, :]) % length) / length
    return np.cos(angles), np.sin(angles)


def make_tables():
    d, z = np.arange(NZ // 2), np.arange(NZ)
    cos_z, sin_z = angle_tables(d, z, NZ)
    alternating = (1.0 - 2.0 * (z % 2))[None, :]
    into = np.concatenate([cos_z, alternating, -sin_z[1:]], 0)
    weight = np.where(d == 0, 1.0, 2.0)[:, None]
    back = np.concatenate([weight * cos_z, alternating, -2.0 * sin_z[1:]], 0)
    back = back * (0.5 / (NX * NY * NZ))
    y = np.arange(NY)
    cos_y, sin_y = angle_tables(y, y, NY)
    row = np.arange(NX)
    x_of = (row // 8 % 8) * 16 + (row % 8) * 2 + row // 64
    j_of = (row % 8) * 16 + (row // 8 % 4) * 4 + row // 32
    cos_x, sin_x = angle_tables(j_of, x_of, NX)
    x_into = np.block([[cos_x, sin_x], [-sin_x, cos_x]])
    x_back = x_into.T
    return dict(
        into=halves(into),
        back=halves(back),
        cos_y=halves(cos_y),
        sin_y=halves(sin_y),
        x_into=halves(x_into),
        x_back=halves(x_back),
    )


def pair_mean(size):
    rows, columns = np.arange(size), np.arange(128)
    return (0.125 * (rows[:, None] // 2 == columns[None, :])).astype(ml_dtypes.bfloat16)


def split(values):
    high = values.astype(BF16)
    return high, (values - high.astype(F32)).astype(BF16)


def product(a, b, dims=(((1,), (0,)), ((), ()))):
    return lax.dot_general(a, b, dims, preferred_element_type=F32)


def product3(a, b, dims=(((1,), (0,)), ((), ()))):
    return product(a[0], b[0], dims) + product(a[1], b[0], dims) + product(a[0], b[1], dims)


def swapped_parts(part0, part1):
    first = lax.broadcasted_iota(jnp.int32, part0.shape, 1) // 32 % 2 == 0
    new0 = jnp.where(first, part0, pltpu.roll(part1, 32, 1))
    new1 = jnp.where(first, pltpu.roll(part0, 96, 1), part1)
    return new0, new1


def blocks_transposed(parts):
    lane = lax.broadcasted_iota(jnp.int32, parts[0].shape, 1)
    low, even = lane < 64, lane // 32 % 2 == 0
    a, b, c, d = parts
    ac = jnp.where(low, a, pltpu.roll(c, 64, 1)), jnp.where(low, pltpu.roll(a, 64, 1), c)
    bd = jnp.where(low, b, pltpu.roll(d, 64, 1)), jnp.where(low, pltpu.roll(b, 64, 1), d)
    out = []
    for u, v in zip(ac, bd):
        out.append(jnp.where(even, u, pltpu.roll(v, 32, 1)))
        out.append(jnp.where(even, pltpu.roll(u, 96, 1), v))
    return out


def into_kernel(noise, spectrum, t_high, t_low, out):
    table = t_high[...], t_low[...]
    nt = (((1,), (1,)), ((), ()))
    for pair in range(4):
        starts = [f * 512 + (4 * pair + x) * 32 for x in range(4) for f in range(2)]
        block = jnp.concatenate([noise[s : s + 32, :] for s in starts], 0)
        made = product3(table, split(block), nt)
        for at in range(2):
            xh = 2 * pair + at
            part0 = made[:128, at * 128 : at * 128 + 128]
            part1 = made[128:, at * 128 : at * 128 + 128]
            out[pl.ds(xh, DEVICES, stride=SEND_ROWS), :] = part0
            out[pl.ds(8 + xh, DEVICES, stride=SEND_ROWS), :] = part1
            new0, new1 = swapped_parts(part0[:8], part1[:8])
            out[xh : xh + 1, :] = new0[:1]
            out[8 + xh : 9 + xh, :] = new1[:1]
    for q in range(4):
        rows = spectrum[q * 128 : q * 128 + 128, :]
        plane = rows[:, :128].T
        out[pl.ds(16 + q, DEVICES, stride=SEND_ROWS), :] = plane
        out[pl.ds(20 + q, DEVICES, stride=SEND_ROWS), :] = plane
        out[20 + q : 21 + q, :] = rows[:, 128:].T[:1]


def middle_kernel(got, cy_high, cy_low, sy_high, sy_low, xi_high, xi_low, xb_high, xb_low, out, high, low, scale):
    cos_y = cy_high[...], cy_low[...]
    sin_y = sy_high[...], sy_low[...]
    x_into = xi_high[...], xi_low[...]
    x_back = xb_high[...], xb_low[...]
    for q in range(4):
        lanes = slice(q * 128, q * 128 + 128)
        for part in range(2):
            pieces = []
            for i in range(4):
                at = [(px * N_PY + 4 * q + i) * SEND_ROWS + 8 * part for px in range(N_PX)]
                pieces.append(jnp.concatenate([got[s : s + 8, :] for s in at], 0))
            for b, block in enumerate(blocks_transposed(pieces)):
                xl, f = b // 2, b % 2
                row = f * 256 + part * 128 + xl * 64
                h, l = split(block)
                high[row : row + 64, lanes] = h
                low[row : row + 64, lanes] = l
        for f in range(2):
            pieces = []
            for i in range(4):
                at = [(4 * q + i) * SEND_ROWS + 16 + 4 * f + r for r in range(4)]
                step = N_PY * SEND_ROWS
                pieces.append(jnp.concatenate([got[pl.ds(s, N_PX, stride=step), :] for s in at], 0))
            for b, block in enumerate(blocks_transposed(pieces)):
                scale[f * 128 + b * 32 : f * 128 + b * 32 + 32, lanes] = block
    for f in range(2):
        rows = slice(f * 256, f * 256 + 256)
        values = high[rows, :], low[rows, :]
        by_cos = product3(values, cos_y)
        by_sin = product3(values, sin_y)
        along_y = jnp.concatenate([by_cos[:128] + by_sin[128:], by_cos[128:] - by_sin[:128]], 0)
        along_x = product3(x_into, split(along_y))
        s = scale[f * 128 : f * 128 + 128, :]
        scaled = jnp.concatenate([along_x[:128] * s, along_x[128:] * s], 0)
        values = split(product3(x_back, split(scaled)))
        high[rows, :] = values[0]
        low[rows, :] = values[1]
    done = []
    for f in range(2):
        rows = slice(f * 256, f * 256 + 256)
        values = high[rows, :], low[rows, :]
        by_cos = product3(values, cos_y)
        by_sin = product3(values, sin_y)
        done.append((by_cos[:128] - by_sin[128:], by_cos[128:] + by_sin[:128]))
    for q in range(4):
        lanes = slice(q * 128, q * 128 + 128)
        for part in range(2):
            pieces = [done[b % 2][part][(b // 2) * 64 : (b // 2) * 64 + 64, lanes] for b in range(4)]
            for i, block in enumerate(blocks_transposed(pieces)):
                for px in range(N_PX):
                    at = (px * N_PY + 4 * q + i) * BACK_ROWS + 8 * part
                    out[at : at + 8, :] = block[px * 8 : px * 8 + 8]


def last_kernel(got, b_high, b_low, mean1, mean2, mean3, modulus, route, sums, sums2, sums3):
    table = b_high[...], b_low[...]
    first_row = lax.broadcasted_iota(jnp.int32, (128, 128), 0) == 0
    for pair in range(4):
        rows = []
        for at in range(2):
            xh = 2 * pair + at
            part0 = got[pl.ds(xh, DEVICES, stride=BACK_ROWS), :]
            part1 = got[pl.ds(8 + xh, DEVICES, stride=BACK_ROWS), :]
            new0, new1 = swapped_parts(part0, part1)
            part0 = jnp.where(first_row, new0, part0)
            part1 = jnp.where(first_row, new1, part1)
            rows.append(jnp.concatenate([part0.T, part1.T], 1))
        values = jnp.exp(product3(split(jnp.concatenate(rows, 0)), table))
        for at in range(2):
            xh = 2 * pair + at
            for f in range(2):
                first = values[at * 128 + f * 32 : at * 128 + f * 32 + 32]
                second = values[at * 128 + 64 + f * 32 : at * 128 + 64 + f * 32 + 32]
                base = f * 512 + xh * 64
                modulus[base : base + 32, :] = first
                modulus[base + 32 : base + 64, :] = second
                both = first + second
                sums[0, f * 256 + xh * 32 : f * 256 + xh * 32 + 32, :] = both[:, :128]
                sums[1, f * 256 + xh * 32 : f * 256 + xh * 32 + 32, :] = both[:, 128:]
    one = jnp.zeros((256, 128), F32)
    for half in range(2):
        cells = sums[half, pl.ds(0, 256, stride=2), :] + sums[half, pl.ds(1, 256, stride=2), :]
        weights = mean1[half * 128 : half * 128 + 128, :]
        h, l = split(cells)
        one = one + (product(h, weights) + product(l, weights))
    for p in range(N_PY):
        route[p * ROUTE_ROWS : p * ROUTE_ROWS + 16, :] = one[p * 16 : p * 16 + 16]
    for k in range(8):
        sums2[k * 16 : k * 16 + 16, :] = one[k * 32 : k * 32 + 16] + one[k * 32 + 16 : k * 32 + 32]
    h, l = split(sums2[pl.ds(0, 64, stride=2), :] + sums2[pl.ds(1, 64, stride=2), :])
    two = product(h, mean2[...]) + product(l, mean2[...])
    sums2[0:64, :] = two
    for i in range(4):
        route[pl.ds(16 + i, N_PY, stride=ROUTE_ROWS), :] = sums2[pl.ds(i, N_PY, stride=4), :]
    for k in range(4):
        sums3[k * 8 : k * 8 + 8, :] = two[k * 16 : k * 16 + 8] + two[k * 16 + 8 : k * 16 + 16]
    h, l = split(sums3[pl.ds(0, 16, stride=2), :] + sums3[pl.ds(1, 16, stride=2), :])
    route[pl.ds(20, N_PY, stride=ROUTE_ROWS), :] = product(h, mean3[...]) + product(l, mean3[...])
    for i in range(3):
        route[pl.ds(21 + i, N_PY, stride=ROUTE_ROWS), :] = jnp.zeros((N_PY, 128), F32)


def pick_kernel(table, got, out):
    for g in range(N_PY):
        out[g, 0:16, :] = got[table[0, g], 0:16, :]
        out[g, 16:20, :] = got[table[1, g], 16:20, :]
        out[g, 20:24, :] = got[table[2, g], 20:24, :]


def unpack_kernel(got, one, two, three):
    for p in range(N_PY):
        one[p * 16 : p * 16 + 16, :] = got[p, 0:16, :]
        two[p * 4 : p * 4 + 4, :] = got[p, 16:20, 0:64]
        three[p : p + 1, :] = got[p, 20:21, 0:32]


def call(body, name, outs, *operands, scratch=(), **options):
    return pl.pallas_call(
        body,
        out_shape=[jax.ShapeDtypeStruct(s, F32) for s in outs],
        scratch_shapes=list(scratch),
        name=name,
        **options,
    )(*operands)


def on_device(white_noise, spectrum, group_table):
    tables = {k: tuple(jnp.asarray(t) for t in v) for k, v in make_tables().items()}
    noise = white_noise.reshape(1024, NZ)
    (sent,) = call(
        into_kernel,
        "into_z",
        [(DEVICES * SEND_ROWS, 128)],
        noise,
        spectrum.reshape(512, NZ),
        *tables["into"],
    )
    got = lax.all_to_all(sent.reshape(DEVICES, SEND_ROWS, 128), ("px", "py"), 0, 0, tiled=True)
    (restored,) = call(
        middle_kernel,
        "planes",
        [(DEVICES * BACK_ROWS, 128)],
        got.reshape(DEVICES * SEND_ROWS, 128),
        *tables["cos_y"],
        *tables["sin_y"],
        *tables["x_into"],
        *tables["x_back"],
        scratch=(pltpu.VMEM((512, 512), BF16), pltpu.VMEM((512, 512), BF16), pltpu.VMEM((256, 512), F32)),
    )
    back = lax.all_to_all(restored.reshape(DEVICES, BACK_ROWS, 128), ("px", "py"), 0, 0, tiled=True)
    modulus, route = call(
        last_kernel,
        "back_z",
        [(1024, NZ), (N_PY * ROUTE_ROWS, 128)],
        back.reshape(DEVICES * BACK_ROWS, 128),
        *tables["back"],
        jnp.asarray(pair_mean(256)[:, :128]),
        jnp.asarray(pair_mean(128)),
        jnp.asarray(pair_mean(128) * (np.arange(128) < 64)[:, None].astype(ml_dtypes.bfloat16)),
        scratch=(pltpu.VMEM((2, 512, 128), F32), pltpu.VMEM((128, 128), F32), pltpu.VMEM((32, 128), F32)),
    )
    spread = lax.all_to_all(route.reshape(N_PY, ROUTE_ROWS, 128), "py", 0, 0, tiled=True)
    vmem = pl.BlockSpec(memory_space=pltpu.VMEM)
    (picked,) = call(
        pick_kernel,
        "pick",
        [(N_PY, ROUTE_ROWS, 128)],
        group_table,
        spread,
        in_specs=[pl.BlockSpec(memory_space=pltpu.SMEM), vmem],
    )
    levels = lax.all_to_all(picked, "py", 0, 0, tiled=True)
    one, two, three = call(unpack_kernel, "unpack", [(256, 128), (64, 64), (16, 32)], levels)
    return (
        modulus.reshape(2, 16, 32, NZ),
        one.reshape(2, 8, 16, 128),
        two.reshape(2, 4, 8, 64),
        three.reshape(2, 2, 4, 32),
    )


def solution(mesh):
    block = P(None, "px", "py", None)
    return jax.shard_map(
        on_device,
        mesh=mesh,
        in_specs=(block, P("px", "py", None), P()),
        out_specs=(block, block, block, block),
        check_vma=False,
    )
```

```python
import math

import jax
import jax.numpy as jnp
import ml_dtypes
import numpy as np
from jax import lax
from jax.experimental import pallas as pl
from jax.experimental.pallas import tpu as pltpu
from jax.sharding import PartitionSpec as P

NX, NY, NZ = 128, 512, 256
N_PX, N_PY = 8, 16
DEVICES = N_PX * N_PY
SEND_ROWS = 24
BACK_ROWS = 16
ROUTE_ROWS = 24
VMEM_BYTES = 24 << 20
F32 = jnp.float32
BF16 = jnp.bfloat16
NEAR = pl.BlockSpec(memory_space=pltpu.VMEM)
FAR = pl.BlockSpec(memory_space=pltpu.HBM)


def halves(table):
    high = table.astype(np.float32).astype(ml_dtypes.bfloat16)
    low = (table - high.astype(np.float64)).astype(np.float32).astype(ml_dtypes.bfloat16)
    return high, low


def angle_tables(rows, columns, length):
    angles = 2.0 * math.pi * ((rows[:, None] * columns[None, :]) % length) / length
    return np.cos(angles), np.sin(angles)


def make_tables():
    d, z = np.arange(NZ // 2), np.arange(NZ)
    cos_z, sin_z = angle_tables(d, z, NZ)
    alternating = (1.0 - 2.0 * (z % 2))[None, :]
    into = np.concatenate([cos_z, alternating, -sin_z[1:]], 0)
    y = np.arange(NY)
    cos_y, sin_y = angle_tables(y, y, NY)
    row = np.arange(NX)
    x_of = (row // 8 % 8) * 16 + (row % 8) * 2 + row // 64
    j_of = (row % 8) * 16 + (row // 8 % 4) * 4 + row // 32
    cos_x, sin_x = angle_tables(j_of, x_of, NX)
    x_into = np.block([[cos_x, sin_x], [-sin_x, cos_x]])
    x_back = x_into.T
    return dict(
        into=halves(into),
        cos_y=halves(cos_y),
        sin_y=halves(sin_y),
        x_into=halves(x_into),
        x_back=halves(x_back),
    )


def pair_mean(size):
    rows, columns = np.arange(size), np.arange(128)
    return (0.125 * (rows[:, None] // 2 == columns[None, :])).astype(ml_dtypes.bfloat16)


def split(values):
    high = values.astype(BF16)
    return high, (values - high.astype(F32)).astype(BF16)


def product(a, b, dims=(((1,), (0,)), ((), ()))):
    return lax.dot_general(a, b, dims, preferred_element_type=F32)


def product3(a, b, dims=(((1,), (0,)), ((), ()))):
    return product(a[0], b[0], dims) + product(a[1], b[0], dims) + product(a[0], b[1], dims)


def swapped_parts(part0, part1):
    first = lax.broadcasted_iota(jnp.int32, part0.shape, 1) // 32 % 2 == 0
    new0 = jnp.where(first, part0, pltpu.roll(part1, 32, 1))
    new1 = jnp.where(first, pltpu.roll(part0, 96, 1), part1)
    return new0, new1


def blocks_transposed(parts):
    lane = lax.broadcasted_iota(jnp.int32, parts[0].shape, 1)
    low, even = lane < 64, lane // 32 % 2 == 0
    a, b, c, d = parts
    ac = jnp.where(low, a, pltpu.roll(c, 64, 1)), jnp.where(low, pltpu.roll(a, 64, 1), c)
    bd = jnp.where(low, b, pltpu.roll(d, 64, 1)), jnp.where(low, pltpu.roll(b, 64, 1), d)
    out = []
    for u, v in zip(ac, bd):
        out.append(jnp.where(even, u, pltpu.roll(v, 32, 1)))
        out.append(jnp.where(even, pltpu.roll(u, 96, 1), v))
    return out


def into_kernel(noise_far, spectrum_far, high_far, low_far, out, noise, spectrum, t_high, t_low, arrived):
    moves = [(high_far, t_high, 0, 256), (low_far, t_low, 0, 256)]
    moves += [(noise_far, noise, f * 512 + pair * 128, 128) for pair in range(4) for f in range(2)]
    moves += [(spectrum_far, spectrum, q * 128, 128) for q in range(4)]
    copies = []
    for far, near, at, count in moves:
        rows = pl.ds(at, count)
        copies.append(pltpu.make_async_copy(far.at[rows, :], near.at[rows, :], arrived.at[len(copies)]))
        copies[-1].start()
    copies[0].wait()
    copies[1].wait()
    table = t_high[...], t_low[...]
    nt = (((1,), (1,)), ((), ()))
    for pair in range(4):
        copies[2 + 2 * pair].wait()
        copies[3 + 2 * pair].wait()
        starts = [f * 512 + (4 * pair + x) * 32 for x in range(4) for f in range(2)]
        block = jnp.concatenate([noise[s : s + 32, :] for s in starts], 0)
        made = product3(table, split(block), nt)
        for at in range(2):
            xh = 2 * pair + at
            part0 = made[:128, at * 128 : at * 128 + 128]
            part1 = made[128:, at * 128 : at * 128 + 128]
            out[pl.ds(xh, DEVICES, stride=SEND_ROWS), :] = part0
            out[pl.ds(8 + xh, DEVICES, stride=SEND_ROWS), :] = part1
            new0, new1 = swapped_parts(part0[:8], part1[:8])
            out[xh : xh + 1, :] = new0[:1]
            out[8 + xh : 9 + xh, :] = new1[:1]
    for q in range(4):
        copies[10 + q].wait()
        rows = spectrum[q * 128 : q * 128 + 128, :]
        plane = rows[:, :128].T
        out[pl.ds(16 + q, DEVICES, stride=SEND_ROWS), :] = plane
        out[pl.ds(20 + q, DEVICES, stride=SEND_ROWS), :] = plane
        out[20 + q : 21 + q, :] = rows[:, 128:].T[:1]


def middle_kernel(got, cy_high, cy_low, sy_high, sy_low, xi_high, xi_low, xb_high, xb_low, out, high, low, scale):
    cos_y = cy_high[...], cy_low[...]
    sin_y = sy_high[...], sy_low[...]
    x_into = xi_high[...], xi_low[...]
    x_back = xb_high[...], xb_low[...]
    for q in range(4):
        lanes = slice(q * 128, q * 128 + 128)
        for part in range(2):
            pieces = []
            for i in range(4):
                at = [(px * N_PY + 4 * q + i) * SEND_ROWS + 8 * part for px in range(N_PX)]
                pieces.append(jnp.concatenate([got[s : s + 8, :] for s in at], 0))
            for b, block in enumerate(blocks_transposed(pieces)):
                xl, f = b // 2, b % 2
                row = f * 256 + part * 128 + xl * 64
                h, l = split(block)
                high[row : row + 64, lanes] = h
                low[row : row + 64, lanes] = l
        for f in range(2):
            pieces = []
            for i in range(4):
                at = [(4 * q + i) * SEND_ROWS + 16 + 4 * f + r for r in range(4)]
                step = N_PY * SEND_ROWS
                pieces.append(jnp.concatenate([got[pl.ds(s, N_PX, stride=step), :] for s in at], 0))
            for b, block in enumerate(blocks_transposed(pieces)):
                scale[f * 128 + b * 32 : f * 128 + b * 32 + 32, lanes] = block
    for f in range(2):
        rows = slice(f * 256, f * 256 + 256)
        values = high[rows, :], low[rows, :]
        by_cos = product3(values, cos_y)
        by_sin = product3(values, sin_y)
        along_y = jnp.concatenate([by_cos[:128] + by_sin[128:], by_cos[128:] - by_sin[:128]], 0)
        along_x = product3(x_into, split(along_y))
        s = scale[f * 128 : f * 128 + 128, :] * (1.0 / (NX * NY * NZ))
        scaled = jnp.concatenate([along_x[:128] * s, along_x[128:] * s], 0)
        values = split(product3(x_back, split(scaled)))
        high[rows, :] = values[0]
        low[rows, :] = values[1]
    done = []
    for f in range(2):
        rows = slice(f * 256, f * 256 + 256)
        values = high[rows, :], low[rows, :]
        by_cos = product3(values, cos_y)
        by_sin = product3(values, sin_y)
        done.append((by_cos[:128] - by_sin[128:], by_cos[128:] + by_sin[:128]))
    for q in range(4):
        lanes = slice(q * 128, q * 128 + 128)
        for part in range(2):
            pieces = [done[b % 2][part][(b // 2) * 64 : (b // 2) * 64 + 64, lanes] for b in range(4)]
            for i, block in enumerate(blocks_transposed(pieces)):
                for px in range(N_PX):
                    at = (px * N_PY + 4 * q + i) * BACK_ROWS + 8 * part
                    out[at : at + 8, :] = block[px * 8 : px * 8 + 8]


def last_kernel(got, b_high, b_low, mean1, mean2, mean3, modulus_far, route, sums, sums2, sums3, modulus, left):
    copies = []
    table = b_high[...], b_low[...]
    first_row = lax.broadcasted_iota(jnp.int32, (128, 128), 0) == 0
    for pair in range(4):
        rows = []
        for at in range(2):
            xh = 2 * pair + at
            part0 = got[pl.ds(xh, DEVICES, stride=BACK_ROWS), :]
            part1 = got[pl.ds(8 + xh, DEVICES, stride=BACK_ROWS), :]
            new0, new1 = swapped_parts(part0, part1)
            part0 = jnp.where(first_row, 0.5 * new0, part0)
            part1 = jnp.where(first_row, 0.5 * new1, part1)
            rows.append(jnp.concatenate([part0.T, part1.T], 1))
        values = jnp.exp(product3(split(jnp.concatenate(rows, 0)), table))
        for at in range(2):
            xh = 2 * pair + at
            for f in range(2):
                first = values[at * 128 + f * 32 : at * 128 + f * 32 + 32]
                second = values[at * 128 + 64 + f * 32 : at * 128 + 64 + f * 32 + 32]
                base = f * 512 + xh * 64
                modulus[base : base + 32, :] = first
                modulus[base + 32 : base + 64, :] = second
                both = first + second
                sums[0, f * 256 + xh * 32 : f * 256 + xh * 32 + 32, :] = both[:, :128]
                sums[1, f * 256 + xh * 32 : f * 256 + xh * 32 + 32, :] = both[:, 128:]
        for f in range(2):
            rows = pl.ds(f * 512 + pair * 128, 128)
            copies.append(pltpu.make_async_copy(modulus.at[rows, :], modulus_far.at[rows, :], left.at[len(copies)]))
            copies[-1].start()
    one = jnp.zeros((256, 128), F32)
    for half in range(2):
        cells = sums[half, pl.ds(0, 256, stride=2), :] + sums[half, pl.ds(1, 256, stride=2), :]
        weights = mean1[half * 128 : half * 128 + 128, :]
        h, l = split(cells)
        one = one + (product(h, weights) + product(l, weights))
    for p in range(N_PY):
        route[p * ROUTE_ROWS : p * ROUTE_ROWS + 16, :] = one[p * 16 : p * 16 + 16]
    for k in range(8):
        sums2[k * 16 : k * 16 + 16, :] = one[k * 32 : k * 32 + 16] + one[k * 32 + 16 : k * 32 + 32]
    h, l = split(sums2[pl.ds(0, 64, stride=2), :] + sums2[pl.ds(1, 64, stride=2), :])
    two = product(h, mean2[...]) + product(l, mean2[...])
    sums2[0:64, :] = two
    for i in range(4):
        route[pl.ds(16 + i, N_PY, stride=ROUTE_ROWS), :] = sums2[pl.ds(i, N_PY, stride=4), :]
    for k in range(4):
        sums3[k * 8 : k * 8 + 8, :] = two[k * 16 : k * 16 + 8] + two[k * 16 + 8 : k * 16 + 16]
    h, l = split(sums3[pl.ds(0, 16, stride=2), :] + sums3[pl.ds(1, 16, stride=2), :])
    route[pl.ds(20, N_PY, stride=ROUTE_ROWS), :] = product(h, mean3[...]) + product(l, mean3[...])
    for i in range(3):
        route[pl.ds(21 + i, N_PY, stride=ROUTE_ROWS), :] = jnp.zeros((N_PY, 128), F32)
    for copy in copies:
        copy.wait()


def pick_kernel(table, got, out):
    for g in range(N_PY):
        out[g, 0:16, :] = got[table[0, g], 0:16, :]
        out[g, 16:20, :] = got[table[1, g], 16:20, :]
        out[g, 20:24, :] = got[table[2, g], 20:24, :]


def unpack_kernel(got, one, two, three):
    for p in range(N_PY):
        one[p * 16 : p * 16 + 16, :] = got[p, 0:16, :]
        two[p * 4 : p * 4 + 4, :] = got[p, 16:20, 0:64]
        three[p : p + 1, :] = got[p, 20:21, 0:32]


def on_chip(x):
    return pltpu.with_memory_space_constraint(x, pltpu.VMEM)


def off_chip(x):
    return pltpu.with_memory_space_constraint(x, pltpu.HBM)


def call(body, name, outs, *operands, scratch=(), **options):
    return pl.pallas_call(
        body,
        out_shape=outs,
        scratch_shapes=list(scratch),
        name=name,
        compiler_params=pltpu.CompilerParams(vmem_limit_bytes=VMEM_BYTES),
        **options,
    )(*operands)


def on_device(white_noise, spectrum, group_table):
    far = {k: tuple(jnp.asarray(t) for t in v) for k, v in make_tables().items()}
    tables = {k: tuple(on_chip(t) for t in v) for k, v in far.items()}
    noise = white_noise.reshape(1024, NZ)
    (sent,) = call(
        into_kernel,
        "into_z",
        [pltpu.VMEM((DEVICES * SEND_ROWS, 128), F32)],
        *(off_chip(a) for a in (noise, spectrum.reshape(512, NZ), *far["into"])),
        in_specs=[FAR] * 4,
        scratch=(
            pltpu.VMEM((1024, NZ), F32),
            pltpu.VMEM((512, NZ), F32),
            pltpu.VMEM((256, NZ), BF16),
            pltpu.VMEM((256, NZ), BF16),
            pltpu.SemaphoreType.DMA((14,)),
        ),
    )
    got = lax.all_to_all(sent.reshape(DEVICES, SEND_ROWS, 128), ("px", "py"), 0, 0, tiled=True)
    (restored,) = call(
        middle_kernel,
        "planes",
        [pltpu.VMEM((DEVICES * BACK_ROWS, 128), F32)],
        on_chip(got.reshape(DEVICES * SEND_ROWS, 128)),
        *tables["cos_y"],
        *tables["sin_y"],
        *tables["x_into"],
        *tables["x_back"],
        scratch=(pltpu.VMEM((512, 512), BF16), pltpu.VMEM((512, 512), BF16), pltpu.VMEM((256, 512), F32)),
    )
    back = lax.all_to_all(restored.reshape(DEVICES, BACK_ROWS, 128), ("px", "py"), 0, 0, tiled=True)
    modulus, route = call(
        last_kernel,
        "back_z",
        [jax.ShapeDtypeStruct((1024, NZ), F32), pltpu.VMEM((N_PY * ROUTE_ROWS, 128), F32)],
        on_chip(back.reshape(DEVICES * BACK_ROWS, 128)),
        *tables["into"],
        jnp.asarray(pair_mean(256)[:, :128]),
        jnp.asarray(pair_mean(128)),
        jnp.asarray(pair_mean(128) * (np.arange(128) < 64)[:, None].astype(ml_dtypes.bfloat16)),
        out_specs=[FAR, NEAR],
        scratch=(
            pltpu.VMEM((2, 512, 128), F32),
            pltpu.VMEM((128, 128), F32),
            pltpu.VMEM((32, 128), F32),
            pltpu.VMEM((1024, NZ), F32),
            pltpu.SemaphoreType.DMA((8,)),
        ),
    )
    spread = lax.all_to_all(route.reshape(N_PY, ROUTE_ROWS, 128), "py", 0, 0, tiled=True)
    (picked,) = call(
        pick_kernel,
        "pick",
        [pltpu.VMEM((N_PY, ROUTE_ROWS, 128), F32)],
        group_table,
        on_chip(spread),
        in_specs=[pl.BlockSpec(memory_space=pltpu.SMEM), NEAR],
    )
    levels = lax.all_to_all(picked, "py", 0, 0, tiled=True)
    one, two, three = call(unpack_kernel, "unpack", [jax.ShapeDtypeStruct(s, F32) for s in ((256, 128), (64, 64), (16, 32))], on_chip(levels))
    return (
        modulus.reshape(2, 16, 32, NZ),
        one.reshape(2, 8, 16, 128),
        two.reshape(2, 4, 8, 64),
        three.reshape(2, 2, 4, 32),
    )


def solution(mesh):
    block = P(None, "px", "py", None)
    return jax.shard_map(
        on_device,
        mesh=mesh,
        in_specs=(block, P("px", "py", None), P()),
        out_specs=(block, block, block, block),
        check_vma=False,
    )
```

```python
import math

import jax
import jax.numpy as jnp
import ml_dtypes
import numpy as np
from jax import lax
from jax.experimental import pallas as pl
from jax.experimental.pallas import tpu as pltpu
from jax.sharding import PartitionSpec as P

NX, NY, NZ = 128, 512, 256
N_PX, N_PY = 8, 16
DEVICES = N_PX * N_PY
SEND_ROWS = 24
BACK_ROWS = 16
ROUTE_ROWS = 24
SCALE_ROWS = 136
VMEM_BYTES = 24 << 20
F32 = jnp.float32
BF16 = jnp.bfloat16
NEAR = pl.BlockSpec(memory_space=pltpu.VMEM)
FAR = pl.BlockSpec(memory_space=pltpu.HBM)


def halves(table):
    high = table.astype(np.float32).astype(ml_dtypes.bfloat16)
    low = (table - high.astype(np.float64)).astype(np.float32).astype(ml_dtypes.bfloat16)
    return high, low


def angle_tables(rows, columns, length):
    angles = 2.0 * math.pi * ((rows[:, None] * columns[None, :]) % length) / length
    return np.cos(angles), np.sin(angles)


def make_tables():
    d, z = np.arange(NZ // 2), np.arange(NZ)
    cos_z, sin_z = angle_tables(d, z, NZ)
    alternating = (1.0 - 2.0 * (z % 2))[None, :]
    into = np.concatenate([cos_z, alternating, -sin_z[1:]], 0)
    y, m = np.arange(NY // 4), np.arange(NY // 4)
    along_y = []
    for r in range(4):
        cos_y, sin_y = angle_tables(y, 4 * m + r, NY)
        along_y.append(np.block([[cos_y, -sin_y], [sin_y, cos_y]]))
    row = np.arange(NX)
    x_of = (row // 16) * 16 + (row % 8) * 2 + row // 8 % 2
    cos_x, sin_x = angle_tables(row, x_of, NX)
    x_into = np.block([[cos_x, sin_x], [-sin_x, cos_x]])
    return dict(
        into=halves(into),
        along_y=halves(np.concatenate(along_y, 0)),
        x_into=(np.concatenate(halves(x_into), 0),),
        x_back=(np.concatenate(halves(x_into.T), 0),),
    )


def pair_mean(size):
    rows, columns = np.arange(size), np.arange(128)
    return (0.125 * (rows[:, None] // 2 == columns[None, :])).astype(ml_dtypes.bfloat16)


def split(values):
    high = values.astype(BF16)
    return high, (values - high.astype(F32)).astype(BF16)


def product(a, b, dims=(((1,), (0,)), ((), ()))):
    return lax.dot_general(a, b, dims, preferred_element_type=F32)


def product3(a, b, dims=(((1,), (0,)), ((), ()))):
    return product(a[0], b[0], dims) + product(a[1], b[0], dims) + product(a[0], b[1], dims)


def swapped_parts(part0, part1):
    first = lax.broadcasted_iota(jnp.int32, part0.shape, 1) // 32 % 2 == 0
    new0 = jnp.where(first, part0, pltpu.roll(part1, 32, 1))
    new1 = jnp.where(first, pltpu.roll(part0, 96, 1), part1)
    return new0, new1


def blocks_transposed(parts):
    parts = list(parts)
    width = 128 // len(parts)
    lane = lax.broadcasted_iota(jnp.int32, parts[0].shape, 1) // width
    step = len(parts) // 2
    while step:
        stays = lane // step % 2 == 0
        for i in range(len(parts)):
            if i // step % 2 == 0:
                a, b = parts[i], parts[i + step]
                parts[i] = jnp.where(stays, a, pltpu.roll(b, step * width, 1))
                parts[i + step] = jnp.where(stays, pltpu.roll(a, 128 - step * width, 1), b)
        step //= 2
    return parts


def quarters(values, sign):
    (ar, ai), (br, bi), (cr, ci), (dr, di) = values
    sr, si, tr, ti = ar + cr, ai + ci, br + dr, bi + di
    ur, ui, vr, vi = ar - cr, ai - ci, sign * (br - dr), sign * (bi - di)
    return [(sr + tr, si + ti), (ur - vi, ui + vr), (sr - tr, si - ti), (ur + vi, ui - vr)]


def left_product(table, values):
    high, low = split(values)
    count = table.shape[0] // 2
    both = product(table, high)
    return both[:count] + both[count:] + product(table[:count], low)


def right_product(values, table_high, table_low, dims):
    count = values.shape[0] // 2
    both = product(values, table_high, dims)
    return both[:count] + both[count:] + product(values[:count], table_low, dims)


def into_kernel(noise_far, spectrum_far, high_far, low_far, out, noise, spectrum, t_high, t_low, arrived):
    moves = [(high_far, t_high, 0, 256), (low_far, t_low, 0, 256)]
    moves += [(noise_far, noise, f * 512 + pair * 128, 128) for pair in range(4) for f in range(2)]
    copies = []
    for far, near, at, count in moves:
        rows = pl.ds(at, count)
        copies.append(pltpu.make_async_copy(far.at[rows, :], near.at[rows, :], arrived.at[len(copies)]))
    for half in range(2):
        columns = spectrum_far.at[:, pl.ds(half * 128, 128)]
        copies.append(pltpu.make_async_copy(columns, spectrum.at[half], arrived.at[len(copies)]))
    for copy in copies:
        copy.start()
    copies[0].wait()
    copies[1].wait()
    table = t_high[...], t_low[...]
    nt = (((1,), (1,)), ((), ()))
    for pair in range(4):
        copies[2 + 2 * pair].wait()
        copies[3 + 2 * pair].wait()
        starts = [f * 512 + (4 * pair + x) * 32 for x in range(4) for f in range(2)]
        block = jnp.concatenate([noise[s : s + 32, :] for s in starts], 0)
        made = product3(table, split(block), nt)
        for at in range(2):
            xh = 2 * pair + at
            part0 = made[:128, at * 128 : at * 128 + 128]
            part1 = made[128:, at * 128 : at * 128 + 128]
            out[pl.ds(xh, DEVICES, stride=SEND_ROWS), :] = part0
            out[pl.ds(8 + xh, DEVICES, stride=SEND_ROWS), :] = part1
            new0, new1 = swapped_parts(part0[:8], part1[:8])
            out[xh : xh + 1, :] = new0[:1]
            out[8 + xh : 9 + xh, :] = new1[:1]
    copies[10].wait()
    copies[11].wait()
    for r in range(4):
        plane = spectrum[0, pl.ds(r, 128, stride=4), :].T
        out[pl.ds(16 + r, DEVICES, stride=SEND_ROWS), :] = plane
        out[pl.ds(20 + r, DEVICES, stride=SEND_ROWS), :] = plane
        out[20 + r : 21 + r, :] = spectrum[1, pl.ds(r, 128, stride=4), :].T[:1]


def middle_kernel(got, y_high, y_low, x_into, x_back, out, left, scale):
    plain, turned = (((1,), (0,)), ((), ())), (((1,), (1,)), ((), ()))
    for px in range(N_PX):
        pieces = [got[(px * N_PY + i) * SEND_ROWS + 16 : (px * N_PY + i) * SEND_ROWS + 24, :] for i in range(N_PY)]
        for j, block in enumerate(blocks_transposed(pieces)):
            scale[pl.ds(px * 16 + j, 8, stride=SCALE_ROWS), :] = block
    for px in range(N_PX):
        blocks = []
        for q in range(4):
            at = [(px * N_PY + 4 * q + i) * SEND_ROWS for i in range(4)]
            parts = [blocks_transposed([got[s + 8 * part : s + 8 * part + 8, :] for s in at]) for part in range(2)]
            blocks.append(parts)
        for f in range(2):
            pair = []
            for xl in range(2):
                b = 2 * xl + f
                pair.append(quarters([(blocks[q][0][b], blocks[q][1][b]) for q in range(4)], -1.0))
            row = f * 128 + px * 16
            for r in range(4):
                for part in range(2):
                    high, low = split(jnp.concatenate([pair[0][r][part], pair[1][r][part]], 0))
                    left[r, row : row + 16, part * 128 : part * 128 + 128] = high
                    left[r, 256 + row : 272 + row, part * 128 : part * 128 + 128] = low
    along_y = []
    for r in range(4):
        rows = slice(r * 256, r * 256 + 256)
        along_y.append(right_product(left[r], y_high[rows, :], y_low[rows, :], plain))
    restored = []
    for f in range(2):
        rows = slice(f * 128, f * 128 + 128)
        sides = [jnp.concatenate([a[rows, part * 128 : part * 128 + 128] for a in along_y], 1) for part in range(2)]
        spectral = left_product(x_into[...], jnp.concatenate(sides, 0))
        at = [(f * 4 + r) * SCALE_ROWS for r in range(4)]
        s = jnp.concatenate([scale[k : k + 128, :] for k in at], 1) * (1.0 / (NX * NY * NZ))
        scaled = jnp.concatenate([spectral[:128] * s, spectral[128:] * s], 0)
        restored.append(left_product(x_back[...], scaled))
    back = []
    for r in range(4):
        lanes = slice(r * 128, r * 128 + 128)
        rows = [jnp.concatenate([z[:128, lanes], z[128:, lanes]], 1) for z in restored]
        values = jnp.concatenate(split(jnp.concatenate(rows, 0)), 0)
        at = slice(r * 256, r * 256 + 256)
        back.append(right_product(values, y_high[at, :], y_low[at, :], turned))
    for px in range(N_PX):
        blocks = []
        for b in range(4):
            row = (b % 2) * 128 + px * 16 + (b // 2) * 8
            blocks.append(quarters([(u[row : row + 8, :128], u[row : row + 8, 128:]) for u in back], 1.0))
        for q in range(4):
            for part in range(2):
                for i, block in enumerate(blocks_transposed([blocks[b][q][part] for b in range(4)])):
                    at = (px * N_PY + 4 * q + i) * BACK_ROWS + 8 * part
                    out[at : at + 8, :] = block


def last_kernel(got, b_high, b_low, mean1, mean2, mean3, modulus_far, route, sums, sums2, sums3, modulus, left):
    copies = []
    table = b_high[...], b_low[...]
    first_row = lax.broadcasted_iota(jnp.int32, (128, 128), 0) == 0
    for pair in range(4):
        rows = []
        for at in range(2):
            xh = 2 * pair + at
            part0 = got[pl.ds(xh, DEVICES, stride=BACK_ROWS), :]
            part1 = got[pl.ds(8 + xh, DEVICES, stride=BACK_ROWS), :]
            new0, new1 = swapped_parts(part0, part1)
            part0 = jnp.where(first_row, 0.5 * new0, part0)
            part1 = jnp.where(first_row, 0.5 * new1, part1)
            rows.append(jnp.concatenate([part0.T, part1.T], 1))
        values = jnp.exp(product3(split(jnp.concatenate(rows, 0)), table))
        for at in range(2):
            xh = 2 * pair + at
            for f in range(2):
                first = values[at * 128 + f * 32 : at * 128 + f * 32 + 32]
                second = values[at * 128 + 64 + f * 32 : at * 128 + 64 + f * 32 + 32]
                base = f * 512 + xh * 64
                modulus[base : base + 32, :] = first
                modulus[base + 32 : base + 64, :] = second
                both = first + second
                sums[0, f * 256 + xh * 32 : f * 256 + xh * 32 + 32, :] = both[:, :128]
                sums[1, f * 256 + xh * 32 : f * 256 + xh * 32 + 32, :] = both[:, 128:]
        for f in range(2):
            rows = pl.ds(f * 512 + pair * 128, 128)
            copies.append(pltpu.make_async_copy(modulus.at[rows, :], modulus_far.at[rows, :], left.at[len(copies)]))
            copies[-1].start()
    one = jnp.zeros((256, 128), F32)
    for half in range(2):
        cells = sums[half, pl.ds(0, 256, stride=2), :] + sums[half, pl.ds(1, 256, stride=2), :]
        weights = mean1[half * 128 : half * 128 + 128, :]
        h, l = split(cells)
        one = one + (product(h, weights) + product(l, weights))
    for p in range(N_PY):
        route[p * ROUTE_ROWS : p * ROUTE_ROWS + 16, :] = one[p * 16 : p * 16 + 16]
    for k in range(8):
        sums2[k * 16 : k * 16 + 16, :] = one[k * 32 : k * 32 + 16] + one[k * 32 + 16 : k * 32 + 32]
    h, l = split(sums2[pl.ds(0, 64, stride=2), :] + sums2[pl.ds(1, 64, stride=2), :])
    two = product(h, mean2[...]) + product(l, mean2[...])
    sums2[0:64, :] = two
    for i in range(4):
        route[pl.ds(16 + i, N_PY, stride=ROUTE_ROWS), :] = sums2[pl.ds(i, N_PY, stride=4), :]
    for k in range(4):
        sums3[k * 8 : k * 8 + 8, :] = two[k * 16 : k * 16 + 8] + two[k * 16 + 8 : k * 16 + 16]
    h, l = split(sums3[pl.ds(0, 16, stride=2), :] + sums3[pl.ds(1, 16, stride=2), :])
    route[pl.ds(20, N_PY, stride=ROUTE_ROWS), :] = product(h, mean3[...]) + product(l, mean3[...])
    for i in range(3):
        route[pl.ds(21 + i, N_PY, stride=ROUTE_ROWS), :] = jnp.zeros((N_PY, 128), F32)
    for copy in copies:
        copy.wait()


def pick_kernel(table, got, out):
    for g in range(N_PY):
        out[g, 0:16, :] = got[table[0, g], 0:16, :]
        out[g, 16:20, :] = got[table[1, g], 16:20, :]
        out[g, 20:24, :] = got[table[2, g], 20:24, :]


def unpack_kernel(got, one, two, three):
    for p in range(N_PY):
        one[p * 16 : p * 16 + 16, :] = got[p, 0:16, :]
        two[p * 4 : p * 4 + 4, :] = got[p, 16:20, 0:64]
        three[p : p + 1, :] = got[p, 20:21, 0:32]


def on_chip(x):
    return pltpu.with_memory_space_constraint(x, pltpu.VMEM)


def off_chip(x):
    return pltpu.with_memory_space_constraint(x, pltpu.HBM)


def call(body, name, outs, *operands, scratch=(), **options):
    return pl.pallas_call(
        body,
        out_shape=outs,
        scratch_shapes=list(scratch),
        name=name,
        compiler_params=pltpu.CompilerParams(vmem_limit_bytes=VMEM_BYTES),
        **options,
    )(*operands)


def on_device(white_noise, spectrum, group_table):
    far = {k: tuple(jnp.asarray(t) for t in v) for k, v in make_tables().items()}
    tables = {k: tuple(on_chip(t) for t in v) for k, v in far.items()}
    noise = white_noise.reshape(1024, NZ)
    (sent,) = call(
        into_kernel,
        "into_z",
        [pltpu.VMEM((DEVICES * SEND_ROWS, 128), F32)],
        *(off_chip(a) for a in (noise, spectrum.reshape(512, NZ), *far["into"])),
        in_specs=[FAR] * 4,
        scratch=(
            pltpu.VMEM((1024, NZ), F32),
            pltpu.VMEM((2, 512, 128), F32),
            pltpu.VMEM((256, NZ), BF16),
            pltpu.VMEM((256, NZ), BF16),
            pltpu.SemaphoreType.DMA((12,)),
        ),
    )
    got = lax.all_to_all(sent.reshape(DEVICES, SEND_ROWS, 128), ("px", "py"), 0, 0, tiled=True)
    (restored,) = call(
        middle_kernel,
        "planes",
        [pltpu.VMEM((DEVICES * BACK_ROWS, 128), F32)],
        on_chip(got.reshape(DEVICES * SEND_ROWS, 128)),
        *tables["along_y"],
        *tables["x_into"],
        *tables["x_back"],
        scratch=(pltpu.VMEM((4, 512, 256), BF16), pltpu.VMEM((8 * SCALE_ROWS, 128), F32)),
    )
    back = lax.all_to_all(restored.reshape(DEVICES, BACK_ROWS, 128), ("px", "py"), 0, 0, tiled=True)
    modulus, route = call(
        last_kernel,
        "back_z",
        [jax.ShapeDtypeStruct((1024, NZ), F32), pltpu.VMEM((N_PY * ROUTE_ROWS, 128), F32)],
        on_chip(back.reshape(DEVICES * BACK_ROWS, 128)),
        *tables["into"],
        jnp.asarray(pair_mean(256)[:, :128]),
        jnp.asarray(pair_mean(128)),
        jnp.asarray(pair_mean(128) * (np.arange(128) < 64)[:, None].astype(ml_dtypes.bfloat16)),
        out_specs=[FAR, NEAR],
        scratch=(
            pltpu.VMEM((2, 512, 128), F32),
            pltpu.VMEM((128, 128), F32),
            pltpu.VMEM((32, 128), F32),
            pltpu.VMEM((1024, NZ), F32),
            pltpu.SemaphoreType.DMA((8,)),
        ),
    )
    spread = lax.all_to_all(route.reshape(N_PY, ROUTE_ROWS, 128), "py", 0, 0, tiled=True)
    (picked,) = call(
        pick_kernel,
        "pick",
        [pltpu.VMEM((N_PY, ROUTE_ROWS, 128), F32)],
        group_table,
        on_chip(spread),
        in_specs=[pl.BlockSpec(memory_space=pltpu.SMEM), NEAR],
    )
    levels = lax.all_to_all(picked, "py", 0, 0, tiled=True)
    one, two, three = call(unpack_kernel, "unpack", [jax.ShapeDtypeStruct(s, F32) for s in ((256, 128), (64, 64), (16, 32))], on_chip(levels))
    return (
        modulus.reshape(2, 16, 32, NZ),
        one.reshape(2, 8, 16, 128),
        two.reshape(2, 4, 8, 64),
        three.reshape(2, 2, 4, 32),
    )


def solution(mesh):
    block = P(None, "px", "py", None)
    return jax.shard_map(
        on_device,
        mesh=mesh,
        in_specs=(block, P("px", "py", None), P()),
        out_specs=(block, block, block, block),
        check_vma=False,
    )
```

```python
import math

import jax
import jax.numpy as jnp
import ml_dtypes
import numpy as np
from jax import lax
from jax.experimental import pallas as pl
from jax.experimental.pallas import tpu as pltpu
from jax.sharding import PartitionSpec as P

NX, NY, NZ = 128, 512, 256
N_PX, N_PY = 8, 16
DEVICES = N_PX * N_PY
SEND_ROWS = 21
BACK_ROWS = 16
ROUTE_ROWS = 24
SCALE_ROWS = 136
VMEM_BYTES = 24 << 20
F32 = jnp.float32
BF16 = jnp.bfloat16
NEAR = pl.BlockSpec(memory_space=pltpu.VMEM)
FAR = pl.BlockSpec(memory_space=pltpu.HBM)


def halves(table):
    high = table.astype(np.float32).astype(ml_dtypes.bfloat16)
    low = (table - high.astype(np.float64)).astype(np.float32).astype(ml_dtypes.bfloat16)
    return high, low


def angle_tables(rows, columns, length):
    angles = 2.0 * math.pi * ((rows[:, None] * columns[None, :]) % length) / length
    return np.cos(angles), np.sin(angles)


def make_tables():
    d, z = np.arange(NZ // 2), np.arange(NZ)
    cos_z, sin_z = angle_tables(d, z, NZ)
    alternating = (1.0 - 2.0 * (z % 2))[None, :]
    into = np.concatenate([cos_z, alternating, -sin_z[1:]], 0)
    y, m = np.arange(NY // 4), np.arange(NY // 4)
    along_y = []
    for r in range(4):
        cos_y, sin_y = angle_tables(y, 4 * m + r, NY)
        along_y.append(np.block([[cos_y, -sin_y], [sin_y, cos_y]]))
    row = np.arange(NX)
    x_of = (row // 16) * 16 + (row % 8) * 2 + row // 8 % 2
    cos_x, sin_x = angle_tables(row, x_of, NX)
    x_into = np.block([[cos_x, sin_x], [-sin_x, cos_x]])
    return dict(
        into=halves(into),
        along_y=halves(np.concatenate(along_y, 0)),
        x_into=(np.concatenate(halves(x_into), 0),),
        x_back=(np.concatenate(halves(x_into.T), 0),),
    )


def pair_mean(size):
    rows, columns = np.arange(size), np.arange(128)
    return (0.125 * (rows[:, None] // 2 == columns[None, :])).astype(ml_dtypes.bfloat16)


def split(values):
    high = values.astype(BF16)
    return high, (values - high.astype(F32)).astype(BF16)


def product(a, b, dims=(((1,), (0,)), ((), ()))):
    return lax.dot_general(a, b, dims, preferred_element_type=F32)


def product3(a, b, dims=(((1,), (0,)), ((), ()))):
    return product(a[0], b[0], dims) + product(a[1], b[0], dims) + product(a[0], b[1], dims)


def swapped_parts(part0, part1):
    first = lax.broadcasted_iota(jnp.int32, part0.shape, 1) // 32 % 2 == 0
    new0 = jnp.where(first, part0, pltpu.roll(part1, 32, 1))
    new1 = jnp.where(first, pltpu.roll(part0, 96, 1), part1)
    return new0, new1


def blocks_transposed(parts):
    parts = list(parts)
    width = 128 // len(parts)
    lane = lax.broadcasted_iota(jnp.int32, parts[0].shape, 1) // width
    step = len(parts) // 2
    while step:
        stays = lane // step % 2 == 0
        for i in range(len(parts)):
            if i // step % 2 == 0:
                a, b = parts[i], parts[i + step]
                parts[i] = jnp.where(stays, a, pltpu.roll(b, step * width, 1))
                parts[i + step] = jnp.where(stays, pltpu.roll(a, 128 - step * width, 1), b)
        step //= 2
    return parts


def quarters(values, sign):
    (ar, ai), (br, bi), (cr, ci), (dr, di) = values
    sr, si, tr, ti = ar + cr, ai + ci, br + dr, bi + di
    ur, ui, vr, vi = ar - cr, ai - ci, sign * (br - dr), sign * (bi - di)
    return [(sr + tr, si + ti), (ur - vi, ui + vr), (sr - tr, si - ti), (ur + vi, ui - vr)]


def left_product(table, values):
    high, low = split(values)
    count = table.shape[0] // 2
    both = product(table, high)
    return both[:count] + both[count:] + product(table[:count], low)


def right_product(values, table_high, table_low, dims):
    count = values.shape[0] // 2
    both = product(values, table_high, dims)
    return both[:count] + both[count:] + product(values[:count], table_low, dims)


def into_kernel(noise_far, spectrum_far, high_far, low_far, out, noise, spectrum, t_high, t_low, arrived):
    moves = [(high_far, t_high, 0, 256), (low_far, t_low, 0, 256)]
    moves += [(noise_far, noise, quarter * 256, 256) for quarter in range(4)]
    copies = []
    for far, near, at, count in moves:
        rows = pl.ds(at, count)
        copies.append(pltpu.make_async_copy(far.at[rows, :], near.at[rows, :], arrived.at[len(copies)]))
    for half in range(2):
        columns = spectrum_far.at[:, pl.ds(half * 128, 128)]
        copies.append(pltpu.make_async_copy(columns, spectrum.at[half], arrived.at[len(copies)]))
    for copy in copies:
        copy.start()
    for copy in copies[:6]:
        copy.wait()
    table = t_high[...], t_low[...]
    nt = (((1,), (1,)), ((), ()))
    for pair in range(4):
        starts = [f * 512 + (4 * pair + x) * 32 for x in range(4) for f in range(2)]
        block = jnp.concatenate([noise[s : s + 32, :] for s in starts], 0)
        made = product3(table, split(block), nt)
        for at in range(2):
            xh = 2 * pair + at
            part0 = made[:128, at * 128 : at * 128 + 128]
            part1 = made[128:, at * 128 : at * 128 + 128]
            out[pl.ds(xh, DEVICES, stride=SEND_ROWS), :] = part0
            out[pl.ds(8 + xh, DEVICES, stride=SEND_ROWS), :] = part1
            new0, new1 = swapped_parts(part0[:8], part1[:8])
            out[xh : xh + 1, :] = new0[:1]
            out[8 + xh : 9 + xh, :] = new1[:1]
    for copy in copies[6:]:
        copy.wait()
    lower = lax.axis_index("py") < N_PY // 2
    for r in range(4):
        plane = spectrum[0, pl.ds(r, 128, stride=4), :].T
        other = spectrum[1, pl.ds(r, 128, stride=4), :].T[:1]
        out[pl.ds(16 + r, DEVICES, stride=SEND_ROWS), :] = plane
        out[16 + r : 17 + r, :] = jnp.where(lower, plane[:1], other)
        if r == 0:
            out[pl.ds(20, DEVICES, stride=SEND_ROWS), :] = plane
            out[20:21, :] = jnp.where(lower, other, plane[:1])


def unfold(scale):
    row = lax.broadcasted_iota(jnp.int32, (128, 128), 0)
    lane = lax.broadcasted_iota(jnp.int32, (128, 128), 1)
    around = jnp.where((row + lane) % 128 == 0, 1.0, 0.0).astype(BF16)
    mirrored = jnp.where(row + lane == 127, 1.0, 0.0).astype(BF16)
    column = scale[7 * SCALE_ROWS : 7 * SCALE_ROWS + 128, :]
    for r in range(4):
        own = scale[(3 + r) * SCALE_ROWS : (3 + r) * SCALE_ROWS + 128, :]
        at = (3 + (4 - r) % 4) * SCALE_ROWS
        high, low = split(scale[at : at + 128, :])
        turn = mirrored if r else around
        sides = [product(product(around, part).astype(BF16), turn) for part in (high, low)]
        partner = sides[0] + sides[1]
        zero = jnp.where(lane < 64, own, partner)
        half = jnp.where(lane < 64, partner, own)
        if r == 0:
            zero = jnp.where(lane == 64, column, zero)
            half = jnp.where(lane == 0, column, half)
        scale[(8 + r) * SCALE_ROWS : (8 + r) * SCALE_ROWS + 128, :] = zero
        scale[(12 + r) * SCALE_ROWS : (12 + r) * SCALE_ROWS + 128, :] = half


def middle_kernel(got, y_high, y_low, x_into, x_back, out, left, scale):
    plain, turned = (((1,), (0,)), ((), ())), (((1,), (1,)), ((), ()))
    for px in range(N_PX):
        pieces = [got[pl.ds((px * N_PY + i) * SEND_ROWS + 13, 8), :] for i in range(N_PY)]
        for j, block in enumerate(blocks_transposed(pieces)):
            scale[pl.ds(px * 16 + j, 8, stride=SCALE_ROWS), :] = block
    first = (lax.axis_index("px") == 0) & (lax.axis_index("py") == 0)

    @pl.when(first)
    def _():
        unfold(scale)

    for px in range(N_PX):
        blocks = []
        for q in range(4):
            at = [(px * N_PY + 4 * q + i) * SEND_ROWS for i in range(4)]
            parts = [blocks_transposed([got[pl.ds(s + 8 * part, 8), :] for s in at]) for part in range(2)]
            blocks.append(parts)
        for f in range(2):
            pair = []
            for xl in range(2):
                b = 2 * xl + f
                pair.append(quarters([(blocks[q][0][b], blocks[q][1][b]) for q in range(4)], -1.0))
            row = f * 128 + px * 16
            for r in range(4):
                for part in range(2):
                    high, low = split(jnp.concatenate([pair[0][r][part], pair[1][r][part]], 0))
                    left[r, row : row + 16, part * 128 : part * 128 + 128] = high
                    left[r, 256 + row : 272 + row, part * 128 : part * 128 + 128] = low
    along_y = []
    for r in range(4):
        rows = slice(r * 256, r * 256 + 256)
        along_y.append(right_product(left[r], y_high[rows, :], y_low[rows, :], plain))
    restored = []
    for f in range(2):
        rows = slice(f * 128, f * 128 + 128)
        sides = [jnp.concatenate([a[rows, part * 128 : part * 128 + 128] for a in along_y], 1) for part in range(2)]
        spectral = left_product(x_into[...], jnp.concatenate(sides, 0))
        base = jnp.where(first, 8 + 4 * f, 3)
        at = [pl.multiple_of((base + r) * SCALE_ROWS, 8) for r in range(4)]
        s = jnp.concatenate([scale[pl.ds(k, 128), :] for k in at], 1) * (1.0 / (NX * NY * NZ))
        scaled = jnp.concatenate([spectral[:128] * s, spectral[128:] * s], 0)
        restored.append(left_product(x_back[...], scaled))
    back = []
    for r in range(4):
        lanes = slice(r * 128, r * 128 + 128)
        rows = [jnp.concatenate([z[:128, lanes], z[128:, lanes]], 1) for z in restored]
        values = jnp.concatenate(split(jnp.concatenate(rows, 0)), 0)
        at = slice(r * 256, r * 256 + 256)
        back.append(right_product(values, y_high[at, :], y_low[at, :], turned))
    for px in range(N_PX):
        blocks = []
        for b in range(4):
            row = (b % 2) * 128 + px * 16 + (b // 2) * 8
            blocks.append(quarters([(u[row : row + 8, :128], u[row : row + 8, 128:]) for u in back], 1.0))
        for q in range(4):
            for part in range(2):
                for i, block in enumerate(blocks_transposed([blocks[b][q][part] for b in range(4)])):
                    at = (px * N_PY + 4 * q + i) * BACK_ROWS + 8 * part
                    out[at : at + 8, :] = block


def last_kernel(got, b_high, b_low, mean1, mean2, mean3, modulus_far, route, sums, sums2, sums3, modulus, left):
    copies = []
    table = b_high[...], b_low[...]
    first_row = lax.broadcasted_iota(jnp.int32, (128, 128), 0) == 0
    for pair in range(4):
        rows = []
        for at in range(2):
            xh = 2 * pair + at
            part0 = got[pl.ds(xh, DEVICES, stride=BACK_ROWS), :]
            part1 = got[pl.ds(8 + xh, DEVICES, stride=BACK_ROWS), :]
            new0, new1 = swapped_parts(part0, part1)
            part0 = jnp.where(first_row, 0.5 * new0, part0)
            part1 = jnp.where(first_row, 0.5 * new1, part1)
            rows.append(jnp.concatenate([part0.T, part1.T], 1))
        values = jnp.exp(product3(split(jnp.concatenate(rows, 0)), table))
        for at in range(2):
            xh = 2 * pair + at
            for f in range(2):
                first = values[at * 128 + f * 32 : at * 128 + f * 32 + 32]
                second = values[at * 128 + 64 + f * 32 : at * 128 + 64 + f * 32 + 32]
                base = f * 512 + xh * 64
                modulus[base : base + 32, :] = first
                modulus[base + 32 : base + 64, :] = second
                both = first + second
                sums[0, f * 256 + xh * 32 : f * 256 + xh * 32 + 32, :] = both[:, :128]
                sums[1, f * 256 + xh * 32 : f * 256 + xh * 32 + 32, :] = both[:, 128:]
        for f in range(2):
            rows = pl.ds(f * 512 + pair * 128, 128)
            copies.append(pltpu.make_async_copy(modulus.at[rows, :], modulus_far.at[rows, :], left.at[len(copies)]))
            copies[-1].start()
    one = jnp.zeros((256, 128), F32)
    for half in range(2):
        cells = sums[half, pl.ds(0, 256, stride=2), :] + sums[half, pl.ds(1, 256, stride=2), :]
        weights = mean1[half * 128 : half * 128 + 128, :]
        h, l = split(cells)
        one = one + (product(h, weights) + product(l, weights))
    for p in range(N_PY):
        route[p * ROUTE_ROWS : p * ROUTE_ROWS + 16, :] = one[p * 16 : p * 16 + 16]
    for k in range(8):
        sums2[k * 16 : k * 16 + 16, :] = one[k * 32 : k * 32 + 16] + one[k * 32 + 16 : k * 32 + 32]
    h, l = split(sums2[pl.ds(0, 64, stride=2), :] + sums2[pl.ds(1, 64, stride=2), :])
    two = product(h, mean2[...]) + product(l, mean2[...])
    sums2[0:64, :] = two
    for i in range(4):
        route[pl.ds(16 + i, N_PY, stride=ROUTE_ROWS), :] = sums2[pl.ds(i, N_PY, stride=4), :]
    for k in range(4):
        sums3[k * 8 : k * 8 + 8, :] = two[k * 16 : k * 16 + 8] + two[k * 16 + 8 : k * 16 + 16]
    h, l = split(sums3[pl.ds(0, 16, stride=2), :] + sums3[pl.ds(1, 16, stride=2), :])
    route[pl.ds(20, N_PY, stride=ROUTE_ROWS), :] = product(h, mean3[...]) + product(l, mean3[...])
    for i in range(3):
        route[pl.ds(21 + i, N_PY, stride=ROUTE_ROWS), :] = jnp.zeros((N_PY, 128), F32)
    for copy in copies:
        copy.wait()


def pick_kernel(table, got, out):
    for g in range(N_PY):
        out[g, 0:16, :] = got[table[0, g], 0:16, :]
        out[g, 16:20, :] = got[table[1, g], 16:20, :]
        out[g, 20:24, :] = got[table[2, g], 20:24, :]


def unpack_kernel(got, one, two, three):
    for p in range(N_PY):
        one[p * 16 : p * 16 + 16, :] = got[p, 0:16, :]
        two[p * 4 : p * 4 + 4, :] = got[p, 16:20, 0:64]
        three[p : p + 1, :] = got[p, 20:21, 0:32]


def on_chip(x):
    return pltpu.with_memory_space_constraint(x, pltpu.VMEM)


def off_chip(x):
    return pltpu.with_memory_space_constraint(x, pltpu.HBM)


def call(body, name, outs, *operands, scratch=(), **options):
    return pl.pallas_call(
        body,
        out_shape=outs,
        scratch_shapes=list(scratch),
        name=name,
        compiler_params=pltpu.CompilerParams(vmem_limit_bytes=VMEM_BYTES),
        **options,
    )(*operands)


def on_device(white_noise, spectrum, group_table):
    far = {k: tuple(jnp.asarray(t) for t in v) for k, v in make_tables().items()}
    tables = {k: tuple(on_chip(t) for t in v) for k, v in far.items()}
    noise = white_noise.reshape(1024, NZ)
    (sent,) = call(
        into_kernel,
        "into_z",
        [pltpu.VMEM((DEVICES * SEND_ROWS, 128), F32)],
        *(off_chip(a) for a in (noise, spectrum.reshape(512, NZ), *far["into"])),
        in_specs=[FAR] * 4,
        scratch=(
            pltpu.VMEM((1024, NZ), F32),
            pltpu.VMEM((2, 512, 128), F32),
            pltpu.VMEM((256, NZ), BF16),
            pltpu.VMEM((256, NZ), BF16),
            pltpu.SemaphoreType.DMA((8,)),
        ),
    )
    got = lax.all_to_all(sent.reshape(DEVICES, SEND_ROWS, 1, 128), ("px", "py"), 0, 0, tiled=True)
    (restored,) = call(
        middle_kernel,
        "planes",
        [pltpu.VMEM((DEVICES * BACK_ROWS, 128), F32)],
        on_chip(got.reshape(DEVICES * SEND_ROWS, 128)),
        *tables["along_y"],
        *tables["x_into"],
        *tables["x_back"],
        scratch=(pltpu.VMEM((4, 512, 256), BF16), pltpu.VMEM((16 * SCALE_ROWS, 128), F32)),
    )
    back = lax.all_to_all(restored.reshape(DEVICES, BACK_ROWS, 128), ("px", "py"), 0, 0, tiled=True)
    modulus, route = call(
        last_kernel,
        "back_z",
        [jax.ShapeDtypeStruct((1024, NZ), F32), pltpu.VMEM((N_PY * ROUTE_ROWS, 128), F32)],
        on_chip(back.reshape(DEVICES * BACK_ROWS, 128)),
        *tables["into"],
        jnp.asarray(pair_mean(256)[:, :128]),
        jnp.asarray(pair_mean(128)),
        jnp.asarray(pair_mean(128) * (np.arange(128) < 64)[:, None].astype(ml_dtypes.bfloat16)),
        out_specs=[FAR, NEAR],
        scratch=(
            pltpu.VMEM((2, 512, 128), F32),
            pltpu.VMEM((128, 128), F32),
            pltpu.VMEM((32, 128), F32),
            pltpu.VMEM((1024, NZ), F32),
            pltpu.SemaphoreType.DMA((8,)),
        ),
    )
    spread = lax.all_to_all(route.reshape(N_PY, ROUTE_ROWS, 128), "py", 0, 0, tiled=True)
    (picked,) = call(
        pick_kernel,
        "pick",
        [pltpu.VMEM((N_PY, ROUTE_ROWS, 128), F32)],
        group_table,
        on_chip(spread),
        in_specs=[pl.BlockSpec(memory_space=pltpu.SMEM), NEAR],
    )
    levels = lax.all_to_all(picked, "py", 0, 0, tiled=True)
    one, two, three = call(unpack_kernel, "unpack", [jax.ShapeDtypeStruct(s, F32) for s in ((256, 128), (64, 64), (16, 32))], on_chip(levels))
    return (
        modulus.reshape(2, 16, 32, NZ),
        one.reshape(2, 8, 16, 128),
        two.reshape(2, 4, 8, 64),
        three.reshape(2, 2, 4, 32),
    )


def solution(mesh):
    block = P(None, "px", "py", None)
    return jax.shard_map(
        on_device,
        mesh=mesh,
        in_specs=(block, P("px", "py", None), P()),
        out_specs=(block, block, block, block),
        check_vma=False,
    )
```

```python
import math

import jax
import jax.numpy as jnp
import ml_dtypes
import numpy as np
from jax import lax
from jax.experimental import pallas as pl
from jax.experimental.pallas import tpu as pltpu
from jax.sharding import PartitionSpec as P

NX, NY, NZ = 128, 512, 256
N_PX, N_PY = 8, 16
DEVICES = N_PX * N_PY
SEND_ROWS = 21
BACK_ROWS = 16
ROUTE_ROWS = 24
SCALE_ROWS = 136
VMEM_BYTES = 24 << 20
F32 = jnp.float32
BF16 = jnp.bfloat16
NEAR = pl.BlockSpec(memory_space=pltpu.VMEM)
FAR = pl.BlockSpec(memory_space=pltpu.HBM)


def halves(table):
    high = table.astype(np.float32).astype(ml_dtypes.bfloat16)
    low = (table - high.astype(np.float64)).astype(np.float32).astype(ml_dtypes.bfloat16)
    return high, low


def angle_tables(rows, columns, length):
    angles = 2.0 * math.pi * ((rows[:, None] * columns[None, :]) % length) / length
    return np.cos(angles), np.sin(angles)


def make_tables():
    d, z = np.arange(NZ // 2), np.arange(NZ)
    cos_z, sin_z = angle_tables(d, z, NZ)
    alternating = (1.0 - 2.0 * (z % 2))[None, :]
    into = np.concatenate([cos_z, alternating, -sin_z[1:]], 0)
    y, m = np.arange(NY // 4), np.arange(NY // 4)
    along_y = []
    for r in range(4):
        cos_y, sin_y = angle_tables(y, 4 * m + r, NY)
        along_y.append(np.block([[cos_y, -sin_y], [sin_y, cos_y]]))
    row = np.arange(NX)
    x_of = (row // 16) * 16 + (row % 8) * 2 + row // 8 % 2
    cos_x, sin_x = angle_tables(row, x_of, NX)
    x_into = np.block([[cos_x, sin_x], [-sin_x, cos_x]])
    return dict(
        into=halves(into),
        along_y=halves(np.concatenate(along_y, 0)),
        x_into=(np.concatenate(halves(x_into), 0),),
        x_back=(np.concatenate(halves(x_into.T), 0),),
    )


def pair_mean(size):
    rows, columns = np.arange(size), np.arange(128)
    return (0.125 * (rows[:, None] // 2 == columns[None, :])).astype(ml_dtypes.bfloat16)


def split(values):
    high = values.astype(BF16)
    return high, (values - high.astype(F32)).astype(BF16)


def product(a, b, dims=(((1,), (0,)), ((), ()))):
    return lax.dot_general(a, b, dims, preferred_element_type=F32)


def product3(a, b, dims=(((1,), (0,)), ((), ()))):
    return product(a[0], b[0], dims) + product(a[1], b[0], dims) + product(a[0], b[1], dims)


def swapped_parts(part0, part1):
    first = lax.broadcasted_iota(jnp.int32, part0.shape, 1) // 32 % 2 == 0
    new0 = jnp.where(first, part0, pltpu.roll(part1, 32, 1))
    new1 = jnp.where(first, pltpu.roll(part0, 96, 1), part1)
    return new0, new1


def blocks_transposed(parts):
    parts = list(parts)
    width = 128 // len(parts)
    lane = lax.broadcasted_iota(jnp.int32, parts[0].shape, 1) // width
    step = len(parts) // 2
    while step:
        stays = lane // step % 2 == 0
        for i in range(len(parts)):
            if i // step % 2 == 0:
                a, b = parts[i], parts[i + step]
                parts[i] = jnp.where(stays, a, pltpu.roll(b, step * width, 1))
                parts[i + step] = jnp.where(stays, pltpu.roll(a, 128 - step * width, 1), b)
        step //= 2
    return parts


def quarters(values, sign):
    (ar, ai), (br, bi), (cr, ci), (dr, di) = values
    sr, si, tr, ti = ar + cr, ai + ci, br + dr, bi + di
    ur, ui, vr, vi = ar - cr, ai - ci, sign * (br - dr), sign * (bi - di)
    return [(sr + tr, si + ti), (ur - vi, ui + vr), (sr - tr, si - ti), (ur + vi, ui - vr)]


def left_product(table, values):
    high, low = split(values)
    count = table.shape[0] // 2
    both = product(table, high)
    return both[:count] + both[count:] + product(table[:count], low)


def right_product(values, table_high, table_low, dims):
    count = values.shape[0] // 2
    both = product(values, table_high, dims)
    return both[:count] + both[count:] + product(values[:count], table_low, dims)


def into_kernel(noise_far, spectrum_far, high_far, low_far, out, noise, spectrum, t_high, t_low, arrived):
    moves = [(high_far, t_high, 0, 256), (low_far, t_low, 0, 256)]
    moves += [(noise_far, noise, quarter * 256, 256) for quarter in range(4)]
    copies = []
    for far, near, at, count in moves:
        rows = pl.ds(at, count)
        copies.append(pltpu.make_async_copy(far.at[rows, :], near.at[rows, :], arrived.at[len(copies)]))
    for half in range(2):
        columns = spectrum_far.at[:, pl.ds(half * 128, 128)]
        copies.append(pltpu.make_async_copy(columns, spectrum.at[half], arrived.at[len(copies)]))
    for copy in copies:
        copy.start()
    for copy in copies[:6]:
        copy.wait()
    table = t_high[...], t_low[...]
    nt = (((1,), (1,)), ((), ()))
    for pair in range(4):
        starts = [f * 512 + (4 * pair + x) * 32 for x in range(4) for f in range(2)]
        block = jnp.concatenate([noise[s : s + 32, :] for s in starts], 0)
        made = product3(table, split(block), nt)
        for at in range(2):
            xh = 2 * pair + at
            part0 = made[:128, at * 128 : at * 128 + 128]
            part1 = made[128:, at * 128 : at * 128 + 128]
            out[pl.ds(xh, DEVICES, stride=SEND_ROWS), :] = part0
            out[pl.ds(8 + xh, DEVICES, stride=SEND_ROWS), :] = part1
            new0, new1 = swapped_parts(part0[:8], part1[:8])
            out[xh : xh + 1, :] = new0[:1]
            out[8 + xh : 9 + xh, :] = new1[:1]
    for copy in copies[6:]:
        copy.wait()
    lower = lax.axis_index("py") < N_PY // 2
    for r in range(4):
        plane = spectrum[0, pl.ds(r, 128, stride=4), :].T
        other = spectrum[1, pl.ds(r, 128, stride=4), :].T[:1]
        out[pl.ds(16 + r, DEVICES, stride=SEND_ROWS), :] = plane
        out[16 + r : 17 + r, :] = jnp.where(lower, plane[:1], other)
        if r == 0:
            out[pl.ds(20, DEVICES, stride=SEND_ROWS), :] = plane
            out[20:21, :] = jnp.where(lower, other, plane[:1])


def unfold(scale, first):
    row = lax.broadcasted_iota(jnp.int32, (128, 128), 0)
    lane = lax.broadcasted_iota(jnp.int32, (128, 128), 1)
    around = jnp.where((row + lane) % 128 == 0, 1.0, 0.0).astype(BF16)
    mirrored = jnp.where(row + lane == 127, 1.0, 0.0).astype(BF16)
    column = scale[7 * SCALE_ROWS : 7 * SCALE_ROWS + 128, :]
    for r in range(4):
        own = scale[(3 + r) * SCALE_ROWS : (3 + r) * SCALE_ROWS + 128, :]
        at = (3 + (4 - r) % 4) * SCALE_ROWS
        high, low = split(scale[at : at + 128, :])
        turn = mirrored if r else around
        sides = [product(product(around, part).astype(BF16), turn) for part in (high, low)]
        partner = sides[0] + sides[1]
        zero = jnp.where(lane < 64, own, partner)
        half = jnp.where(lane < 64, partner, own)
        if r == 0:
            zero = jnp.where(lane == 64, column, zero)
            half = jnp.where(lane == 0, column, half)
        scale[(8 + r) * SCALE_ROWS : (8 + r) * SCALE_ROWS + 128, :] = jnp.where(first, zero, own)
        scale[(12 + r) * SCALE_ROWS : (12 + r) * SCALE_ROWS + 128, :] = jnp.where(first, half, own)


def middle_kernel(got, y_high, y_low, x_into, x_back, out, left, scale):
    plain, turned = (((1,), (0,)), ((), ())), (((1,), (1,)), ((), ()))
    for px in range(N_PX):
        blocks = []
        for q in range(4):
            at = [(px * N_PY + 4 * q + i) * SEND_ROWS for i in range(4)]
            parts = [blocks_transposed([got[pl.ds(s + 8 * part, 8), :] for s in at]) for part in range(2)]
            blocks.append(parts)
        for f in range(2):
            pair = []
            for xl in range(2):
                b = 2 * xl + f
                pair.append(quarters([(blocks[q][0][b], blocks[q][1][b]) for q in range(4)], -1.0))
            row = f * 128 + px * 16
            for r in range(4):
                for part in range(2):
                    high, low = split(jnp.concatenate([pair[0][r][part], pair[1][r][part]], 0))
                    left[r, row : row + 16, part * 128 : part * 128 + 128] = high
                    left[r, 256 + row : 272 + row, part * 128 : part * 128 + 128] = low
    along_y = []
    for r in range(4):
        rows = slice(r * 256, r * 256 + 256)
        along_y.append(right_product(left[r], y_high[rows, :], y_low[rows, :], plain))
    for px in range(N_PX):
        pieces = [got[pl.ds((px * N_PY + i) * SEND_ROWS + 13, 8), :] for i in range(N_PY)]
        for j, block in enumerate(blocks_transposed(pieces)):
            scale[pl.ds(px * 16 + j, 8, stride=SCALE_ROWS), :] = block
    unfold(scale, (lax.axis_index("px") == 0) & (lax.axis_index("py") == 0))
    restored = []
    for f in range(2):
        rows = slice(f * 128, f * 128 + 128)
        sides = [jnp.concatenate([a[rows, part * 128 : part * 128 + 128] for a in along_y], 1) for part in range(2)]
        spectral = left_product(x_into[...], jnp.concatenate(sides, 0))
        at = [(8 + f * 4 + r) * SCALE_ROWS for r in range(4)]
        s = jnp.concatenate([scale[k : k + 128, :] for k in at], 1) * (1.0 / (NX * NY * NZ))
        scaled = jnp.concatenate([spectral[:128] * s, spectral[128:] * s], 0)
        restored.append(left_product(x_back[...], scaled))
    back = []
    for r in range(4):
        lanes = slice(r * 128, r * 128 + 128)
        rows = [jnp.concatenate([z[:128, lanes], z[128:, lanes]], 1) for z in restored]
        values = jnp.concatenate(split(jnp.concatenate(rows, 0)), 0)
        at = slice(r * 256, r * 256 + 256)
        back.append(right_product(values, y_high[at, :], y_low[at, :], turned))
    for px in range(N_PX):
        blocks = []
        for b in range(4):
            row = (b % 2) * 128 + px * 16 + (b // 2) * 8
            blocks.append(quarters([(u[row : row + 8, :128], u[row : row + 8, 128:]) for u in back], 1.0))
        for q in range(4):
            for part in range(2):
                for i, block in enumerate(blocks_transposed([blocks[b][q][part] for b in range(4)])):
                    at = (px * N_PY + 4 * q + i) * BACK_ROWS + 8 * part
                    out[at : at + 8, :] = block


def last_kernel(got, b_high, b_low, mean1, mean2, mean3, modulus_far, route, sums, sums2, sums3, modulus, left):
    copies = []
    table = b_high[...], b_low[...]
    first_row = lax.broadcasted_iota(jnp.int32, (128, 128), 0) == 0
    for pair in range(4):
        rows = []
        for at in range(2):
            xh = 2 * pair + at
            part0 = got[pl.ds(xh, DEVICES, stride=BACK_ROWS), :]
            part1 = got[pl.ds(8 + xh, DEVICES, stride=BACK_ROWS), :]
            new0, new1 = swapped_parts(part0, part1)
            part0 = jnp.where(first_row, 0.5 * new0, part0)
            part1 = jnp.where(first_row, 0.5 * new1, part1)
            rows.append(jnp.concatenate([part0.T, part1.T], 1))
        values = jnp.exp(product3(split(jnp.concatenate(rows, 0)), table))
        for at in range(2):
            xh = 2 * pair + at
            for f in range(2):
                first = values[at * 128 + f * 32 : at * 128 + f * 32 + 32]
                second = values[at * 128 + 64 + f * 32 : at * 128 + 64 + f * 32 + 32]
                base = f * 512 + xh * 64
                modulus[base : base + 32, :] = first
                modulus[base + 32 : base + 64, :] = second
                both = first + second
                sums[0, f * 256 + xh * 32 : f * 256 + xh * 32 + 32, :] = both[:, :128]
                sums[1, f * 256 + xh * 32 : f * 256 + xh * 32 + 32, :] = both[:, 128:]
        for f in range(2):
            rows = pl.ds(f * 512 + pair * 128, 128)
            copies.append(pltpu.make_async_copy(modulus.at[rows, :], modulus_far.at[rows, :], left.at[len(copies)]))
            copies[-1].start()
    one = jnp.zeros((256, 128), F32)
    for half in range(2):
        cells = sums[half, pl.ds(0, 256, stride=2), :] + sums[half, pl.ds(1, 256, stride=2), :]
        weights = mean1[half * 128 : half * 128 + 128, :]
        h, l = split(cells)
        one = one + (product(h, weights) + product(l, weights))
    for p in range(N_PY):
        route[p * ROUTE_ROWS : p * ROUTE_ROWS + 16, :] = one[p * 16 : p * 16 + 16]
    for k in range(8):
        sums2[k * 16 : k * 16 + 16, :] = one[k * 32 : k * 32 + 16] + one[k * 32 + 16 : k * 32 + 32]
    h, l = split(sums2[pl.ds(0, 64, stride=2), :] + sums2[pl.ds(1, 64, stride=2), :])
    two = product(h, mean2[...]) + product(l, mean2[...])
    sums2[0:64, :] = two
    for i in range(4):
        route[pl.ds(16 + i, N_PY, stride=ROUTE_ROWS), :] = sums2[pl.ds(i, N_PY, stride=4), :]
    for k in range(4):
        sums3[k * 8 : k * 8 + 8, :] = two[k * 16 : k * 16 + 8] + two[k * 16 + 8 : k * 16 + 16]
    h, l = split(sums3[pl.ds(0, 16, stride=2), :] + sums3[pl.ds(1, 16, stride=2), :])
    route[pl.ds(20, N_PY, stride=ROUTE_ROWS), :] = product(h, mean3[...]) + product(l, mean3[...])
    for i in range(3):
        route[pl.ds(21 + i, N_PY, stride=ROUTE_ROWS), :] = jnp.zeros((N_PY, 128), F32)
    for copy in copies:
        copy.wait()


def pick_kernel(table, got, out):
    for g in range(N_PY):
        out[g, 0:16, :] = got[table[0, g], 0:16, :]
        out[g, 16:20, :] = got[table[1, g], 16:20, :]
        out[g, 20:24, :] = got[table[2, g], 20:24, :]


def unpack_kernel(got, one, two, three):
    for p in range(N_PY):
        one[p * 16 : p * 16 + 16, :] = got[p, 0:16, :]
        two[p * 4 : p * 4 + 4, :] = got[p, 16:20, 0:64]
        three[p : p + 1, :] = got[p, 20:21, 0:32]


def on_chip(x):
    return pltpu.with_memory_space_constraint(x, pltpu.VMEM)


def off_chip(x):
    return pltpu.with_memory_space_constraint(x, pltpu.HBM)


def call(body, name, outs, *operands, scratch=(), **options):
    return pl.pallas_call(
        body,
        out_shape=outs,
        scratch_shapes=list(scratch),
        name=name,
        compiler_params=pltpu.CompilerParams(vmem_limit_bytes=VMEM_BYTES),
        **options,
    )(*operands)


def on_device(white_noise, spectrum, group_table):
    far = {k: tuple(jnp.asarray(t) for t in v) for k, v in make_tables().items()}
    tables = {k: tuple(on_chip(t) for t in v) for k, v in far.items()}
    noise = white_noise.reshape(1024, NZ)
    (sent,) = call(
        into_kernel,
        "into_z",
        [pltpu.VMEM((DEVICES * SEND_ROWS, 128), F32)],
        *(off_chip(a) for a in (noise, spectrum.reshape(512, NZ), *far["into"])),
        in_specs=[FAR] * 4,
        scratch=(
            pltpu.VMEM((1024, NZ), F32),
            pltpu.VMEM((2, 512, 128), F32),
            pltpu.VMEM((256, NZ), BF16),
            pltpu.VMEM((256, NZ), BF16),
            pltpu.SemaphoreType.DMA((8,)),
        ),
    )
    got = lax.all_to_all(sent.reshape(DEVICES, SEND_ROWS, 1, 128), ("px", "py"), 0, 0, tiled=True)
    (restored,) = call(
        middle_kernel,
        "planes",
        [pltpu.VMEM((DEVICES * BACK_ROWS, 128), F32)],
        on_chip(got.reshape(DEVICES * SEND_ROWS, 128)),
        *tables["along_y"],
        *tables["x_into"],
        *tables["x_back"],
        scratch=(pltpu.VMEM((4, 512, 256), BF16), pltpu.VMEM((16 * SCALE_ROWS, 128), F32)),
    )
    back = lax.all_to_all(restored.reshape(DEVICES, BACK_ROWS, 128), ("px", "py"), 0, 0, tiled=True)
    modulus, route = call(
        last_kernel,
        "back_z",
        [jax.ShapeDtypeStruct((1024, NZ), F32), pltpu.VMEM((N_PY * ROUTE_ROWS, 128), F32)],
        on_chip(back.reshape(DEVICES * BACK_ROWS, 128)),
        *tables["into"],
        jnp.asarray(pair_mean(256)[:, :128]),
        jnp.asarray(pair_mean(128)),
        jnp.asarray(pair_mean(128) * (np.arange(128) < 64)[:, None].astype(ml_dtypes.bfloat16)),
        out_specs=[FAR, NEAR],
        scratch=(
            pltpu.VMEM((2, 512, 128), F32),
            pltpu.VMEM((128, 128), F32),
            pltpu.VMEM((32, 128), F32),
            pltpu.VMEM((1024, NZ), F32),
            pltpu.SemaphoreType.DMA((8,)),
        ),
    )
    spread = lax.all_to_all(route.reshape(N_PY, ROUTE_ROWS, 128), "py", 0, 0, tiled=True)
    (picked,) = call(
        pick_kernel,
        "pick",
        [pltpu.VMEM((N_PY, ROUTE_ROWS, 128), F32)],
        group_table,
        on_chip(spread),
        in_specs=[pl.BlockSpec(memory_space=pltpu.SMEM), NEAR],
    )
    levels = lax.all_to_all(picked, "py", 0, 0, tiled=True)
    one, two, three = call(unpack_kernel, "unpack", [jax.ShapeDtypeStruct(s, F32) for s in ((256, 128), (64, 64), (16, 32))], on_chip(levels))
    return (
        modulus.reshape(2, 16, 32, NZ),
        one.reshape(2, 8, 16, 128),
        two.reshape(2, 4, 8, 64),
        three.reshape(2, 2, 4, 32),
    )


def solution(mesh):
    block = P(None, "px", "py", None)
    return jax.shard_map(
        on_device,
        mesh=mesh,
        in_specs=(block, P("px", "py", None), P()),
        out_specs=(block, block, block, block),
        check_vma=False,
    )
```

```python
import math

import jax
import jax.numpy as jnp
import ml_dtypes
import numpy as np
from jax import lax
from jax.experimental import pallas as pl
from jax.experimental.pallas import tpu as pltpu
from jax.sharding import PartitionSpec as P

NX, NY, NZ = 128, 512, 256
N_PX, N_PY = 8, 16
DEVICES = N_PX * N_PY
SEND_ROWS = 21
BACK_ROWS = 16
ROUTE_ROWS = 24
SIDES = 2
SIDE_ROWS = NX // SIDES
VMEM_BYTES = 24 << 20
F32 = jnp.float32
BF16 = jnp.bfloat16
PLANE_SCRATCH = (pltpu.VMEM((SIDES, 4, 4 * SIDE_ROWS, 256), BF16), pltpu.VMEM((1536, 128), F32))
NEAR = pl.BlockSpec(memory_space=pltpu.VMEM)
FAR = pl.BlockSpec(memory_space=pltpu.HBM)


def halves(table):
    high = table.astype(np.float32).astype(ml_dtypes.bfloat16)
    low = (table - high.astype(np.float64)).astype(np.float32).astype(ml_dtypes.bfloat16)
    return high, low


def angle_tables(rows, columns, length):
    angles = 2.0 * math.pi * ((rows[:, None] * columns[None, :]) % length) / length
    return np.cos(angles), np.sin(angles)


def make_tables():
    d, z = np.arange(NZ // 2), np.arange(NZ)
    cos_z, sin_z = angle_tables(d, z, NZ)
    alternating = (1.0 - 2.0 * (z % 2))[None, :]
    into = np.concatenate([cos_z, alternating, -sin_z[1:]], 0)
    y, m = np.arange(NY // 4), np.arange(NY // 4)
    along_y = []
    for r in range(4):
        cos_y, sin_y = angle_tables(y, 4 * m + r, NY)
        along_y.append(np.block([[cos_y, -sin_y], [sin_y, cos_y]]))
    row = np.arange(NX)
    x_of = (row // 16) * 16 + (row % 8) * 2 + row // 8 % 2
    j_of = (row % 8) * 16 + row // 8
    cos_x, sin_x = angle_tables(j_of, x_of, NX)
    x_into = np.block([[cos_x, sin_x], [-sin_x, cos_x]])
    return dict(
        into=halves(into),
        along_y=halves(np.concatenate(along_y, 0)),
        x_into=(np.concatenate(halves(x_into), 0),),
        x_back=(np.concatenate(halves(x_into.T), 0),),
    )


def pair_mean(size):
    rows, columns = np.arange(size), np.arange(128)
    return (0.125 * (rows[:, None] // 2 == columns[None, :])).astype(ml_dtypes.bfloat16)


def split(values):
    high = values.astype(BF16)
    return high, (values - high.astype(F32)).astype(BF16)


def product(a, b, dims=(((1,), (0,)), ((), ()))):
    return lax.dot_general(a, b, dims, preferred_element_type=F32)


def product3(a, b, dims=(((1,), (0,)), ((), ()))):
    return product(a[0], b[0], dims) + product(a[1], b[0], dims) + product(a[0], b[1], dims)


def swapped_parts(part0, part1):
    first = lax.broadcasted_iota(jnp.int32, part0.shape, 1) // 32 % 2 == 0
    new0 = jnp.where(first, part0, pltpu.roll(part1, 32, 1))
    new1 = jnp.where(first, pltpu.roll(part0, 96, 1), part1)
    return new0, new1


def blocks_transposed(parts):
    parts = list(parts)
    width = 128 // len(parts)
    lane = lax.broadcasted_iota(jnp.int32, parts[0].shape, 1) // width
    step = len(parts) // 2
    while step:
        stays = lane // step % 2 == 0
        for i in range(len(parts)):
            if i // step % 2 == 0:
                a, b = parts[i], parts[i + step]
                parts[i] = jnp.where(stays, a, pltpu.roll(b, step * width, 1))
                parts[i + step] = jnp.where(stays, pltpu.roll(a, 128 - step * width, 1), b)
        step //= 2
    return parts


def quarters(values, sign):
    (ar, ai), (br, bi), (cr, ci), (dr, di) = values
    sr, si, tr, ti = ar + cr, ai + ci, br + dr, bi + di
    ur, ui, vr, vi = ar - cr, ai - ci, sign * (br - dr), sign * (bi - di)
    return [(sr + tr, si + ti), (ur - vi, ui + vr), (sr - tr, si - ti), (ur + vi, ui - vr)]


def left_product(table, values):
    high, low = split(values)
    count = table.shape[0] // 2
    both = product(table, high)
    return both[:count] + both[count:] + product(table[:count], low)


def right_product(values, table_high, table_low, dims):
    count = values.shape[0] // 2
    both = product(values, table_high, dims)
    return both[:count] + both[count:] + product(values[:count], table_low, dims)


def into_kernel(noise_far, spectrum_far, high_far, low_far, out, noise, spectrum, t_high, t_low, arrived):
    moves = [(high_far, t_high, 0, 256), (low_far, t_low, 0, 256)]
    moves += [(noise_far, noise, quarter * 256, 256) for quarter in range(4)]
    copies = []
    for far, near, at, count in moves:
        rows = pl.ds(at, count)
        copies.append(pltpu.make_async_copy(far.at[rows, :], near.at[rows, :], arrived.at[len(copies)]))
    for half in range(2):
        columns = spectrum_far.at[:, pl.ds(half * 128, 128)]
        copies.append(pltpu.make_async_copy(columns, spectrum.at[half], arrived.at[len(copies)]))
    for copy in copies:
        copy.start()
    for copy in copies[:6]:
        copy.wait()
    table = t_high[...], t_low[...]
    nt = (((1,), (1,)), ((), ()))
    for pair in range(4):
        starts = [f * 512 + (4 * pair + x) * 32 for x in range(4) for f in range(2)]
        block = jnp.concatenate([noise[s : s + 32, :] for s in starts], 0)
        made = product3(table, split(block), nt)
        for at in range(2):
            xh = 2 * pair + at
            part0 = made[:128, at * 128 : at * 128 + 128]
            part1 = made[128:, at * 128 : at * 128 + 128]
            out[pl.ds(xh, DEVICES, stride=SEND_ROWS), :] = part0
            out[pl.ds(8 + xh, DEVICES, stride=SEND_ROWS), :] = part1
            new0, new1 = swapped_parts(part0[:8], part1[:8])
            out[xh : xh + 1, :] = new0[:1]
            out[8 + xh : 9 + xh, :] = new1[:1]
    for copy in copies[6:]:
        copy.wait()
    lower = lax.axis_index("py") < N_PY // 2
    for r in range(4):
        plane = spectrum[0, pl.ds(r, 128, stride=4), :].T
        other = spectrum[1, pl.ds(r, 128, stride=4), :].T[:1]
        out[pl.ds(16 + r, DEVICES, stride=SEND_ROWS), :] = plane
        out[16 + r : 17 + r, :] = jnp.where(lower, plane[:1], other)
        if r == 0:
            out[pl.ds(20, DEVICES, stride=SEND_ROWS), :] = plane
            out[20:21, :] = jnp.where(lower, other, plane[:1])


def unfold(got, scale, first):
    row = lax.broadcasted_iota(jnp.int32, (128, 128), 0)
    lane = lax.broadcasted_iota(jnp.int32, (128, 128), 1)
    j_sum = row % 8 * 16 + row // 8 + lane % 8 * 16 + lane // 8
    rows_turned = jnp.where(j_sum % 128 == 0, 1.0, 0.0).astype(BF16)
    around = jnp.where((row + lane) % 128 == 0, 1.0, 0.0).astype(BF16)
    mirrored = jnp.where(row + lane == 127, 1.0, 0.0).astype(BF16)
    columns = []
    for py in (8, 0):
        v = got[pl.ds(py * SEND_ROWS + 20, N_PX, stride=N_PY * SEND_ROWS), :]
        columns.append(jnp.concatenate([jnp.broadcast_to(v[:, 8 * j : 8 * j + 1], (8, 128)) for j in range(16)], 0))
    for r in range(4):
        own = scale[r * 128 : r * 128 + 128, :]
        at = (4 - r) % 4 * 128
        high, low = split(scale[at : at + 128, :])
        turn = mirrored if r else around
        sides = [product(product(rows_turned, part).astype(BF16), turn) for part in (high, low)]
        partner = sides[0] + sides[1]
        zero = jnp.where(lane < 64, own, partner)
        half = jnp.where(lane < 64, partner, own)
        if r == 0:
            zero = jnp.where(lane == 64, columns[0], zero)
            half = jnp.where(lane == 0, columns[1], half)
        scale[512 + r * 128 : 640 + r * 128, :] = jnp.where(first, zero, own)
        scale[1024 + r * 128 : 1152 + r * 128, :] = jnp.where(first, half, own)


def middle_kernel(got, y_high, y_low, x_into, x_back, out, left, scale):
    plain, turned = (((1,), (0,)), ((), ())), (((1,), (1,)), ((), ()))
    along_y = []
    for side in range(SIDES):
        for at_px in range(N_PX // SIDES):
            px = side * (N_PX // SIDES) + at_px
            blocks = []
            for q in range(4):
                at = [(px * N_PY + 4 * q + i) * SEND_ROWS for i in range(4)]
                parts = [blocks_transposed([got[pl.ds(s + 8 * part, 8), :] for s in at]) for part in range(2)]
                blocks.append(parts)
            for f in range(2):
                pair = []
                for xl in range(2):
                    b = 2 * xl + f
                    pair.append(quarters([(blocks[q][0][b], blocks[q][1][b]) for q in range(4)], -1.0))
                row = f * SIDE_ROWS + at_px * 16
                for r in range(4):
                    for part in range(2):
                        lanes = slice(part * 128, part * 128 + 128)
                        high, low = split(jnp.concatenate([pair[0][r][part], pair[1][r][part]], 0))
                        left[side, r, row : row + 16, lanes] = high
                        left[side, r, 2 * SIDE_ROWS + row : 2 * SIDE_ROWS + row + 16, lanes] = low
        made = []
        for r in range(4):
            rows = slice(r * 256, r * 256 + 256)
            made.append(right_product(left[side, r], y_high[rows, :], y_low[rows, :], plain))
        along_y.append(made)
    spectral = []
    for f in range(2):
        rows = slice(f * SIDE_ROWS, f * SIDE_ROWS + SIDE_ROWS)
        parts = []
        for part in range(2):
            lanes = slice(part * 128, part * 128 + 128)
            for made in along_y:
                parts.append(jnp.concatenate([a[rows, lanes] for a in made], 1))
        spectral.append(left_product(x_into[...], jnp.concatenate(parts, 0)))
    for r in range(4):
        step = N_PY * SEND_ROWS
        pieces = [got[pl.ds(py * SEND_ROWS + 16 + r, N_PX, stride=step), :] for py in range(N_PY)]
        for j, block in enumerate(blocks_transposed(pieces)):
            scale[r * 128 + j * 8 : r * 128 + j * 8 + 8, :] = block
    unfold(got, scale, (lax.axis_index("px") == 0) & (lax.axis_index("py") == 0))
    restored = []
    for f in range(2):
        at = [512 + (f * 4 + r) * 128 for r in range(4)]
        s = jnp.concatenate([scale[k : k + 128, :] for k in at], 1) * (1.0 / (NX * NY * NZ))
        scaled = jnp.concatenate([spectral[f][:128] * s, spectral[f][128:] * s], 0)
        restored.append(left_product(x_back[...], scaled))
    for side in range(SIDES):
        back = []
        for r in range(4):
            lanes = slice(r * 128, r * 128 + 128)
            at, end = side * SIDE_ROWS, side * SIDE_ROWS + SIDE_ROWS
            rows = [jnp.concatenate([z[at:end, lanes], z[128 + at : 128 + end, lanes]], 1) for z in restored]
            values = jnp.concatenate(split(jnp.concatenate(rows, 0)), 0)
            table = slice(r * 256, r * 256 + 256)
            back.append(right_product(values, y_high[table, :], y_low[table, :], turned))
        for at_px in range(N_PX // SIDES):
            px = side * (N_PX // SIDES) + at_px
            blocks = []
            for b in range(4):
                row = (b % 2) * SIDE_ROWS + at_px * 16 + (b // 2) * 8
                blocks.append(quarters([(u[row : row + 8, :128], u[row : row + 8, 128:]) for u in back], 1.0))
            for q in range(4):
                for part in range(2):
                    for i, block in enumerate(blocks_transposed([blocks[b][q][part] for b in range(4)])):
                        at = (px * N_PY + 4 * q + i) * BACK_ROWS + 8 * part
                        out[at : at + 8, :] = block


def last_kernel(got, b_high, b_low, mean1, mean2, mean3, modulus_far, route, sums, sums2, sums3, modulus, left):
    copies = []
    table = b_high[...], b_low[...]
    first_row = lax.broadcasted_iota(jnp.int32, (128, 128), 0) == 0
    for pair in range(4):
        rows = []
        for at in range(2):
            xh = 2 * pair + at
            part0 = got[pl.ds(xh, DEVICES, stride=BACK_ROWS), :]
            part1 = got[pl.ds(8 + xh, DEVICES, stride=BACK_ROWS), :]
            new0, new1 = swapped_parts(part0, part1)
            part0 = jnp.where(first_row, 0.5 * new0, part0)
            part1 = jnp.where(first_row, 0.5 * new1, part1)
            rows.append(jnp.concatenate([part0.T, part1.T], 1))
        values = jnp.exp(product3(split(jnp.concatenate(rows, 0)), table))
        for at in range(2):
            xh = 2 * pair + at
            for f in range(2):
                first = values[at * 128 + f * 32 : at * 128 + f * 32 + 32]
                second = values[at * 128 + 64 + f * 32 : at * 128 + 64 + f * 32 + 32]
                base = f * 512 + xh * 64
                modulus[base : base + 32, :] = first
                modulus[base + 32 : base + 64, :] = second
                both = first + second
                sums[0, f * 256 + xh * 32 : f * 256 + xh * 32 + 32, :] = both[:, :128]
                sums[1, f * 256 + xh * 32 : f * 256 + xh * 32 + 32, :] = both[:, 128:]
        for f in range(2):
            rows = pl.ds(f * 512 + pair * 128, 128)
            copies.append(pltpu.make_async_copy(modulus.at[rows, :], modulus_far.at[rows, :], left.at[len(copies)]))
            copies[-1].start()
    one = jnp.zeros((256, 128), F32)
    for half in range(2):
        cells = sums[half, pl.ds(0, 256, stride=2), :] + sums[half, pl.ds(1, 256, stride=2), :]
        weights = mean1[half * 128 : half * 128 + 128, :]
        h, l = split(cells)
        one = one + (product(h, weights) + product(l, weights))
    for p in range(N_PY):
        route[p * ROUTE_ROWS : p * ROUTE_ROWS + 16, :] = one[p * 16 : p * 16 + 16]
    for k in range(8):
        sums2[k * 16 : k * 16 + 16, :] = one[k * 32 : k * 32 + 16] + one[k * 32 + 16 : k * 32 + 32]
    h, l = split(sums2[pl.ds(0, 64, stride=2), :] + sums2[pl.ds(1, 64, stride=2), :])
    two = product(h, mean2[...]) + product(l, mean2[...])
    sums2[0:64, :] = two
    for i in range(4):
        route[pl.ds(16 + i, N_PY, stride=ROUTE_ROWS), :] = sums2[pl.ds(i, N_PY, stride=4), :]
    for k in range(4):
        sums3[k * 8 : k * 8 + 8, :] = two[k * 16 : k * 16 + 8] + two[k * 16 + 8 : k * 16 + 16]
    h, l = split(sums3[pl.ds(0, 16, stride=2), :] + sums3[pl.ds(1, 16, stride=2), :])
    route[pl.ds(20, N_PY, stride=ROUTE_ROWS), :] = product(h, mean3[...]) + product(l, mean3[...])
    for i in range(3):
        route[pl.ds(21 + i, N_PY, stride=ROUTE_ROWS), :] = jnp.zeros((N_PY, 128), F32)
    for copy in copies:
        copy.wait()


def pick_kernel(table, got, out):
    for g in range(N_PY):
        out[g, 0:16, :] = got[table[0, g], 0:16, :]
        out[g, 16:20, :] = got[table[1, g], 16:20, :]
        out[g, 20:24, :] = got[table[2, g], 20:24, :]


def unpack_kernel(got, one_far, two_far, three_far, two, three, left):
    copies = [pltpu.make_async_copy(got.at[:, pl.ds(0, 16), :], one_far, left.at[0])]
    copies[0].start()
    for p in range(N_PY):
        two[p * 4 : p * 4 + 4, :] = got[p, 16:20, 0:64]
        three[p : p + 1, :] = got[p, 20:21, 0:32]
    copies.append(pltpu.make_async_copy(two, two_far, left.at[1]))
    copies.append(pltpu.make_async_copy(three, three_far, left.at[2]))
    copies[1].start()
    copies[2].start()
    for copy in copies:
        copy.wait()


def on_chip(x):
    return pltpu.with_memory_space_constraint(x, pltpu.VMEM)


def off_chip(x):
    return pltpu.with_memory_space_constraint(x, pltpu.HBM)


def call(body, name, outs, *operands, scratch=(), **options):
    return pl.pallas_call(
        body,
        out_shape=outs,
        scratch_shapes=list(scratch),
        name=name,
        compiler_params=pltpu.CompilerParams(vmem_limit_bytes=VMEM_BYTES),
        **options,
    )(*operands)


def on_device(white_noise, spectrum, group_table):
    far = {k: tuple(jnp.asarray(t) for t in v) for k, v in make_tables().items()}
    tables = {k: tuple(on_chip(t) for t in v) for k, v in far.items()}
    noise = white_noise.reshape(1024, NZ)
    (sent,) = call(
        into_kernel,
        "into_z",
        [pltpu.VMEM((DEVICES * SEND_ROWS, 128), F32)],
        *(off_chip(a) for a in (noise, spectrum.reshape(512, NZ), *far["into"])),
        in_specs=[FAR] * 4,
        scratch=(
            pltpu.VMEM((1024, NZ), F32),
            pltpu.VMEM((2, 512, 128), F32),
            pltpu.VMEM((256, NZ), BF16),
            pltpu.VMEM((256, NZ), BF16),
            pltpu.SemaphoreType.DMA((8,)),
        ),
    )
    got = lax.all_to_all(sent.reshape(DEVICES, SEND_ROWS, 1, 128), ("px", "py"), 0, 0, tiled=True)
    (restored,) = call(
        middle_kernel,
        "planes",
        [pltpu.VMEM((DEVICES * BACK_ROWS, 128), F32)],
        on_chip(got.reshape(DEVICES * SEND_ROWS, 128)),
        *tables["along_y"],
        *tables["x_into"],
        *tables["x_back"],
        scratch=PLANE_SCRATCH,
    )
    back = lax.all_to_all(restored.reshape(DEVICES, BACK_ROWS, 128), ("px", "py"), 0, 0, tiled=True)
    modulus, route = call(
        last_kernel,
        "back_z",
        [jax.ShapeDtypeStruct((1024, NZ), F32), pltpu.VMEM((N_PY * ROUTE_ROWS, 128), F32)],
        on_chip(back.reshape(DEVICES * BACK_ROWS, 128)),
        *tables["into"],
        jnp.asarray(pair_mean(256)[:, :128]),
        jnp.asarray(pair_mean(128)),
        jnp.asarray(pair_mean(128) * (np.arange(128) < 64)[:, None].astype(ml_dtypes.bfloat16)),
        out_specs=[FAR, NEAR],
        scratch=(
            pltpu.VMEM((2, 512, 128), F32),
            pltpu.VMEM((128, 128), F32),
            pltpu.VMEM((32, 128), F32),
            pltpu.VMEM((1024, NZ), F32),
            pltpu.SemaphoreType.DMA((8,)),
        ),
    )
    spread = lax.all_to_all(route.reshape(N_PY, ROUTE_ROWS, 128), "py", 0, 0, tiled=True)
    (picked,) = call(
        pick_kernel,
        "pick",
        [pltpu.VMEM((N_PY, ROUTE_ROWS, 128), F32)],
        group_table,
        on_chip(spread),
        in_specs=[pl.BlockSpec(memory_space=pltpu.SMEM), NEAR],
    )
    levels = lax.all_to_all(picked, "py", 0, 0, tiled=True)
    one, two, three = call(
        unpack_kernel,
        "unpack",
        [jax.ShapeDtypeStruct(s, F32) for s in ((16, 16, 128), (64, 64), (16, 32))],
        on_chip(levels),
        out_specs=[FAR] * 3,
        scratch=(pltpu.VMEM((64, 64), F32), pltpu.VMEM((16, 32), F32), pltpu.SemaphoreType.DMA((3,))),
    )
    return (
        modulus.reshape(2, 16, 32, NZ),
        one.reshape(2, 8, 16, 128),
        two.reshape(2, 4, 8, 64),
        three.reshape(2, 2, 4, 32),
    )


def solution(mesh):
    block = P(None, "px", "py", None)
    return jax.shard_map(
        on_device,
        mesh=mesh,
        in_specs=(block, P("px", "py", None), P()),
        out_specs=(block, block, block, block),
        check_vma=False,
    )
```

```python
import math

import jax
import jax.numpy as jnp
import ml_dtypes
import numpy as np
from jax import lax
from jax.experimental import pallas as pl
from jax.experimental.pallas import tpu as pltpu
from jax.sharding import PartitionSpec as P

NX, NY, NZ = 128, 512, 256
N_PX, N_PY = 8, 16
DEVICES = N_PX * N_PY
SEND_ROWS = 21
BACK_ROWS = 16
ROUTE_ROWS = 24
SIDES = 2
SIDE_ROWS = NX // SIDES
VMEM_BYTES = 24 << 20
F32 = jnp.float32
BF16 = jnp.bfloat16
PLANE_SCRATCH = (pltpu.VMEM((SIDES, 4, 4 * SIDE_ROWS, 256), BF16), pltpu.VMEM((1536, 128), F32))
NEAR = pl.BlockSpec(memory_space=pltpu.VMEM)
FAR = pl.BlockSpec(memory_space=pltpu.HBM)


def halves(table):
    high = table.astype(np.float32).astype(ml_dtypes.bfloat16)
    low = (table - high.astype(np.float64)).astype(np.float32).astype(ml_dtypes.bfloat16)
    return high, low


def angle_tables(rows, columns, length):
    angles = 2.0 * math.pi * ((rows[:, None] * columns[None, :]) % length) / length
    return np.cos(angles), np.sin(angles)


def make_tables():
    d, z = np.arange(NZ // 2), np.arange(NZ)
    cos_z, sin_z = angle_tables(d, z, NZ)
    alternating = (1.0 - 2.0 * (z % 2))[None, :]
    into = np.concatenate([cos_z, alternating, -sin_z[1:]], 0)
    y, m = np.arange(NY // 4), np.arange(NY // 4)
    along_y = []
    for r in range(4):
        cos_y, sin_y = angle_tables(y, 4 * m + r, NY)
        along_y.append(np.block([[cos_y, -sin_y], [sin_y, cos_y]]))
    row = np.arange(NX)
    x_of = (row // 16) * 16 + (row % 8) * 2 + row // 8 % 2
    j_of = (row % 8) * 16 + row // 8
    cos_x, sin_x = angle_tables(j_of, x_of, NX)
    x_into = np.block([[cos_x, sin_x], [-sin_x, cos_x]])
    return dict(
        into=halves(into),
        along_y=halves(np.concatenate(along_y, 0)),
        x_into=(np.concatenate(halves(x_into), 0),),
        x_back=(np.concatenate(halves(x_into.T), 0),),
    )


def pair_mean(size):
    rows, columns = np.arange(size), np.arange(128)
    return (0.125 * (rows[:, None] // 2 == columns[None, :])).astype(ml_dtypes.bfloat16)


def split(values):
    high = values.astype(BF16)
    return high, (values - high.astype(F32)).astype(BF16)


def product(a, b, dims=(((1,), (0,)), ((), ()))):
    return lax.dot_general(a, b, dims, preferred_element_type=F32)


def product3(a, b, dims=(((1,), (0,)), ((), ()))):
    return product(a[0], b[0], dims) + product(a[1], b[0], dims) + product(a[0], b[1], dims)


def places(turn):
    numbers = [(p + 4 - turn) % 4 for p in range(4)]
    return [b % 2 * 512 + b // 2 * 32 for b in numbers]


def swapped_parts(part0, part1, turn):
    first = (lax.broadcasted_iota(jnp.int32, part0.shape, 1) // 32 + turn) % 2 == 0
    new0 = jnp.where(first, part0, pltpu.roll(part1, 32, 1))
    new1 = jnp.where(first, pltpu.roll(part0, 96, 1), part1)
    return new0, new1


def blocks_transposed(parts):
    parts = list(parts)
    width = 128 // len(parts)
    lane = lax.broadcasted_iota(jnp.int32, parts[0].shape, 1) // width
    step = len(parts) // 2
    while step:
        stays = lane // step % 2 == 0
        for i in range(len(parts)):
            if i // step % 2 == 0:
                a, b = parts[i], parts[i + step]
                parts[i] = jnp.where(stays, a, pltpu.roll(b, step * width, 1))
                parts[i + step] = jnp.where(stays, pltpu.roll(a, 128 - step * width, 1), b)
        step //= 2
    return parts


def picked_blocks(parts):
    block = lax.broadcasted_iota(jnp.int32, parts[0].shape, 1) // 32
    picked = []
    for k in range(4):
        value = parts[-k % 4]
        for p in range(1, 4):
            value = jnp.where(block == p, parts[(p - k) % 4], value)
        picked.append(value)
    return picked


def gathered_blocks(parts):
    return [pltpu.roll(v, 128 - 32 * b, 1) if b else v for b, v in enumerate(picked_blocks(parts))]


def scattered_blocks(parts):
    return picked_blocks([pltpu.roll(v, 32 * b, 1) if b else v for b, v in enumerate(parts)])


def quarters(values, sign):
    (ar, ai), (br, bi), (cr, ci), (dr, di) = values
    sr, si, tr, ti = ar + cr, ai + ci, br + dr, bi + di
    ur, ui, vr, vi = ar - cr, ai - ci, sign * (br - dr), sign * (bi - di)
    return [(sr + tr, si + ti), (ur - vi, ui + vr), (sr - tr, si - ti), (ur + vi, ui - vr)]


def left_product(table, values):
    high, low = split(values)
    count = table.shape[0] // 2
    both = product(table, high)
    return both[:count] + both[count:] + product(table[:count], low)


def right_product(values, table_high, table_low, dims):
    count = values.shape[0] // 2
    both = product(values, table_high, dims)
    return both[:count] + both[count:] + product(values[:count], table_low, dims)


def into_kernel(noise_far, spectrum_far, high_far, low_far, out, noise, spectrum, t_high, t_low, arrived):
    moves = [(high_far, t_high, 0, 256), (low_far, t_low, 0, 256)]
    moves += [(noise_far, noise, quarter * 256, 256) for quarter in range(4)]
    copies = []
    for far, near, at, count in moves:
        rows = pl.ds(at, count)
        copies.append(pltpu.make_async_copy(far.at[rows, :], near.at[rows, :], arrived.at[len(copies)]))
    for half in range(2):
        columns = spectrum_far.at[:, pl.ds(half * 128, 128)]
        copies.append(pltpu.make_async_copy(columns, spectrum.at[half], arrived.at[len(copies)]))
    for copy in copies:
        copy.start()
    for copy in copies[:6]:
        copy.wait()
    table = t_high[...], t_low[...]
    nt = (((1,), (1,)), ((), ()))
    turn = lax.axis_index("py") % 4
    for pair in range(4):
        starts = [pl.multiple_of(base + (2 * pair + at) * 64, 32) for at in range(2) for base in places(turn)]
        block = jnp.concatenate([noise[pl.ds(s, 32), :] for s in starts], 0)
        made = product3(table, split(block), nt)
        for at in range(2):
            xh = 2 * pair + at
            part0 = made[:128, at * 128 : at * 128 + 128]
            part1 = made[128:, at * 128 : at * 128 + 128]
            out[pl.ds(xh, DEVICES, stride=SEND_ROWS), :] = part0
            out[pl.ds(8 + xh, DEVICES, stride=SEND_ROWS), :] = part1
            new0, new1 = swapped_parts(part0[:8], part1[:8], turn)
            out[xh : xh + 1, :] = new0[:1]
            out[8 + xh : 9 + xh, :] = new1[:1]
    for copy in copies[6:]:
        copy.wait()
    lower = lax.axis_index("py") < N_PY // 2
    for r in range(4):
        plane = spectrum[0, pl.ds(r, 128, stride=4), :].T
        other = spectrum[1, pl.ds(r, 128, stride=4), :].T[:1]
        out[pl.ds(16 + r, DEVICES, stride=SEND_ROWS), :] = plane
        out[16 + r : 17 + r, :] = jnp.where(lower, plane[:1], other)
        if r == 0:
            out[pl.ds(20, DEVICES, stride=SEND_ROWS), :] = plane
            out[20:21, :] = jnp.where(lower, other, plane[:1])


def unfold(got, scale, first):
    row = lax.broadcasted_iota(jnp.int32, (128, 128), 0)
    lane = lax.broadcasted_iota(jnp.int32, (128, 128), 1)
    j_sum = row % 8 * 16 + row // 8 + lane % 8 * 16 + lane // 8
    rows_turned = jnp.where(j_sum % 128 == 0, 1.0, 0.0).astype(BF16)
    around = jnp.where((row + lane) % 128 == 0, 1.0, 0.0).astype(BF16)
    mirrored = jnp.where(row + lane == 127, 1.0, 0.0).astype(BF16)
    columns = []
    for py in (8, 0):
        v = got[pl.ds(py * SEND_ROWS + 20, N_PX, stride=N_PY * SEND_ROWS), :]
        columns.append(jnp.concatenate([jnp.broadcast_to(v[:, 8 * j : 8 * j + 1], (8, 128)) for j in range(16)], 0))
    for r in range(4):
        own = scale[r * 128 : r * 128 + 128, :]
        at = (4 - r) % 4 * 128
        high, low = split(scale[at : at + 128, :])
        turn = mirrored if r else around
        sides = [product(product(rows_turned, part).astype(BF16), turn) for part in (high, low)]
        partner = sides[0] + sides[1]
        zero = jnp.where(lane < 64, own, partner)
        half = jnp.where(lane < 64, partner, own)
        if r == 0:
            zero = jnp.where(lane == 64, columns[0], zero)
            half = jnp.where(lane == 0, columns[1], half)
        scale[512 + r * 128 : 640 + r * 128, :] = jnp.where(first, zero, own)
        scale[1024 + r * 128 : 1152 + r * 128, :] = jnp.where(first, half, own)


def middle_kernel(got, y_high, y_low, x_into, x_back, out, left, scale):
    plain, turned = (((1,), (0,)), ((), ())), (((1,), (1,)), ((), ()))
    along_y = []
    for side in range(SIDES):
        for at_px in range(N_PX // SIDES):
            px = side * (N_PX // SIDES) + at_px
            blocks = []
            for q in range(4):
                at = [(px * N_PY + 4 * q + i) * SEND_ROWS for i in range(4)]
                parts = [gathered_blocks([got[pl.ds(s + 8 * part, 8), :] for s in at]) for part in range(2)]
                blocks.append(parts)
            for f in range(2):
                pair = []
                for xl in range(2):
                    b = 2 * xl + f
                    pair.append(quarters([(blocks[q][0][b], blocks[q][1][b]) for q in range(4)], -1.0))
                row = f * SIDE_ROWS + at_px * 16
                for r in range(4):
                    for part in range(2):
                        lanes = slice(part * 128, part * 128 + 128)
                        high, low = split(jnp.concatenate([pair[0][r][part], pair[1][r][part]], 0))
                        left[side, r, row : row + 16, lanes] = high
                        left[side, r, 2 * SIDE_ROWS + row : 2 * SIDE_ROWS + row + 16, lanes] = low
        made = []
        for r in range(4):
            rows = slice(r * 256, r * 256 + 256)
            made.append(right_product(left[side, r], y_high[rows, :], y_low[rows, :], plain))
        along_y.append(made)
    spectral = []
    for f in range(2):
        rows = slice(f * SIDE_ROWS, f * SIDE_ROWS + SIDE_ROWS)
        parts = []
        for part in range(2):
            lanes = slice(part * 128, part * 128 + 128)
            for made in along_y:
                parts.append(jnp.concatenate([a[rows, lanes] for a in made], 1))
        spectral.append(left_product(x_into[...], jnp.concatenate(parts, 0)))
    for r in range(4):
        step = N_PY * SEND_ROWS
        pieces = [got[pl.ds(py * SEND_ROWS + 16 + r, N_PX, stride=step), :] for py in range(N_PY)]
        for j, block in enumerate(blocks_transposed(pieces)):
            scale[r * 128 + j * 8 : r * 128 + j * 8 + 8, :] = block
    unfold(got, scale, (lax.axis_index("px") == 0) & (lax.axis_index("py") == 0))
    restored = []
    for f in range(2):
        at = [512 + (f * 4 + r) * 128 for r in range(4)]
        s = jnp.concatenate([scale[k : k + 128, :] for k in at], 1) * (1.0 / (NX * NY * NZ))
        scaled = jnp.concatenate([spectral[f][:128] * s, spectral[f][128:] * s], 0)
        restored.append(left_product(x_back[...], scaled))
    for side in range(SIDES):
        back = []
        for r in range(4):
            lanes = slice(r * 128, r * 128 + 128)
            at, end = side * SIDE_ROWS, side * SIDE_ROWS + SIDE_ROWS
            rows = [jnp.concatenate([z[at:end, lanes], z[128 + at : 128 + end, lanes]], 1) for z in restored]
            values = jnp.concatenate(split(jnp.concatenate(rows, 0)), 0)
            table = slice(r * 256, r * 256 + 256)
            back.append(right_product(values, y_high[table, :], y_low[table, :], turned))
        for at_px in range(N_PX // SIDES):
            px = side * (N_PX // SIDES) + at_px
            blocks = []
            for b in range(4):
                row = (b % 2) * SIDE_ROWS + at_px * 16 + (b // 2) * 8
                blocks.append(quarters([(u[row : row + 8, :128], u[row : row + 8, 128:]) for u in back], 1.0))
            for q in range(4):
                for part in range(2):
                    for i, block in enumerate(scattered_blocks([blocks[b][q][part] for b in range(4)])):
                        at = (px * N_PY + 4 * q + i) * BACK_ROWS + 8 * part
                        out[at : at + 8, :] = block


def last_kernel(got, b_high, b_low, mean1, mean2, mean3, modulus_far, route, sums, sums2, sums3, modulus, left):
    copies = []
    table = b_high[...], b_low[...]
    turn = lax.axis_index("py") % 4
    first_row = lax.broadcasted_iota(jnp.int32, (128, 128), 0) == 0
    for pair in range(4):
        rows = []
        for at in range(2):
            xh = 2 * pair + at
            part0 = got[pl.ds(xh, DEVICES, stride=BACK_ROWS), :]
            part1 = got[pl.ds(8 + xh, DEVICES, stride=BACK_ROWS), :]
            new0, new1 = swapped_parts(part0, part1, turn)
            part0 = jnp.where(first_row, 0.5 * new0, part0)
            part1 = jnp.where(first_row, 0.5 * new1, part1)
            rows.append(jnp.concatenate([part0.T, part1.T], 1))
        values = jnp.exp(product3(split(jnp.concatenate(rows, 0)), table))
        for at in range(2):
            xh = 2 * pair + at
            cells = [values[at * 128 + p * 32 : at * 128 + p * 32 + 32] for p in range(4)]
            for p, base in enumerate(places(turn)):
                modulus[pl.ds(pl.multiple_of(base + xh * 64, 32), 32), :] = cells[p]
            for p in range(2):
                both = cells[p] + cells[p + 2]
                rows = pl.ds(pl.multiple_of((p + turn) % 2 * 256 + xh * 32, 32), 32)
                sums[0, rows, :] = both[:, :128]
                sums[1, rows, :] = both[:, 128:]
        for f in range(2):
            rows = pl.ds(f * 512 + pair * 128, 128)
            copies.append(pltpu.make_async_copy(modulus.at[rows, :], modulus_far.at[rows, :], left.at[len(copies)]))
            copies[-1].start()
    one = jnp.zeros((256, 128), F32)
    for half in range(2):
        cells = sums[half, pl.ds(0, 256, stride=2), :] + sums[half, pl.ds(1, 256, stride=2), :]
        weights = mean1[half * 128 : half * 128 + 128, :]
        h, l = split(cells)
        one = one + (product(h, weights) + product(l, weights))
    for p in range(N_PY):
        route[p * ROUTE_ROWS : p * ROUTE_ROWS + 16, :] = one[p * 16 : p * 16 + 16]
    for k in range(8):
        sums2[k * 16 : k * 16 + 16, :] = one[k * 32 : k * 32 + 16] + one[k * 32 + 16 : k * 32 + 32]
    h, l = split(sums2[pl.ds(0, 64, stride=2), :] + sums2[pl.ds(1, 64, stride=2), :])
    two = product(h, mean2[...]) + product(l, mean2[...])
    sums2[0:64, :] = two
    for i in range(4):
        route[pl.ds(16 + i, N_PY, stride=ROUTE_ROWS), :] = sums2[pl.ds(i, N_PY, stride=4), :]
    for k in range(4):
        sums3[k * 8 : k * 8 + 8, :] = two[k * 16 : k * 16 + 8] + two[k * 16 + 8 : k * 16 + 16]
    h, l = split(sums3[pl.ds(0, 16, stride=2), :] + sums3[pl.ds(1, 16, stride=2), :])
    route[pl.ds(20, N_PY, stride=ROUTE_ROWS), :] = product(h, mean3[...]) + product(l, mean3[...])
    for i in range(3):
        route[pl.ds(21 + i, N_PY, stride=ROUTE_ROWS), :] = jnp.zeros((N_PY, 128), F32)
    for copy in copies:
        copy.wait()


def pick_kernel(table, got, out):
    for g in range(N_PY):
        out[g, 0:16, :] = got[table[0, g], 0:16, :]
        out[g, 16:20, :] = got[table[1, g], 16:20, :]
        out[g, 20:24, :] = got[table[2, g], 20:24, :]


def unpack_kernel(got, one_far, two_far, three_far, two, three, left):
    copies = [pltpu.make_async_copy(got.at[:, pl.ds(0, 16), :], one_far, left.at[0])]
    copies[0].start()
    for p in range(N_PY):
        two[p * 4 : p * 4 + 4, :] = got[p, 16:20, 0:64]
        three[p : p + 1, :] = got[p, 20:21, 0:32]
    copies.append(pltpu.make_async_copy(two, two_far, left.at[1]))
    copies.append(pltpu.make_async_copy(three, three_far, left.at[2]))
    copies[1].start()
    copies[2].start()
    for copy in copies:
        copy.wait()


def on_chip(x):
    return pltpu.with_memory_space_constraint(x, pltpu.VMEM)


def off_chip(x):
    return pltpu.with_memory_space_constraint(x, pltpu.HBM)


def call(body, name, outs, *operands, scratch=(), **options):
    return pl.pallas_call(
        body,
        out_shape=outs,
        scratch_shapes=list(scratch),
        name=name,
        compiler_params=pltpu.CompilerParams(vmem_limit_bytes=VMEM_BYTES),
        **options,
    )(*operands)


def on_device(white_noise, spectrum, group_table):
    far = {k: tuple(jnp.asarray(t) for t in v) for k, v in make_tables().items()}
    tables = {k: tuple(on_chip(t) for t in v) for k, v in far.items()}
    noise = white_noise.reshape(1024, NZ)
    (sent,) = call(
        into_kernel,
        "into_z",
        [pltpu.VMEM((DEVICES * SEND_ROWS, 128), F32)],
        *(off_chip(a) for a in (noise, spectrum.reshape(512, NZ), *far["into"])),
        in_specs=[FAR] * 4,
        scratch=(
            pltpu.VMEM((1024, NZ), F32),
            pltpu.VMEM((2, 512, 128), F32),
            pltpu.VMEM((256, NZ), BF16),
            pltpu.VMEM((256, NZ), BF16),
            pltpu.SemaphoreType.DMA((8,)),
        ),
    )
    got = lax.all_to_all(sent.reshape(DEVICES, SEND_ROWS, 1, 128), ("px", "py"), 0, 0, tiled=True)
    (restored,) = call(
        middle_kernel,
        "planes",
        [pltpu.VMEM((DEVICES * BACK_ROWS, 128), F32)],
        on_chip(got.reshape(DEVICES * SEND_ROWS, 128)),
        *tables["along_y"],
        *tables["x_into"],
        *tables["x_back"],
        scratch=PLANE_SCRATCH,
    )
    back = lax.all_to_all(restored.reshape(DEVICES, BACK_ROWS, 128), ("px", "py"), 0, 0, tiled=True)
    modulus, route = call(
        last_kernel,
        "back_z",
        [jax.ShapeDtypeStruct((1024, NZ), F32), pltpu.VMEM((N_PY * ROUTE_ROWS, 128), F32)],
        on_chip(back.reshape(DEVICES * BACK_ROWS, 128)),
        *tables["into"],
        jnp.asarray(pair_mean(256)[:, :128]),
        jnp.asarray(pair_mean(128)),
        jnp.asarray(pair_mean(128) * (np.arange(128) < 64)[:, None].astype(ml_dtypes.bfloat16)),
        out_specs=[FAR, NEAR],
        scratch=(
            pltpu.VMEM((2, 512, 128), F32),
            pltpu.VMEM((128, 128), F32),
            pltpu.VMEM((32, 128), F32),
            pltpu.VMEM((1024, NZ), F32),
            pltpu.SemaphoreType.DMA((8,)),
        ),
    )
    spread = lax.all_to_all(route.reshape(N_PY, ROUTE_ROWS, 128), "py", 0, 0, tiled=True)
    (picked,) = call(
        pick_kernel,
        "pick",
        [pltpu.VMEM((N_PY, ROUTE_ROWS, 128), F32)],
        group_table,
        on_chip(spread),
        in_specs=[pl.BlockSpec(memory_space=pltpu.SMEM), NEAR],
    )
    levels = lax.all_to_all(picked, "py", 0, 0, tiled=True)
    one, two, three = call(
        unpack_kernel,
        "unpack",
        [jax.ShapeDtypeStruct(s, F32) for s in ((16, 16, 128), (64, 64), (16, 32))],
        on_chip(levels),
        out_specs=[FAR] * 3,
        scratch=(pltpu.VMEM((64, 64), F32), pltpu.VMEM((16, 32), F32), pltpu.SemaphoreType.DMA((3,))),
    )
    return (
        modulus.reshape(2, 16, 32, NZ),
        one.reshape(2, 8, 16, 128),
        two.reshape(2, 4, 8, 64),
        three.reshape(2, 2, 4, 32),
    )


def solution(mesh):
    block = P(None, "px", "py", None)
    return jax.shard_map(
        on_device,
        mesh=mesh,
        in_specs=(block, P("px", "py", None), P()),
        out_specs=(block, block, block, block),
        check_vma=False,
    )
```

```python
import math

import jax
import jax.numpy as jnp
import ml_dtypes
import numpy as np
from jax import lax
from jax.experimental import pallas as pl
from jax.experimental.pallas import tpu as pltpu
from jax.sharding import PartitionSpec as P

NX, NY, NZ = 128, 512, 256
N_PX, N_PY = 8, 16
DEVICES = N_PX * N_PY
SEND_ROWS = 21
BACK_ROWS = 16
ROUTE_ROWS = 20
SIDES = 2
SIDE_ROWS = NX // SIDES
VMEM_BYTES = 24 << 20
ROUTE = (N_PY, ROUTE_ROWS // 4, 4, 128)
F32 = jnp.float32
BF16 = jnp.bfloat16
PLANE_SCRATCH = (pltpu.VMEM((SIDES, 4, 4 * SIDE_ROWS, 256), BF16), pltpu.VMEM((1536, 128), F32))
NEAR = pl.BlockSpec(memory_space=pltpu.VMEM)
FAR = pl.BlockSpec(memory_space=pltpu.HBM)


def halves(table):
    high = table.astype(np.float32).astype(ml_dtypes.bfloat16)
    low = (table - high.astype(np.float64)).astype(np.float32).astype(ml_dtypes.bfloat16)
    return high, low


def angle_tables(rows, columns, length):
    angles = 2.0 * math.pi * ((rows[:, None] * columns[None, :]) % length) / length
    return np.cos(angles), np.sin(angles)


def make_tables():
    d, z = np.arange(NZ // 2), np.arange(NZ)
    cos_z, sin_z = angle_tables(d, z, NZ)
    alternating = (1.0 - 2.0 * (z % 2))[None, :]
    into = np.concatenate([cos_z, alternating, -sin_z[1:]], 0)
    y, m = np.arange(NY // 4), np.arange(NY // 4)
    along_y = []
    for r in range(4):
        cos_y, sin_y = angle_tables(y, 4 * m + r, NY)
        along_y.append(np.block([[cos_y, -sin_y], [sin_y, cos_y]]))
    row = np.arange(NX)
    x_of = (row // 16) * 16 + (row % 8) * 2 + row // 8 % 2
    j_of = (row % 8) * 16 + row // 8
    cos_x, sin_x = angle_tables(j_of, x_of, NX)
    x_into = np.block([[cos_x, sin_x], [-sin_x, cos_x]])
    return dict(
        into=halves(into),
        along_y=halves(np.concatenate(along_y, 0)),
        x_into=(np.concatenate(halves(x_into), 0),),
        x_back=(np.concatenate(halves(x_into.T), 0),),
    )


def pair_mean(size, first=0):
    rows, columns = np.arange(size), np.arange(128) - first
    return (0.125 * (rows[:, None] // 2 == columns[None, :])).astype(ml_dtypes.bfloat16)


def split(values):
    high = values.astype(BF16)
    return high, (values - high.astype(F32)).astype(BF16)


def product(a, b, dims=(((1,), (0,)), ((), ()))):
    return lax.dot_general(a, b, dims, preferred_element_type=F32)


def product3(a, b, dims=(((1,), (0,)), ((), ()))):
    return product(a[0], b[0], dims) + product(a[1], b[0], dims) + product(a[0], b[1], dims)


def places(turn):
    numbers = [(p + 4 - turn) % 4 for p in range(4)]
    return [b % 2 * 512 + b // 2 * 32 for b in numbers]


def swapped_parts(part0, part1, turn):
    first = (lax.broadcasted_iota(jnp.int32, part0.shape, 1) // 32 + turn) % 2 == 0
    new0 = jnp.where(first, part0, pltpu.roll(part1, 32, 1))
    new1 = jnp.where(first, pltpu.roll(part0, 96, 1), part1)
    return new0, new1


def blocks_transposed(parts):
    parts = list(parts)
    width = 128 // len(parts)
    lane = lax.broadcasted_iota(jnp.int32, parts[0].shape, 1) // width
    step = len(parts) // 2
    while step:
        stays = lane // step % 2 == 0
        for i in range(len(parts)):
            if i // step % 2 == 0:
                a, b = parts[i], parts[i + step]
                parts[i] = jnp.where(stays, a, pltpu.roll(b, step * width, 1))
                parts[i + step] = jnp.where(stays, pltpu.roll(a, 128 - step * width, 1), b)
        step //= 2
    return parts


def picked_blocks(parts):
    block = lax.broadcasted_iota(jnp.int32, parts[0].shape, 1) // 32
    picked = []
    for k in range(4):
        value = parts[-k % 4]
        for p in range(1, 4):
            value = jnp.where(block == p, parts[(p - k) % 4], value)
        picked.append(value)
    return picked


def gathered_blocks(parts):
    return [pltpu.roll(v, 128 - 32 * b, 1) if b else v for b, v in enumerate(picked_blocks(parts))]


def scattered_blocks(parts):
    return picked_blocks([pltpu.roll(v, 32 * b, 1) if b else v for b, v in enumerate(parts)])


def quarters(values, sign):
    (ar, ai), (br, bi), (cr, ci), (dr, di) = values
    sr, si, tr, ti = ar + cr, ai + ci, br + dr, bi + di
    ur, ui, vr, vi = ar - cr, ai - ci, sign * (br - dr), sign * (bi - di)
    return [(sr + tr, si + ti), (ur - vi, ui + vr), (sr - tr, si - ti), (ur + vi, ui - vr)]


def left_product(table, values):
    high, low = split(values)
    count = table.shape[0] // 2
    both = product(table, high)
    return both[:count] + both[count:] + product(table[:count], low)


def right_product(values, table_high, table_low, dims):
    count = values.shape[0] // 2
    both = product(values, table_high, dims)
    return both[:count] + both[count:] + product(values[:count], table_low, dims)


def into_kernel(noise_far, spectrum_far, high_far, low_far, out, noise, spectrum, t_high, t_low, arrived):
    moves = [(high_far, t_high, 0, 256), (low_far, t_low, 0, 256)]
    moves += [(noise_far, noise, quarter * 256, 256) for quarter in range(4)]
    copies = []
    for far, near, at, count in moves:
        rows = pl.ds(at, count)
        copies.append(pltpu.make_async_copy(far.at[rows, :], near.at[rows, :], arrived.at[len(copies)]))
    for half in range(2):
        columns = spectrum_far.at[:, pl.ds(half * 128, 128)]
        copies.append(pltpu.make_async_copy(columns, spectrum.at[half], arrived.at[len(copies)]))
    for copy in copies:
        copy.start()
    for copy in copies[:6]:
        copy.wait()
    table = t_high[...], t_low[...]
    nt = (((1,), (1,)), ((), ()))
    turn = lax.axis_index("py") % 4
    for pair in range(4):
        starts = [pl.multiple_of(base + (2 * pair + at) * 64, 32) for at in range(2) for base in places(turn)]
        block = jnp.concatenate([noise[pl.ds(s, 32), :] for s in starts], 0)
        made = product3(table, split(block), nt)
        for at in range(2):
            xh = 2 * pair + at
            part0 = made[:128, at * 128 : at * 128 + 128]
            part1 = made[128:, at * 128 : at * 128 + 128]
            out[pl.ds(xh, DEVICES, stride=SEND_ROWS), :] = part0
            out[pl.ds(8 + xh, DEVICES, stride=SEND_ROWS), :] = part1
            new0, new1 = swapped_parts(part0[:8], part1[:8], turn)
            out[xh : xh + 1, :] = new0[:1]
            out[8 + xh : 9 + xh, :] = new1[:1]
    for copy in copies[6:]:
        copy.wait()
    lower = lax.axis_index("py") < N_PY // 2
    for r in range(4):
        plane = spectrum[0, pl.ds(r, 128, stride=4), :].T
        other = spectrum[1, pl.ds(r, 128, stride=4), :].T[:1]
        out[pl.ds(16 + r, DEVICES, stride=SEND_ROWS), :] = plane
        out[16 + r : 17 + r, :] = jnp.where(lower, plane[:1], other)
        if r == 0:
            out[pl.ds(20, DEVICES, stride=SEND_ROWS), :] = plane
            out[20:21, :] = jnp.where(lower, other, plane[:1])


def unfold(got, scale, first):
    row = lax.broadcasted_iota(jnp.int32, (128, 128), 0)
    lane = lax.broadcasted_iota(jnp.int32, (128, 128), 1)
    j_sum = row % 8 * 16 + row // 8 + lane % 8 * 16 + lane // 8
    rows_turned = jnp.where(j_sum % 128 == 0, 1.0, 0.0).astype(BF16)
    around = jnp.where((row + lane) % 128 == 0, 1.0, 0.0).astype(BF16)
    mirrored = jnp.where(row + lane == 127, 1.0, 0.0).astype(BF16)
    columns = []
    for py in (8, 0):
        v = got[pl.ds(py * SEND_ROWS + 20, N_PX, stride=N_PY * SEND_ROWS), :]
        columns.append(jnp.concatenate([jnp.broadcast_to(v[:, 8 * j : 8 * j + 1], (8, 128)) for j in range(16)], 0))
    for r in range(4):
        own = scale[r * 128 : r * 128 + 128, :]
        at = (4 - r) % 4 * 128
        high, low = split(scale[at : at + 128, :])
        turn = mirrored if r else around
        sides = [product(product(rows_turned, part).astype(BF16), turn) for part in (high, low)]
        partner = sides[0] + sides[1]
        zero = jnp.where(lane < 64, own, partner)
        half = jnp.where(lane < 64, partner, own)
        if r == 0:
            zero = jnp.where(lane == 64, columns[0], zero)
            half = jnp.where(lane == 0, columns[1], half)
        scale[512 + r * 128 : 640 + r * 128, :] = jnp.where(first, zero, own)
        scale[1024 + r * 128 : 1152 + r * 128, :] = jnp.where(first, half, own)


def middle_kernel(got, y_high, y_low, x_into, x_back, out, left, scale):
    plain, turned = (((1,), (0,)), ((), ())), (((1,), (1,)), ((), ()))
    along_y = []
    for side in range(SIDES):
        for at_px in range(N_PX // SIDES):
            px = side * (N_PX // SIDES) + at_px
            blocks = []
            for q in range(4):
                at = [(px * N_PY + 4 * q + i) * SEND_ROWS for i in range(4)]
                parts = [gathered_blocks([got[pl.ds(s + 8 * part, 8), :] for s in at]) for part in range(2)]
                blocks.append(parts)
            for f in range(2):
                pair = []
                for xl in range(2):
                    b = 2 * xl + f
                    pair.append(quarters([(blocks[q][0][b], blocks[q][1][b]) for q in range(4)], -1.0))
                row = f * SIDE_ROWS + at_px * 16
                for r in range(4):
                    for part in range(2):
                        lanes = slice(part * 128, part * 128 + 128)
                        high, low = split(jnp.concatenate([pair[0][r][part], pair[1][r][part]], 0))
                        left[side, r, row : row + 16, lanes] = high
                        left[side, r, 2 * SIDE_ROWS + row : 2 * SIDE_ROWS + row + 16, lanes] = low
        made = []
        for r in range(4):
            rows = slice(r * 256, r * 256 + 256)
            made.append(right_product(left[side, r], y_high[rows, :], y_low[rows, :], plain))
        along_y.append(made)
    for r in range(4):
        step = N_PY * SEND_ROWS
        pieces = [got[pl.ds(py * SEND_ROWS + 16 + r, N_PX, stride=step), :] for py in range(N_PY)]
        for j, block in enumerate(blocks_transposed(pieces)):
            scale[r * 128 + j * 8 : r * 128 + j * 8 + 8, :] = block
    unfold(got, scale, (lax.axis_index("px") == 0) & (lax.axis_index("py") == 0))
    spectral = []
    for f in range(2):
        rows = slice(f * SIDE_ROWS, f * SIDE_ROWS + SIDE_ROWS)
        parts = []
        for part in range(2):
            lanes = slice(part * 128, part * 128 + 128)
            for made in along_y:
                parts.append(jnp.concatenate([a[rows, lanes] for a in made], 1))
        spectral.append(left_product(x_into[...], jnp.concatenate(parts, 0)))
    restored = []
    for f in range(2):
        at = [512 + (f * 4 + r) * 128 for r in range(4)]
        s = jnp.concatenate([scale[k : k + 128, :] for k in at], 1) * (1.0 / (NX * NY * NZ))
        scaled = jnp.concatenate([spectral[f][:128] * s, spectral[f][128:] * s], 0)
        restored.append(left_product(x_back[...], scaled))
    for side in range(SIDES):
        back = []
        for r in range(4):
            lanes = slice(r * 128, r * 128 + 128)
            at, end = side * SIDE_ROWS, side * SIDE_ROWS + SIDE_ROWS
            rows = [jnp.concatenate([z[at:end, lanes], z[128 + at : 128 + end, lanes]], 1) for z in restored]
            values = jnp.concatenate(split(jnp.concatenate(rows, 0)), 0)
            table = slice(r * 256, r * 256 + 256)
            back.append(right_product(values, y_high[table, :], y_low[table, :], turned))
        for at_px in range(N_PX // SIDES):
            px = side * (N_PX // SIDES) + at_px
            blocks = []
            for b in range(4):
                row = (b % 2) * SIDE_ROWS + at_px * 16 + (b // 2) * 8
                blocks.append(quarters([(u[row : row + 8, :128], u[row : row + 8, 128:]) for u in back], 1.0))
            for q in range(4):
                for part in range(2):
                    for i, block in enumerate(scattered_blocks([blocks[b][q][part] for b in range(4)])):
                        at = (px * N_PY + 4 * q + i) * BACK_ROWS + 8 * part
                        out[at : at + 8, :] = block


def last_kernel(got, b_high, b_low, mean1, mean2, mean3, modulus_far, route, sums, sums2, sums3, modulus, left):
    copies = []
    table = b_high[...], b_low[...]
    turn = lax.axis_index("py") % 4
    first_row = lax.broadcasted_iota(jnp.int32, (128, 128), 0) == 0
    for pair in range(4):
        rows = []
        for at in range(2):
            xh = 2 * pair + at
            part0 = got[pl.ds(xh, DEVICES, stride=BACK_ROWS), :]
            part1 = got[pl.ds(8 + xh, DEVICES, stride=BACK_ROWS), :]
            new0, new1 = swapped_parts(part0, part1, turn)
            part0 = jnp.where(first_row, 0.5 * new0, part0)
            part1 = jnp.where(first_row, 0.5 * new1, part1)
            rows.append(jnp.concatenate([part0.T, part1.T], 1))
        values = jnp.exp(product3(split(jnp.concatenate(rows, 0)), table))
        for at in range(2):
            xh = 2 * pair + at
            cells = [values[at * 128 + p * 32 : at * 128 + p * 32 + 32] for p in range(4)]
            for p, base in enumerate(places(turn)):
                modulus[pl.ds(pl.multiple_of(base + xh * 64, 32), 32), :] = cells[p]
            for p in range(2):
                both = cells[p] + cells[p + 2]
                rows = pl.ds(pl.multiple_of((p + turn) % 2 * 256 + xh * 32, 32), 32)
                sums[0, rows, :] = both[:, :128]
                sums[1, rows, :] = both[:, 128:]
        for f in range(2):
            rows = pl.ds(f * 512 + pair * 128, 128)
            copies.append(pltpu.make_async_copy(modulus.at[rows, :], modulus_far.at[rows, :], left.at[len(copies)]))
            copies[-1].start()
    one = jnp.zeros((256, 128), F32)
    for half in range(2):
        cells = sums[half, pl.ds(0, 256, stride=2), :] + sums[half, pl.ds(1, 256, stride=2), :]
        weights = mean1[half * 128 : half * 128 + 128, :]
        h, l = split(cells)
        one = one + (product(h, weights) + product(l, weights))
    for p in range(N_PY):
        route[p * ROUTE_ROWS : p * ROUTE_ROWS + 16, :] = one[p * 16 : p * 16 + 16]
    for k in range(8):
        sums2[k * 16 : k * 16 + 16, :] = one[k * 32 : k * 32 + 16] + one[k * 32 + 16 : k * 32 + 32]
    h, l = split(sums2[pl.ds(0, 64, stride=2), :] + sums2[pl.ds(1, 64, stride=2), :])
    two = product(h, mean2[...]) + product(l, mean2[...])
    sums2[0:64, :] = two
    for k in range(4):
        sums3[k * 8 : k * 8 + 8, :] = two[k * 16 : k * 16 + 8] + two[k * 16 + 8 : k * 16 + 16]
    h, l = split(sums3[pl.ds(0, 16, stride=2), :] + sums3[pl.ds(1, 16, stride=2), :])
    three = product(h, mean3[...]) + product(l, mean3[...])
    for i in range(4):
        row = sums2[pl.ds(i, N_PY, stride=4), :]
        route[pl.ds(16 + i, N_PY, stride=ROUTE_ROWS), :] = row if i else row + three
    for copy in copies:
        copy.wait()


def pick_kernel(table, got, out):
    low = lax.broadcasted_iota(jnp.int32, (4, 128), 1) < 64
    for g in range(N_PY):
        for k in range(4):
            out[g, k, :, :] = got[table[0, g], k, :, :]
        out[g, 4, :, :] = jnp.where(low, got[table[1, g], 4, :, :], got[table[2, g], 4, :, :])


def unpack_kernel(got, one_far, two_far, three_far, two, three, left):
    copies = [pltpu.make_async_copy(got.at[:, pl.ds(0, 4), :, :], one_far, left.at[0])]
    copies[0].start()
    for p in range(N_PY):
        last = got[p, 4, :, :]
        two[p * 4 : p * 4 + 4, :] = last[:, 0:64]
        three[p : p + 1, :] = last[0:1, 64:96]
    copies.append(pltpu.make_async_copy(two, two_far, left.at[1]))
    copies.append(pltpu.make_async_copy(three, three_far, left.at[2]))
    copies[1].start()
    copies[2].start()
    for copy in copies:
        copy.wait()


def on_chip(x):
    return pltpu.with_memory_space_constraint(x, pltpu.VMEM)


def off_chip(x):
    return pltpu.with_memory_space_constraint(x, pltpu.HBM)


def call(body, name, outs, *operands, scratch=(), **options):
    return pl.pallas_call(
        body,
        out_shape=outs,
        scratch_shapes=list(scratch),
        name=name,
        compiler_params=pltpu.CompilerParams(vmem_limit_bytes=VMEM_BYTES),
        **options,
    )(*operands)


def on_device(white_noise, spectrum, group_table):
    far = {k: tuple(jnp.asarray(t) for t in v) for k, v in make_tables().items()}
    tables = {k: tuple(on_chip(t) for t in v) for k, v in far.items()}
    noise = white_noise.reshape(1024, NZ)
    (sent,) = call(
        into_kernel,
        "into_z",
        [pltpu.VMEM((DEVICES * SEND_ROWS, 128), F32)],
        *(off_chip(a) for a in (noise, spectrum.reshape(512, NZ), *far["into"])),
        in_specs=[FAR] * 4,
        scratch=(
            pltpu.VMEM((1024, NZ), F32),
            pltpu.VMEM((2, 512, 128), F32),
            pltpu.VMEM((256, NZ), BF16),
            pltpu.VMEM((256, NZ), BF16),
            pltpu.SemaphoreType.DMA((8,)),
        ),
    )
    got = lax.all_to_all(sent.reshape(DEVICES, SEND_ROWS, 1, 128), ("px", "py"), 0, 0, tiled=True)
    (restored,) = call(
        middle_kernel,
        "planes",
        [pltpu.VMEM((DEVICES * BACK_ROWS, 128), F32)],
        on_chip(got.reshape(DEVICES * SEND_ROWS, 128)),
        *tables["along_y"],
        *tables["x_into"],
        *tables["x_back"],
        scratch=PLANE_SCRATCH,
    )
    back = lax.all_to_all(restored.reshape(DEVICES, BACK_ROWS, 128), ("px", "py"), 0, 0, tiled=True)
    modulus, route = call(
        last_kernel,
        "back_z",
        [jax.ShapeDtypeStruct((1024, NZ), F32), pltpu.VMEM((N_PY * ROUTE_ROWS, 128), F32)],
        on_chip(back.reshape(DEVICES * BACK_ROWS, 128)),
        *tables["into"],
        jnp.asarray(pair_mean(256)[:, :128]),
        jnp.asarray(pair_mean(128)),
        jnp.asarray(pair_mean(128, 64)),
        out_specs=[FAR, NEAR],
        scratch=(
            pltpu.VMEM((2, 512, 128), F32),
            pltpu.VMEM((128, 128), F32),
            pltpu.VMEM((32, 128), F32),
            pltpu.VMEM((1024, NZ), F32),
            pltpu.SemaphoreType.DMA((8,)),
        ),
    )
    spread = lax.all_to_all(route.reshape(ROUTE), "py", 0, 0, tiled=True)
    (picked,) = call(
        pick_kernel,
        "pick",
        [pltpu.VMEM(ROUTE, F32)],
        group_table,
        on_chip(spread),
        in_specs=[pl.BlockSpec(memory_space=pltpu.SMEM), NEAR],
    )
    levels = lax.all_to_all(picked, "py", 0, 0, tiled=True)
    one, two, three = call(
        unpack_kernel,
        "unpack",
        [jax.ShapeDtypeStruct(s, F32) for s in ((16, 4, 4, 128), (64, 64), (16, 32))],
        on_chip(levels),
        out_specs=[FAR] * 3,
        scratch=(pltpu.VMEM((64, 64), F32), pltpu.VMEM((16, 32), F32), pltpu.SemaphoreType.DMA((3,))),
    )
    return (
        modulus.reshape(2, 16, 32, NZ),
        one.reshape(2, 8, 16, 128),
        two.reshape(2, 4, 8, 64),
        three.reshape(2, 2, 4, 32),
    )


def solution(mesh):
    block = P(None, "px", "py", None)
    return jax.shard_map(
        on_device,
        mesh=mesh,
        in_specs=(block, P("px", "py", None), P()),
        out_specs=(block, block, block, block),
        check_vma=False,
    )
```

```python
import math

import jax
import jax.numpy as jnp
import ml_dtypes
import numpy as np
from jax import lax
from jax.experimental import pallas as pl
from jax.experimental.pallas import tpu as pltpu
from jax.sharding import PartitionSpec as P

NX, NY, NZ = 128, 512, 256
N_PX, N_PY = 8, 16
DEVICES = N_PX * N_PY
SEND_ROWS = 21
BACK_ROWS = 16
ROUTE_ROWS = 20
SIDES = 2
SIDE_ROWS = NX // SIDES
VMEM_BYTES = 24 << 20
ROUTE = (N_PY, ROUTE_ROWS // 4, 4, 128)
F32 = jnp.float32
BF16 = jnp.bfloat16
PLANE_SCRATCH = (pltpu.VMEM((SIDES, 4, 4 * SIDE_ROWS, 256), BF16), pltpu.VMEM((1536, 128), F32))
NEAR = pl.BlockSpec(memory_space=pltpu.VMEM)
FAR = pl.BlockSpec(memory_space=pltpu.HBM)


def halves(table):
    high = table.astype(np.float32).astype(ml_dtypes.bfloat16)
    low = (table - high.astype(np.float64)).astype(np.float32).astype(ml_dtypes.bfloat16)
    return high, low


def angle_tables(rows, columns, length):
    angles = 2.0 * math.pi * ((rows[:, None] * columns[None, :]) % length) / length
    return np.cos(angles), np.sin(angles)


def make_tables():
    d, z = np.arange(NZ // 2), np.arange(NZ)
    cos_z, sin_z = angle_tables(d, z, NZ)
    alternating = (1.0 - 2.0 * (z % 2))[None, :]
    into = np.concatenate([cos_z, alternating, -sin_z[1:]], 0)
    y, m = np.arange(NY // 4), np.arange(NY // 4)
    along_y = []
    for r in range(4):
        cos_y, sin_y = angle_tables(y, 4 * m + r, NY)
        along_y.append(np.block([[cos_y, -sin_y], [sin_y, cos_y]]))
    row = np.arange(NX)
    x_of = (row // 16) * 16 + (row % 8) * 2 + row // 8 % 2
    j_of = (row % 8) * 16 + row // 8
    cos_x, sin_x = angle_tables(j_of, x_of, NX)
    x_into = np.block([[cos_x, sin_x], [-sin_x, cos_x]])
    return dict(
        into=halves(into),
        along_y=halves(np.concatenate(along_y, 0)),
        x_into=(np.concatenate(halves(x_into), 0),),
        x_back=(np.concatenate(halves(x_into.T), 0),),
    )


def pair_mean(size, first=0):
    rows, columns = np.arange(size), np.arange(128) - first
    return (0.125 * (rows[:, None] // 2 == columns[None, :])).astype(ml_dtypes.bfloat16)


def split(values):
    high = values.astype(BF16)
    return high, (values - high.astype(F32)).astype(BF16)


def product(a, b, dims=(((1,), (0,)), ((), ()))):
    return lax.dot_general(a, b, dims, preferred_element_type=F32)


def product3(a, b, dims=(((1,), (0,)), ((), ()))):
    return product(a[0], b[0], dims) + product(a[1], b[0], dims) + product(a[0], b[1], dims)


def places(turn):
    numbers = [(p + 4 - turn) % 4 for p in range(4)]
    return [b % 2 * 512 + b // 2 * 32 for b in numbers]


def swapped_parts(part0, part1, turn):
    first = (lax.broadcasted_iota(jnp.int32, part0.shape, 1) // 32 + turn) % 2 == 0
    new0 = jnp.where(first, part0, pltpu.roll(part1, 32, 1))
    new1 = jnp.where(first, pltpu.roll(part0, 96, 1), part1)
    return new0, new1


def blocks_transposed(parts):
    parts = list(parts)
    width = 128 // len(parts)
    lane = lax.broadcasted_iota(jnp.int32, parts[0].shape, 1) // width
    step = len(parts) // 2
    while step:
        stays = lane // step % 2 == 0
        for i in range(len(parts)):
            if i // step % 2 == 0:
                a, b = parts[i], parts[i + step]
                parts[i] = jnp.where(stays, a, pltpu.roll(b, step * width, 1))
                parts[i + step] = jnp.where(stays, pltpu.roll(a, 128 - step * width, 1), b)
        step //= 2
    return parts


def picked_blocks(parts):
    block = lax.broadcasted_iota(jnp.int32, parts[0].shape, 1) // 32
    picked = []
    for k in range(4):
        value = parts[-k % 4]
        for p in range(1, 4):
            value = jnp.where(block == p, parts[(p - k) % 4], value)
        picked.append(value)
    return picked


def gathered_blocks(parts):
    return [pltpu.roll(v, 128 - 32 * b, 1) if b else v for b, v in enumerate(picked_blocks(parts))]


def scattered_blocks(parts):
    return picked_blocks([pltpu.roll(v, 32 * b, 1) if b else v for b, v in enumerate(parts)])


def quarters(values, sign):
    (ar, ai), (br, bi), (cr, ci), (dr, di) = values
    sr, si, tr, ti = ar + cr, ai + ci, br + dr, bi + di
    ur, ui, vr, vi = ar - cr, ai - ci, sign * (br - dr), sign * (bi - di)
    return [(sr + tr, si + ti), (ur - vi, ui + vr), (sr - tr, si - ti), (ur + vi, ui - vr)]


def left_product(table, values):
    high, low = split(values)
    count = table.shape[0] // 2
    both = product(table, high)
    return both[:count] + both[count:] + product(table[:count], low)


def right_product(values, table_high, table_low, dims):
    count = values.shape[0] // 2
    both = product(values, table_high, dims)
    return both[:count] + both[count:] + product(values[:count], table_low, dims)


def into_kernel(noise_far, spectrum_far, high_far, low_far, out, noise, spectrum, t_high, t_low, arrived):
    moves = [(high_far, t_high, 0, 256), (low_far, t_low, 0, 256)]
    moves += [(noise_far, noise, quarter * 256, 256) for quarter in range(4)]
    copies = []
    for far, near, at, count in moves:
        rows = pl.ds(at, count)
        copies.append(pltpu.make_async_copy(far.at[rows, :], near.at[rows, :], arrived.at[len(copies)]))
    for half in range(2):
        columns = spectrum_far.at[:, pl.ds(half * 128, 128)]
        copies.append(pltpu.make_async_copy(columns, spectrum.at[half], arrived.at[len(copies)]))
    for copy in copies:
        copy.start()
    for copy in copies[:6]:
        copy.wait()
    table = t_high[...], t_low[...]
    nt = (((1,), (1,)), ((), ()))
    turn = lax.axis_index("py") % 4
    for pair in range(4):
        starts = [pl.multiple_of(base + (2 * pair + at) * 64, 32) for at in range(2) for base in places(turn)]
        block = jnp.concatenate([noise[pl.ds(s, 32), :] for s in starts], 0)
        made = product3(table, split(block), nt)
        for at in range(2):
            xh = 2 * pair + at
            part0 = made[:128, at * 128 : at * 128 + 128]
            part1 = made[128:, at * 128 : at * 128 + 128]
            out[pl.ds(xh, DEVICES, stride=SEND_ROWS), :] = part0
            out[pl.ds(8 + xh, DEVICES, stride=SEND_ROWS), :] = part1
            new0, new1 = swapped_parts(part0[:8], part1[:8], turn)
            out[xh : xh + 1, :] = new0[:1]
            out[8 + xh : 9 + xh, :] = new1[:1]
    for copy in copies[6:]:
        copy.wait()
    lower = lax.axis_index("py") < N_PY // 2
    for r in range(4):
        plane = spectrum[0, pl.ds(r, 128, stride=4), :].T
        other = spectrum[1, pl.ds(r, 128, stride=4), :].T[:1]
        out[pl.ds(16 + r, DEVICES, stride=SEND_ROWS), :] = plane
        out[16 + r : 17 + r, :] = jnp.where(lower, plane[:1], other)
        if r == 0:
            out[pl.ds(20, DEVICES, stride=SEND_ROWS), :] = plane
            out[20:21, :] = jnp.where(lower, other, plane[:1])


def unfold(got, scale, first):
    row = lax.broadcasted_iota(jnp.int32, (128, 128), 0)
    lane = lax.broadcasted_iota(jnp.int32, (128, 128), 1)
    j_sum = row % 8 * 16 + row // 8 + lane % 8 * 16 + lane // 8
    rows_turned = jnp.where(j_sum % 128 == 0, 1.0, 0.0).astype(BF16)
    around = jnp.where((row + lane) % 128 == 0, 1.0, 0.0).astype(BF16)
    mirrored = jnp.where(row + lane == 127, 1.0, 0.0).astype(BF16)
    columns = []
    for py in (8, 0):
        v = got[pl.ds(py * SEND_ROWS + 20, N_PX, stride=N_PY * SEND_ROWS), :]
        columns.append(jnp.concatenate([jnp.broadcast_to(v[:, 8 * j : 8 * j + 1], (8, 128)) for j in range(16)], 0))
    for r in range(4):
        own = scale[r * 128 : r * 128 + 128, :]
        at = (4 - r) % 4 * 128
        high, low = split(scale[at : at + 128, :])
        turn = mirrored if r else around
        sides = [product(product(rows_turned, part).astype(BF16), turn) for part in (high, low)]
        partner = sides[0] + sides[1]
        zero = jnp.where(lane < 64, own, partner)
        half = jnp.where(lane < 64, partner, own)
        if r == 0:
            zero = jnp.where(lane == 64, columns[0], zero)
            half = jnp.where(lane == 0, columns[1], half)
        scale[512 + r * 128 : 640 + r * 128, :] = jnp.where(first, zero, own)
        scale[1024 + r * 128 : 1152 + r * 128, :] = jnp.where(first, half, own)


def middle_kernel(got, y_high, y_low, x_into, x_back, out, left, scale):
    plain, turned = (((1,), (0,)), ((), ())), (((1,), (1,)), ((), ()))
    along_y = []
    for side in range(SIDES):
        for at_px in range(N_PX // SIDES):
            px = side * (N_PX // SIDES) + at_px
            blocks = []
            for q in range(4):
                at = [(px * N_PY + 4 * q + i) * SEND_ROWS for i in range(4)]
                parts = [gathered_blocks([got[pl.ds(s + 8 * part, 8), :] for s in at]) for part in range(2)]
                blocks.append(parts)
            for f in range(2):
                pair = []
                for xl in range(2):
                    b = 2 * xl + f
                    pair.append(quarters([(blocks[q][0][b], blocks[q][1][b]) for q in range(4)], -1.0))
                row = f * SIDE_ROWS + at_px * 16
                for r in range(4):
                    for part in range(2):
                        lanes = slice(part * 128, part * 128 + 128)
                        high, low = split(jnp.concatenate([pair[0][r][part], pair[1][r][part]], 0))
                        left[side, r, row : row + 16, lanes] = high
                        left[side, r, 2 * SIDE_ROWS + row : 2 * SIDE_ROWS + row + 16, lanes] = low
        made = []
        for r in range(4):
            rows = slice(r * 256, r * 256 + 256)
            made.append(right_product(left[side, r], y_high[rows, :], y_low[rows, :], plain))
        along_y.append(made)
    for r in range(4):
        step = N_PY * SEND_ROWS
        pieces = [got[pl.ds(py * SEND_ROWS + 16 + r, N_PX, stride=step), :] for py in range(N_PY)]
        for j, block in enumerate(blocks_transposed(pieces)):
            scale[r * 128 + j * 8 : r * 128 + j * 8 + 8, :] = block
    unfold(got, scale, (lax.axis_index("px") == 0) & (lax.axis_index("py") == 0))
    spectral = []
    for f in range(2):
        rows = slice(f * SIDE_ROWS, f * SIDE_ROWS + SIDE_ROWS)
        parts = []
        for part in range(2):
            lanes = slice(part * 128, part * 128 + 128)
            for made in along_y:
                parts.append(jnp.concatenate([a[rows, lanes] for a in made], 1))
        spectral.append(left_product(x_into[...], jnp.concatenate(parts, 0)))
    restored = []
    for f in range(2):
        at = [512 + (f * 4 + r) * 128 for r in range(4)]
        s = jnp.concatenate([scale[k : k + 128, :] for k in at], 1) * (1.0 / (NX * NY * NZ))
        scaled = jnp.concatenate([spectral[f][:128] * s, spectral[f][128:] * s], 0)
        restored.append(left_product(x_back[...], scaled))
    for side in range(SIDES):
        back = []
        for r in range(4):
            lanes = slice(r * 128, r * 128 + 128)
            at, end = side * SIDE_ROWS, side * SIDE_ROWS + SIDE_ROWS
            rows = [jnp.concatenate([z[at:end, lanes], z[128 + at : 128 + end, lanes]], 1) for z in restored]
            values = jnp.concatenate(split(jnp.concatenate(rows, 0)), 0)
            table = slice(r * 256, r * 256 + 256)
            back.append(right_product(values, y_high[table, :], y_low[table, :], turned))
        for at_px in range(N_PX // SIDES):
            px = side * (N_PX // SIDES) + at_px
            blocks = []
            for b in range(4):
                row = (b % 2) * SIDE_ROWS + at_px * 16 + (b // 2) * 8
                blocks.append(quarters([(u[row : row + 8, :128], u[row : row + 8, 128:]) for u in back], 1.0))
            for q in range(4):
                for part in range(2):
                    for i, block in enumerate(scattered_blocks([blocks[b][q][part] for b in range(4)])):
                        at = (px * N_PY + 4 * q + i) * BACK_ROWS + 8 * part
                        out[at : at + 8, :] = block


def last_kernel(got, b_high, b_low, mean1, mean2, mean3, modulus_far, route, sums, sums2, sums3, modulus, left):
    copies = []
    table = b_high[...], b_low[...]
    turn = lax.axis_index("py") % 4
    first_row = lax.broadcasted_iota(jnp.int32, (128, 128), 0) == 0
    for pair in range(4):
        rows = []
        for at in range(2):
            xh = 2 * pair + at
            part0 = got[pl.ds(xh, DEVICES, stride=BACK_ROWS), :]
            part1 = got[pl.ds(8 + xh, DEVICES, stride=BACK_ROWS), :]
            new0, new1 = swapped_parts(part0, part1, turn)
            part0 = jnp.where(first_row, 0.5 * new0, part0)
            part1 = jnp.where(first_row, 0.5 * new1, part1)
            rows.append(jnp.concatenate([part0.T, part1.T], 1))
        values = jnp.exp(product3(split(jnp.concatenate(rows, 0)), table))
        for at in range(2):
            xh = 2 * pair + at
            cells = [values[at * 128 + p * 32 : at * 128 + p * 32 + 32] for p in range(4)]
            for p, base in enumerate(places(turn)):
                modulus[pl.ds(pl.multiple_of(base + xh * 64, 32), 32), :] = cells[p]
            for p in range(2):
                both = cells[p] + cells[p + 2]
                rows = pl.ds(pl.multiple_of((p + turn) % 2 * 256 + xh * 32, 32), 32)
                sums[0, rows, :] = both[:, :128]
                sums[1, rows, :] = both[:, 128:]
        for f in range(2):
            rows = pl.ds(f * 512 + pair * 128, 128)
            copies.append(pltpu.make_async_copy(modulus.at[rows, :], modulus_far.at[rows, :], left.at[len(copies)]))
            copies[-1].start()
    one = jnp.zeros((256, 128), F32)
    for half in range(2):
        cells = sums[half, pl.ds(0, 256, stride=2), :] + sums[half, pl.ds(1, 256, stride=2), :]
        weights = mean1[half * 128 : half * 128 + 128, :]
        h, l = split(cells)
        one = one + (product(h, weights) + product(l, weights))
    for p in range(N_PY):
        route[p * ROUTE_ROWS : p * ROUTE_ROWS + 16, :] = one[p * 16 : p * 16 + 16]
    for k in range(8):
        sums2[k * 16 : k * 16 + 16, :] = one[k * 32 : k * 32 + 16] + one[k * 32 + 16 : k * 32 + 32]
    h, l = split(sums2[pl.ds(0, 64, stride=2), :] + sums2[pl.ds(1, 64, stride=2), :])
    two = product(h, mean2[...]) + product(l, mean2[...])
    sums2[0:64, :] = two
    for k in range(4):
        sums3[k * 8 : k * 8 + 8, :] = two[k * 16 : k * 16 + 8] + two[k * 16 + 8 : k * 16 + 16]
    h, l = split(sums3[pl.ds(0, 16, stride=2), :] + sums3[pl.ds(1, 16, stride=2), :])
    three = product(h, mean3[...]) + product(l, mean3[...])
    for i in range(4):
        row = sums2[pl.ds(i, N_PY, stride=4), :]
        route[pl.ds(16 + i, N_PY, stride=ROUTE_ROWS), :] = row if i else row + three
    for copy in copies:
        copy.wait()


def pick_kernel(table_row, got, out):
    table = table_row[...]
    low = lax.broadcasted_iota(jnp.int32, (4, 128), 1) < 64
    for g in range(N_PY):
        for k in range(4):
            out[g, k, :, :] = got[table[0, g], k, :, :]
        out[g, 4, :, :] = jnp.where(low, got[table[1, g], 4, :, :], got[table[2, g], 4, :, :])


def unpack_kernel(got, one_far, two_far, three_far, two, three, left):
    copies = [pltpu.make_async_copy(got.at[:, pl.ds(0, 4), :, :], one_far, left.at[0])]
    copies[0].start()
    for p in range(N_PY):
        last = got[p, 4, :, :]
        two[p * 4 : p * 4 + 4, :] = last[:, 0:64]
        three[p : p + 1, :] = last[0:1, 64:96]
    copies.append(pltpu.make_async_copy(two, two_far, left.at[1]))
    copies.append(pltpu.make_async_copy(three, three_far, left.at[2]))
    copies[1].start()
    copies[2].start()
    for copy in copies:
        copy.wait()


def on_chip(x):
    return pltpu.with_memory_space_constraint(x, pltpu.VMEM)


def off_chip(x):
    return pltpu.with_memory_space_constraint(x, pltpu.HBM)


def call(body, name, outs, *operands, scratch=(), **options):
    return pl.pallas_call(
        body,
        out_shape=outs,
        scratch_shapes=list(scratch),
        name=name,
        compiler_params=pltpu.CompilerParams(vmem_limit_bytes=VMEM_BYTES),
        **options,
    )(*operands)


def on_device(white_noise, spectrum, group_table):
    far = {k: tuple(jnp.asarray(t) for t in v) for k, v in make_tables().items()}
    tables = {k: tuple(on_chip(t) for t in v) for k, v in far.items()}
    noise = white_noise.reshape(1024, NZ)
    (sent,) = call(
        into_kernel,
        "into_z",
        [pltpu.VMEM((DEVICES * SEND_ROWS, 128), F32)],
        *(off_chip(a) for a in (noise, spectrum.reshape(512, NZ), *far["into"])),
        in_specs=[FAR] * 4,
        scratch=(
            pltpu.VMEM((1024, NZ), F32),
            pltpu.VMEM((2, 512, 128), F32),
            pltpu.VMEM((256, NZ), BF16),
            pltpu.VMEM((256, NZ), BF16),
            pltpu.SemaphoreType.DMA((8,)),
        ),
    )
    got = lax.all_to_all(sent.reshape(DEVICES, SEND_ROWS, 1, 128), ("px", "py"), 0, 0, tiled=True)
    (restored,) = call(
        middle_kernel,
        "planes",
        [pltpu.VMEM((DEVICES * BACK_ROWS, 128), F32)],
        on_chip(got.reshape(DEVICES * SEND_ROWS, 128)),
        *tables["along_y"],
        *tables["x_into"],
        *tables["x_back"],
        scratch=PLANE_SCRATCH,
    )
    back = lax.all_to_all(restored.reshape(DEVICES, BACK_ROWS, 128), ("px", "py"), 0, 0, tiled=True)
    modulus, route = call(
        last_kernel,
        "back_z",
        [jax.ShapeDtypeStruct((1024, NZ), F32), pltpu.VMEM((N_PY * ROUTE_ROWS, 128), F32)],
        on_chip(back.reshape(DEVICES * BACK_ROWS, 128)),
        *tables["into"],
        jnp.asarray(pair_mean(256)[:, :128]),
        jnp.asarray(pair_mean(128)),
        jnp.asarray(pair_mean(128, 64)),
        out_specs=[FAR, NEAR],
        scratch=(
            pltpu.VMEM((2, 512, 128), F32),
            pltpu.VMEM((128, 128), F32),
            pltpu.VMEM((32, 128), F32),
            pltpu.VMEM((1024, NZ), F32),
            pltpu.SemaphoreType.DMA((8,)),
        ),
    )
    spread = lax.all_to_all(route.reshape(ROUTE), "py", 0, 0, tiled=True)
    (picked,) = call(
        pick_kernel,
        "pick",
        [pltpu.VMEM(ROUTE, F32)],
        on_chip(group_table),
        on_chip(spread),
    )
    levels = lax.all_to_all(picked, "py", 0, 0, tiled=True)
    one, two, three = call(
        unpack_kernel,
        "unpack",
        [jax.ShapeDtypeStruct(s, F32) for s in ((16, 4, 4, 128), (64, 64), (16, 32))],
        on_chip(levels),
        out_specs=[FAR] * 3,
        scratch=(pltpu.VMEM((64, 64), F32), pltpu.VMEM((16, 32), F32), pltpu.SemaphoreType.DMA((3,))),
    )
    return (
        modulus.reshape(2, 16, 32, NZ),
        one.reshape(2, 8, 16, 128),
        two.reshape(2, 4, 8, 64),
        three.reshape(2, 2, 4, 32),
    )


def solution(mesh):
    block = P(None, "px", "py", None)
    return jax.shard_map(
        on_device,
        mesh=mesh,
        in_specs=(block, P("px", "py", None), P()),
        out_specs=(block, block, block, block),
        check_vma=False,
    )
```

```python
import math

import jax
import jax.numpy as jnp
import ml_dtypes
import numpy as np
from jax import lax
from jax.experimental import pallas as pl
from jax.experimental.pallas import tpu as pltpu
from jax.sharding import PartitionSpec as P

NX, NY, NZ = 128, 512, 256
N_PX, N_PY = 8, 16
DEVICES = N_PX * N_PY
SEND_ROWS = 21
BACK_ROWS = 16
ROUTE_ROWS = 20
SIDES = 2
SIDE_ROWS = NX // SIDES
VMEM_BYTES = 24 << 20
ROUTE = (N_PY, ROUTE_ROWS // 4, 4, 128)
F32 = jnp.float32
BF16 = jnp.bfloat16
PLANE_SCRATCH = (pltpu.VMEM((SIDES, 4, 4 * SIDE_ROWS, 256), BF16), pltpu.VMEM((1536, 128), F32))
NEAR = pl.BlockSpec(memory_space=pltpu.VMEM)
FAR = pl.BlockSpec(memory_space=pltpu.HBM)


def halves(table):
    high = table.astype(np.float32).astype(ml_dtypes.bfloat16)
    low = (table - high.astype(np.float64)).astype(np.float32).astype(ml_dtypes.bfloat16)
    return high, low


def angle_tables(rows, columns, length):
    angles = 2.0 * math.pi * ((rows[:, None] * columns[None, :]) % length) / length
    return np.cos(angles), np.sin(angles)


def make_tables():
    d, z = np.arange(NZ // 2), np.arange(NZ)
    cos_z, sin_z = angle_tables(d, z, NZ)
    alternating = (1.0 - 2.0 * (z % 2))[None, :]
    into = np.concatenate([cos_z, alternating, -sin_z[1:]], 0)
    y, m = np.arange(NY // 4), np.arange(NY // 4)
    along_y = []
    for r in range(4):
        cos_y, sin_y = angle_tables(y, 4 * m + r, NY)
        along_y.append(np.block([[cos_y, -sin_y], [sin_y, cos_y]]))
    row = np.arange(NX)
    x_of = (row // 16) * 16 + (row % 8) * 2 + row // 8 % 2
    j_of = (row % 8) * 16 + row // 8
    cos_x, sin_x = angle_tables(j_of, x_of, NX)
    x_into = np.block([[cos_x, sin_x], [-sin_x, cos_x]])
    return dict(
        into=halves(into),
        along_y=halves(np.concatenate(along_y, 0)),
        x_into=(np.concatenate(halves(x_into), 0),),
        x_back=(np.concatenate(halves(x_into.T), 0),),
    )


def cell_mean(width, first=0):
    rows, columns = np.arange(NZ), np.arange(128) - first
    return (width**-3.0 * (rows[:, None] // width == columns[None, :])).astype(ml_dtypes.bfloat16)


def split(values):
    high = values.astype(BF16)
    return high, (values - high.astype(F32)).astype(BF16)


def product(a, b, dims=(((1,), (0,)), ((), ()))):
    return lax.dot_general(a, b, dims, preferred_element_type=F32)


def product3(a, b, dims=(((1,), (0,)), ((), ()))):
    return product(a[0], b[0], dims) + product(a[1], b[0], dims) + product(a[0], b[1], dims)


def places(turn):
    numbers = [(p + 4 - turn) % 4 for p in range(4)]
    return [b % 2 * 512 + b // 2 * 32 for b in numbers]


def swapped_parts(part0, part1, turn):
    first = (lax.broadcasted_iota(jnp.int32, part0.shape, 1) // 32 + turn) % 2 == 0
    new0 = jnp.where(first, part0, pltpu.roll(part1, 32, 1))
    new1 = jnp.where(first, pltpu.roll(part0, 96, 1), part1)
    return new0, new1


def blocks_transposed(parts):
    parts = list(parts)
    width = 128 // len(parts)
    lane = lax.broadcasted_iota(jnp.int32, parts[0].shape, 1) // width
    step = len(parts) // 2
    while step:
        stays = lane // step % 2 == 0
        for i in range(len(parts)):
            if i // step % 2 == 0:
                a, b = parts[i], parts[i + step]
                parts[i] = jnp.where(stays, a, pltpu.roll(b, step * width, 1))
                parts[i + step] = jnp.where(stays, pltpu.roll(a, 128 - step * width, 1), b)
        step //= 2
    return parts


def picked_blocks(parts):
    block = lax.broadcasted_iota(jnp.int32, parts[0].shape, 1) // 32
    picked = []
    for k in range(4):
        value = parts[-k % 4]
        for p in range(1, 4):
            value = jnp.where(block == p, parts[(p - k) % 4], value)
        picked.append(value)
    return picked


def gathered_blocks(parts):
    return [pltpu.roll(v, 128 - 32 * b, 1) if b else v for b, v in enumerate(picked_blocks(parts))]


def scattered_blocks(parts):
    return picked_blocks([pltpu.roll(v, 32 * b, 1) if b else v for b, v in enumerate(parts)])


def quarters(values, sign):
    (ar, ai), (br, bi), (cr, ci), (dr, di) = values
    sr, si, tr, ti = ar + cr, ai + ci, br + dr, bi + di
    ur, ui, vr, vi = ar - cr, ai - ci, sign * (br - dr), sign * (bi - di)
    return [(sr + tr, si + ti), (ur - vi, ui + vr), (sr - tr, si - ti), (ur + vi, ui - vr)]


def left_product(table, values):
    high, low = split(values)
    count = table.shape[0] // 2
    both = product(table, high)
    return both[:count] + both[count:] + product(table[:count], low)


def right_product(values, table_high, table_low, dims):
    count = values.shape[0] // 2
    both = product(values, table_high, dims)
    return both[:count] + both[count:] + product(values[:count], table_low, dims)


def into_kernel(noise_far, spectrum_far, high_far, low_far, out, noise, spectrum, t_high, t_low, arrived):
    moves = [(high_far, t_high, 0, 256), (low_far, t_low, 0, 256)]
    moves += [(noise_far, noise, quarter * 256, 256) for quarter in range(4)]
    copies = []
    for far, near, at, count in moves:
        rows = pl.ds(at, count)
        copies.append(pltpu.make_async_copy(far.at[rows, :], near.at[rows, :], arrived.at[len(copies)]))
    for half in range(2):
        columns = spectrum_far.at[:, pl.ds(half * 128, 128)]
        copies.append(pltpu.make_async_copy(columns, spectrum.at[half], arrived.at[len(copies)]))
    for copy in copies:
        copy.start()
    for copy in copies[:6]:
        copy.wait()
    table = t_high[...], t_low[...]
    nt = (((1,), (1,)), ((), ()))
    turn = lax.axis_index("py") % 4
    for pair in range(4):
        starts = [pl.multiple_of(base + (2 * pair + at) * 64, 32) for at in range(2) for base in places(turn)]
        block = jnp.concatenate([noise[pl.ds(s, 32), :] for s in starts], 0)
        made = product3(table, split(block), nt)
        for at in range(2):
            xh = 2 * pair + at
            part0 = made[:128, at * 128 : at * 128 + 128]
            part1 = made[128:, at * 128 : at * 128 + 128]
            out[pl.ds(xh, DEVICES, stride=SEND_ROWS), :] = part0
            out[pl.ds(8 + xh, DEVICES, stride=SEND_ROWS), :] = part1
            new0, new1 = swapped_parts(part0[:8], part1[:8], turn)
            out[xh : xh + 1, :] = new0[:1]
            out[8 + xh : 9 + xh, :] = new1[:1]
    for copy in copies[6:]:
        copy.wait()
    lower = lax.axis_index("py") < N_PY // 2
    for r in range(4):
        plane = spectrum[0, pl.ds(r, 128, stride=4), :].T
        other = spectrum[1, pl.ds(r, 128, stride=4), :].T[:1]
        out[pl.ds(16 + r, DEVICES, stride=SEND_ROWS), :] = plane
        out[16 + r : 17 + r, :] = jnp.where(lower, plane[:1], other)
        if r == 0:
            out[pl.ds(20, DEVICES, stride=SEND_ROWS), :] = plane
            out[20:21, :] = jnp.where(lower, other, plane[:1])


def unfold(got, scale, first):
    row = lax.broadcasted_iota(jnp.int32, (128, 128), 0)
    lane = lax.broadcasted_iota(jnp.int32, (128, 128), 1)
    j_sum = row % 8 * 16 + row // 8 + lane % 8 * 16 + lane // 8
    rows_turned = jnp.where(j_sum % 128 == 0, 1.0, 0.0).astype(BF16)
    around = jnp.where((row + lane) % 128 == 0, 1.0, 0.0).astype(BF16)
    mirrored = jnp.where(row + lane == 127, 1.0, 0.0).astype(BF16)
    columns = []
    for py in (8, 0):
        v = got[pl.ds(py * SEND_ROWS + 20, N_PX, stride=N_PY * SEND_ROWS), :]
        columns.append(jnp.concatenate([jnp.broadcast_to(v[:, 8 * j : 8 * j + 1], (8, 128)) for j in range(16)], 0))
    for r in range(4):
        own = scale[r * 128 : r * 128 + 128, :]
        at = (4 - r) % 4 * 128
        high, low = split(scale[at : at + 128, :])
        turn = mirrored if r else around
        sides = [product(product(rows_turned, part).astype(BF16), turn) for part in (high, low)]
        partner = sides[0] + sides[1]
        zero = jnp.where(lane < 64, own, partner)
        half = jnp.where(lane < 64, partner, own)
        if r == 0:
            zero = jnp.where(lane == 64, columns[0], zero)
            half = jnp.where(lane == 0, columns[1], half)
        scale[512 + r * 128 : 640 + r * 128, :] = jnp.where(first, zero, own)
        scale[1024 + r * 128 : 1152 + r * 128, :] = jnp.where(first, half, own)


def middle_kernel(got, y_high, y_low, x_into, x_back, out, left, scale):
    plain, turned = (((1,), (0,)), ((), ())), (((1,), (1,)), ((), ()))
    along_y = []
    for side in range(SIDES):
        for at_px in range(N_PX // SIDES):
            px = side * (N_PX // SIDES) + at_px
            blocks = []
            for q in range(4):
                at = [(px * N_PY + 4 * q + i) * SEND_ROWS for i in range(4)]
                parts = [gathered_blocks([got[pl.ds(s + 8 * part, 8), :] for s in at]) for part in range(2)]
                blocks.append(parts)
            for f in range(2):
                pair = []
                for xl in range(2):
                    b = 2 * xl + f
                    pair.append(quarters([(blocks[q][0][b], blocks[q][1][b]) for q in range(4)], -1.0))
                row = f * SIDE_ROWS + at_px * 16
                for r in range(4):
                    for part in range(2):
                        lanes = slice(part * 128, part * 128 + 128)
                        high, low = split(jnp.concatenate([pair[0][r][part], pair[1][r][part]], 0))
                        left[side, r, row : row + 16, lanes] = high
                        left[side, r, 2 * SIDE_ROWS + row : 2 * SIDE_ROWS + row + 16, lanes] = low
        made = []
        for r in range(4):
            rows = slice(r * 256, r * 256 + 256)
            made.append(right_product(left[side, r], y_high[rows, :], y_low[rows, :], plain))
        along_y.append(made)
    for r in range(4):
        step = N_PY * SEND_ROWS
        pieces = [got[pl.ds(py * SEND_ROWS + 16 + r, N_PX, stride=step), :] for py in range(N_PY)]
        for j, block in enumerate(blocks_transposed(pieces)):
            scale[r * 128 + j * 8 : r * 128 + j * 8 + 8, :] = block
    unfold(got, scale, (lax.axis_index("px") == 0) & (lax.axis_index("py") == 0))
    spectral = []
    for f in range(2):
        rows = slice(f * SIDE_ROWS, f * SIDE_ROWS + SIDE_ROWS)
        parts = []
        for part in range(2):
            lanes = slice(part * 128, part * 128 + 128)
            for made in along_y:
                parts.append(jnp.concatenate([a[rows, lanes] for a in made], 1))
        spectral.append(left_product(x_into[...], jnp.concatenate(parts, 0)))
    restored = []
    for f in range(2):
        at = [512 + (f * 4 + r) * 128 for r in range(4)]
        s = jnp.concatenate([scale[k : k + 128, :] for k in at], 1) * (1.0 / (NX * NY * NZ))
        scaled = jnp.concatenate([spectral[f][:128] * s, spectral[f][128:] * s], 0)
        restored.append(left_product(x_back[...], scaled))
    for side in range(SIDES):
        back = []
        for r in range(4):
            lanes = slice(r * 128, r * 128 + 128)
            at, end = side * SIDE_ROWS, side * SIDE_ROWS + SIDE_ROWS
            rows = [jnp.concatenate([z[at:end, lanes], z[128 + at : 128 + end, lanes]], 1) for z in restored]
            values = jnp.concatenate(split(jnp.concatenate(rows, 0)), 0)
            table = slice(r * 256, r * 256 + 256)
            back.append(right_product(values, y_high[table, :], y_low[table, :], turned))
        for at_px in range(N_PX // SIDES):
            px = side * (N_PX // SIDES) + at_px
            blocks = []
            for b in range(4):
                row = (b % 2) * SIDE_ROWS + at_px * 16 + (b // 2) * 8
                blocks.append(quarters([(u[row : row + 8, :128], u[row : row + 8, 128:]) for u in back], 1.0))
            for q in range(4):
                for part in range(2):
                    for i, block in enumerate(scattered_blocks([blocks[b][q][part] for b in range(4)])):
                        at = (px * N_PY + 4 * q + i) * BACK_ROWS + 8 * part
                        out[at : at + 8, :] = block


def box_sums(cells, store):
    for half in range(2):
        store[half, :, :] = cells[half]
    count = cells[0].shape[0] // 2
    return [store[h, pl.ds(0, count, stride=2), :] + store[h, pl.ds(1, count, stride=2), :] for h in range(2)]


def cells_joined(cells, count):
    ends = range(0, cells[0].shape[0], 2 * count)
    return [jnp.concatenate([v[k : k + count] + v[k + count : k + 2 * count] for k in ends], 0) for v in cells]


def averaged(cells, weights):
    high, low = split(jnp.concatenate(cells, 1))
    return product(high, weights[...]) + product(low, weights[...])


def last_kernel(got, b_high, b_low, mean1, mean2, mean3, modulus, route, sums, sums2, sums3):
    table = b_high[...], b_low[...]
    turn = lax.axis_index("py") % 4
    first_row = lax.broadcasted_iota(jnp.int32, (128, 128), 0) == 0
    for pair in range(4):
        rows = []
        for at in range(2):
            xh = 2 * pair + at
            part0 = got[pl.ds(xh, DEVICES, stride=BACK_ROWS), :]
            part1 = got[pl.ds(8 + xh, DEVICES, stride=BACK_ROWS), :]
            new0, new1 = swapped_parts(part0, part1, turn)
            part0 = jnp.where(first_row, 0.5 * new0, part0)
            part1 = jnp.where(first_row, 0.5 * new1, part1)
            rows.append(jnp.concatenate([part0.T, part1.T], 1))
        values = jnp.exp(product3(split(jnp.concatenate(rows, 0)), table))
        for at in range(2):
            xh = 2 * pair + at
            cells = [values[at * 128 + p * 32 : at * 128 + p * 32 + 32] for p in range(4)]
            for p, base in enumerate(places(turn)):
                modulus[pl.ds(pl.multiple_of(base + xh * 64, 32), 32), :] = cells[p]
            for p in range(2):
                both = cells[p] + cells[p + 2]
                rows = pl.ds(pl.multiple_of((p + turn) % 2 * 256 + xh * 32, 32), 32)
                sums[0, rows, :] = both[:, :128]
                sums[1, rows, :] = both[:, 128:]
    cells = [sums[h, pl.ds(0, 256, stride=2), :] + sums[h, pl.ds(1, 256, stride=2), :] for h in range(2)]
    one = averaged(cells, mean1)
    for p in range(N_PY):
        route[p * ROUTE_ROWS : p * ROUTE_ROWS + 16, :] = one[p * 16 : p * 16 + 16]
    cells = box_sums(cells_joined(cells, 16), sums2)
    two = averaged(cells, mean2)
    cells = box_sums(cells_joined(cells, 8), sums3)
    three = averaged(cells, mean3)
    sums[0, 0:64, :] = two
    for i in range(4):
        row = sums[0, pl.ds(i, N_PY, stride=4), :]
        route[pl.ds(16 + i, N_PY, stride=ROUTE_ROWS), :] = row if i else row + three


def pick_kernel(table_row, got, out):
    table = table_row[...]
    low = lax.broadcasted_iota(jnp.int32, (4, 128), 1) < 64
    for g in range(N_PY):
        for k in range(4):
            out[g, k, :, :] = got[table[0, g], k, :, :]
        out[g, 4, :, :] = jnp.where(low, got[table[1, g], 4, :, :], got[table[2, g], 4, :, :])


def unpack_kernel(got, one_far, two_far, three_far, two, three, left):
    copies = [pltpu.make_async_copy(got.at[:, pl.ds(0, 4), :, :], one_far, left.at[0])]
    copies[0].start()
    for p in range(N_PY):
        last = got[p, 4, :, :]
        two[p * 4 : p * 4 + 4, :] = last[:, 0:64]
        three[p : p + 1, :] = last[0:1, 64:96]
    copies.append(pltpu.make_async_copy(two, two_far, left.at[1]))
    copies.append(pltpu.make_async_copy(three, three_far, left.at[2]))
    copies[1].start()
    copies[2].start()
    for copy in copies:
        copy.wait()


def on_chip(x):
    return pltpu.with_memory_space_constraint(x, pltpu.VMEM)


def off_chip(x):
    return pltpu.with_memory_space_constraint(x, pltpu.HBM)


def call(body, name, outs, *operands, scratch=(), **options):
    return pl.pallas_call(
        body,
        out_shape=outs,
        scratch_shapes=list(scratch),
        name=name,
        compiler_params=pltpu.CompilerParams(vmem_limit_bytes=VMEM_BYTES),
        **options,
    )(*operands)


def on_device(white_noise, spectrum, group_table):
    far = {k: tuple(jnp.asarray(t) for t in v) for k, v in make_tables().items()}
    tables = {k: tuple(on_chip(t) for t in v) for k, v in far.items()}
    noise = white_noise.reshape(1024, NZ)
    (sent,) = call(
        into_kernel,
        "into_z",
        [pltpu.VMEM((DEVICES * SEND_ROWS, 128), F32)],
        *(off_chip(a) for a in (noise, spectrum.reshape(512, NZ), *far["into"])),
        in_specs=[FAR] * 4,
        scratch=(
            pltpu.VMEM((1024, NZ), F32),
            pltpu.VMEM((2, 512, 128), F32),
            pltpu.VMEM((256, NZ), BF16),
            pltpu.VMEM((256, NZ), BF16),
            pltpu.SemaphoreType.DMA((8,)),
        ),
    )
    got = lax.all_to_all(sent.reshape(DEVICES, SEND_ROWS, 1, 128), ("px", "py"), 0, 0, tiled=True)
    (restored,) = call(
        middle_kernel,
        "planes",
        [pltpu.VMEM((DEVICES * BACK_ROWS, 128), F32)],
        on_chip(got.reshape(DEVICES * SEND_ROWS, 128)),
        *tables["along_y"],
        *tables["x_into"],
        *tables["x_back"],
        scratch=PLANE_SCRATCH,
    )
    back = lax.all_to_all(restored.reshape(DEVICES, BACK_ROWS, 128), ("px", "py"), 0, 0, tiled=True)
    modulus, route = call(
        last_kernel,
        "back_z",
        [pltpu.VMEM((1024, NZ), F32), pltpu.VMEM((N_PY * ROUTE_ROWS, 128), F32)],
        on_chip(back.reshape(DEVICES * BACK_ROWS, 128)),
        *tables["into"],
        *(on_chip(jnp.asarray(cell_mean(*k))) for k in ((2,), (4,), (8, 64))),
        scratch=(pltpu.VMEM((2, 512, 128), F32), pltpu.VMEM((2, 128, 128), F32), pltpu.VMEM((2, 32, 128), F32)),
    )
    spread = lax.all_to_all(route.reshape(ROUTE), "py", 0, 0, tiled=True)
    (picked,) = call(
        pick_kernel,
        "pick",
        [pltpu.VMEM(ROUTE, F32)],
        on_chip(group_table),
        on_chip(spread),
    )
    levels = lax.all_to_all(picked, "py", 0, 0, tiled=True)
    one, two, three = call(
        unpack_kernel,
        "unpack",
        [jax.ShapeDtypeStruct(s, F32) for s in ((16, 4, 4, 128), (64, 64), (16, 32))],
        on_chip(levels),
        out_specs=[FAR] * 3,
        scratch=(pltpu.VMEM((64, 64), F32), pltpu.VMEM((16, 32), F32), pltpu.SemaphoreType.DMA((3,))),
    )
    return (
        modulus.reshape(2, 16, 32, NZ),
        one.reshape(2, 8, 16, 128),
        two.reshape(2, 4, 8, 64),
        three.reshape(2, 2, 4, 32),
    )


def solution(mesh):
    block = P(None, "px", "py", None)
    return jax.shard_map(
        on_device,
        mesh=mesh,
        in_specs=(block, P("px", "py", None), P()),
        out_specs=(block, block, block, block),
        check_vma=False,
    )
```

```python
import math

import jax
import jax.numpy as jnp
import ml_dtypes
import numpy as np
from jax import lax
from jax.experimental import pallas as pl
from jax.experimental.pallas import tpu as pltpu
from jax.sharding import PartitionSpec as P

NX, NY, NZ = 128, 512, 256
N_PX, N_PY = 8, 16
DEVICES = N_PX * N_PY
SEND_ROWS = 21
BACK_ROWS = 16
ROUTE_ROWS = 20
SIDES = 2
SIDE_ROWS = NX // SIDES
VMEM_BYTES = 24 << 20
ROUTE = (N_PY, ROUTE_ROWS // 4, 4, 128)
F32 = jnp.float32
BF16 = jnp.bfloat16
PLANE_SCRATCH = (pltpu.VMEM((SIDES, 4, 4 * SIDE_ROWS, 256), BF16), pltpu.VMEM((1536, 128), F32))
NEAR = pl.BlockSpec(memory_space=pltpu.VMEM)
FAR = pl.BlockSpec(memory_space=pltpu.HBM)


def halves(table):
    high = table.astype(np.float32).astype(ml_dtypes.bfloat16)
    low = (table - high.astype(np.float64)).astype(np.float32).astype(ml_dtypes.bfloat16)
    return high, low


def angle_tables(rows, columns, length):
    angles = 2.0 * math.pi * ((rows[:, None] * columns[None, :]) % length) / length
    return np.cos(angles), np.sin(angles)


def make_tables():
    d, z = np.arange(NZ // 2), np.arange(NZ)
    cos_z, sin_z = angle_tables(d, z, NZ)
    alternating = (1.0 - 2.0 * (z % 2))[None, :]
    into = np.concatenate([cos_z, alternating, -sin_z[1:]], 0)
    y, m = np.arange(NY // 4), np.arange(NY // 4)
    along_y = []
    for r in range(4):
        cos_y, sin_y = angle_tables(y, 4 * m + r, NY)
        along_y.append(np.block([[cos_y, -sin_y], [sin_y, cos_y]]))
    row = np.arange(NX)
    x_of = (row // 16) * 16 + (row % 8) * 2 + row // 8 % 2
    j_of = (row % 8) * 16 + row // 8
    cos_x, sin_x = angle_tables(j_of, x_of, NX)
    x_into = np.block([[cos_x, sin_x], [-sin_x, cos_x]])
    return dict(
        into=halves(into),
        along_y=halves(np.concatenate(along_y, 0)),
        x_into=(np.concatenate(halves(x_into), 0),),
        x_back=(np.concatenate(halves(x_into.T), 0),),
    )


def pair_mean(size, first=0):
    rows, columns = np.arange(size), np.arange(128) - first
    return (0.125 * (rows[:, None] // 2 == columns[None, :])).astype(ml_dtypes.bfloat16)


def split(values):
    high = values.astype(BF16)
    return high, (values - high.astype(F32)).astype(BF16)


def product(a, b, dims=(((1,), (0,)), ((), ()))):
    return lax.dot_general(a, b, dims, preferred_element_type=F32)


def product3(a, b, dims=(((1,), (0,)), ((), ()))):
    return product(a[0], b[0], dims) + product(a[1], b[0], dims) + product(a[0], b[1], dims)


def places(turn):
    numbers = [(p + 4 - turn) % 4 for p in range(4)]
    return [b % 2 * 512 + b // 2 * 32 for b in numbers]


def swapped_parts(part0, part1, turn):
    first = (lax.broadcasted_iota(jnp.int32, part0.shape, 1) // 32 + turn) % 2 == 0
    new0 = jnp.where(first, part0, pltpu.roll(part1, 32, 1))
    new1 = jnp.where(first, pltpu.roll(part0, 96, 1), part1)
    return new0, new1


def blocks_transposed(parts):
    parts = list(parts)
    width = 128 // len(parts)
    lane = lax.broadcasted_iota(jnp.int32, parts[0].shape, 1) // width
    step = len(parts) // 2
    while step:
        stays = lane // step % 2 == 0
        for i in range(len(parts)):
            if i // step % 2 == 0:
                a, b = parts[i], parts[i + step]
                parts[i] = jnp.where(stays, a, pltpu.roll(b, step * width, 1))
                parts[i + step] = jnp.where(stays, pltpu.roll(a, 128 - step * width, 1), b)
        step //= 2
    return parts


def picked_blocks(parts):
    block = lax.broadcasted_iota(jnp.int32, parts[0].shape, 1) // 32
    picked = []
    for k in range(4):
        value = parts[-k % 4]
        for p in range(1, 4):
            value = jnp.where(block == p, parts[(p - k) % 4], value)
        picked.append(value)
    return picked


def gathered_blocks(parts):
    return [pltpu.roll(v, 128 - 32 * b, 1) if b else v for b, v in enumerate(picked_blocks(parts))]


def scattered_blocks(parts):
    return picked_blocks([pltpu.roll(v, 32 * b, 1) if b else v for b, v in enumerate(parts)])


def quarters(values, sign):
    (ar, ai), (br, bi), (cr, ci), (dr, di) = values
    sr, si, tr, ti = ar + cr, ai + ci, br + dr, bi + di
    ur, ui, vr, vi = ar - cr, ai - ci, sign * (br - dr), sign * (bi - di)
    return [(sr + tr, si + ti), (ur - vi, ui + vr), (sr - tr, si - ti), (ur + vi, ui - vr)]


def left_product(table, values):
    high, low = split(values)
    count = table.shape[0] // 2
    both = product(table, high)
    return both[:count] + both[count:] + product(table[:count], low)


def right_product(values, table_high, table_low, dims):
    count = values.shape[0] // 2
    both = product(values, table_high, dims)
    return both[:count] + both[count:] + product(values[:count], table_low, dims)


def into_kernel(noise_far, spectrum_far, high_far, low_far, out, noise, spectrum, t_high, t_low, arrived):
    moves = [(high_far, t_high, 0, 256), (low_far, t_low, 0, 256)]
    moves += [(noise_far, noise, quarter * 256, 256) for quarter in range(4)]
    copies = []
    for far, near, at, count in moves:
        rows = pl.ds(at, count)
        copies.append(pltpu.make_async_copy(far.at[rows, :], near.at[rows, :], arrived.at[len(copies)]))
    for half in range(2):
        columns = spectrum_far.at[:, pl.ds(half * 128, 128)]
        copies.append(pltpu.make_async_copy(columns, spectrum.at[half], arrived.at[len(copies)]))
    for copy in copies[6:] + copies[:6]:
        copy.start()
    for copy in copies[6:]:
        copy.wait()
    lower = lax.axis_index("py") < N_PY // 2
    for r in range(4):
        plane = spectrum[0, pl.ds(r, 128, stride=4), :].T
        other = spectrum[1, pl.ds(r, 128, stride=4), :].T[:1]
        out[pl.ds(16 + r, DEVICES, stride=SEND_ROWS), :] = plane
        out[16 + r : 17 + r, :] = jnp.where(lower, plane[:1], other)
        if r == 0:
            out[pl.ds(20, DEVICES, stride=SEND_ROWS), :] = plane
            out[20:21, :] = jnp.where(lower, other, plane[:1])
    for copy in copies[:6]:
        copy.wait()
    table = t_high[...], t_low[...]
    nt = (((1,), (1,)), ((), ()))
    turn = lax.axis_index("py") % 4
    for pair in range(4):
        starts = [pl.multiple_of(base + (2 * pair + at) * 64, 32) for at in range(2) for base in places(turn)]
        block = jnp.concatenate([noise[pl.ds(s, 32), :] for s in starts], 0)
        made = product3(table, split(block), nt)
        for at in range(2):
            xh = 2 * pair + at
            part0 = made[:128, at * 128 : at * 128 + 128]
            part1 = made[128:, at * 128 : at * 128 + 128]
            out[pl.ds(xh, DEVICES, stride=SEND_ROWS), :] = part0
            out[pl.ds(8 + xh, DEVICES, stride=SEND_ROWS), :] = part1
            new0, new1 = swapped_parts(part0[:8], part1[:8], turn)
            out[xh : xh + 1, :] = new0[:1]
            out[8 + xh : 9 + xh, :] = new1[:1]


def unfold(got, scale, first):
    row = lax.broadcasted_iota(jnp.int32, (128, 128), 0)
    lane = lax.broadcasted_iota(jnp.int32, (128, 128), 1)
    j_sum = row % 8 * 16 + row // 8 + lane % 8 * 16 + lane // 8
    rows_turned = jnp.where(j_sum % 128 == 0, 1.0, 0.0).astype(BF16)
    around = jnp.where((row + lane) % 128 == 0, 1.0, 0.0).astype(BF16)
    mirrored = jnp.where(row + lane == 127, 1.0, 0.0).astype(BF16)
    columns = []
    for py in (8, 0):
        v = got[pl.ds(py * SEND_ROWS + 20, N_PX, stride=N_PY * SEND_ROWS), :]
        columns.append(jnp.concatenate([jnp.broadcast_to(v[:, 8 * j : 8 * j + 1], (8, 128)) for j in range(16)], 0))
    for r in range(4):
        own = scale[r * 128 : r * 128 + 128, :]
        at = (4 - r) % 4 * 128
        high, low = split(scale[at : at + 128, :])
        turn = mirrored if r else around
        sides = [product(product(rows_turned, part).astype(BF16), turn) for part in (high, low)]
        partner = sides[0] + sides[1]
        zero = jnp.where(lane < 64, own, partner)
        half = jnp.where(lane < 64, partner, own)
        if r == 0:
            zero = jnp.where(lane == 64, columns[0], zero)
            half = jnp.where(lane == 0, columns[1], half)
        scale[512 + r * 128 : 640 + r * 128, :] = jnp.where(first, zero, own)
        scale[1024 + r * 128 : 1152 + r * 128, :] = jnp.where(first, half, own)


def middle_kernel(got, y_high, y_low, x_into, x_back, out, left, scale):
    plain, turned = (((1,), (0,)), ((), ())), (((1,), (1,)), ((), ()))
    along_y = []
    for side in range(SIDES):
        for at_px in range(N_PX // SIDES):
            px = side * (N_PX // SIDES) + at_px
            blocks = []
            for q in range(4):
                at = [(px * N_PY + 4 * q + i) * SEND_ROWS for i in range(4)]
                parts = [gathered_blocks([got[pl.ds(s + 8 * part, 8), :] for s in at]) for part in range(2)]
                blocks.append(parts)
            for f in range(2):
                pair = []
                for xl in range(2):
                    b = 2 * xl + f
                    pair.append(quarters([(blocks[q][0][b], blocks[q][1][b]) for q in range(4)], -1.0))
                row = f * SIDE_ROWS + at_px * 16
                for r in range(4):
                    for part in range(2):
                        lanes = slice(part * 128, part * 128 + 128)
                        high, low = split(jnp.concatenate([pair[0][r][part], pair[1][r][part]], 0))
                        left[side, r, row : row + 16, lanes] = high
                        left[side, r, 2 * SIDE_ROWS + row : 2 * SIDE_ROWS + row + 16, lanes] = low
        made = []
        for r in range(4):
            rows = slice(r * 256, r * 256 + 256)
            made.append(right_product(left[side, r], y_high[rows, :], y_low[rows, :], plain))
        along_y.append(made)
    for r in range(4):
        step = N_PY * SEND_ROWS
        pieces = [got[pl.ds(py * SEND_ROWS + 16 + r, N_PX, stride=step), :] for py in range(N_PY)]
        for j, block in enumerate(blocks_transposed(pieces)):
            scale[r * 128 + j * 8 : r * 128 + j * 8 + 8, :] = block
    unfold(got, scale, (lax.axis_index("px") == 0) & (lax.axis_index("py") == 0))
    spectral = []
    for f in range(2):
        rows = slice(f * SIDE_ROWS, f * SIDE_ROWS + SIDE_ROWS)
        parts = []
        for part in range(2):
            lanes = slice(part * 128, part * 128 + 128)
            for made in along_y:
                parts.append(jnp.concatenate([a[rows, lanes] for a in made], 1))
        spectral.append(left_product(x_into[...], jnp.concatenate(parts, 0)))
    restored = []
    for f in range(2):
        at = [512 + (f * 4 + r) * 128 for r in range(4)]
        s = jnp.concatenate([scale[k : k + 128, :] for k in at], 1) * (1.0 / (NX * NY * NZ))
        scaled = jnp.concatenate([spectral[f][:128] * s, spectral[f][128:] * s], 0)
        restored.append(left_product(x_back[...], scaled))
    for side in range(SIDES):
        back = []
        for r in range(4):
            lanes = slice(r * 128, r * 128 + 128)
            at, end = side * SIDE_ROWS, side * SIDE_ROWS + SIDE_ROWS
            rows = [jnp.concatenate([z[at:end, lanes], z[128 + at : 128 + end, lanes]], 1) for z in restored]
            values = jnp.concatenate(split(jnp.concatenate(rows, 0)), 0)
            table = slice(r * 256, r * 256 + 256)
            back.append(right_product(values, y_high[table, :], y_low[table, :], turned))
        for at_px in range(N_PX // SIDES):
            px = side * (N_PX // SIDES) + at_px
            blocks = []
            for b in range(4):
                row = (b % 2) * SIDE_ROWS + at_px * 16 + (b // 2) * 8
                blocks.append(quarters([(u[row : row + 8, :128], u[row : row + 8, 128:]) for u in back], 1.0))
            for q in range(4):
                for part in range(2):
                    for i, block in enumerate(scattered_blocks([blocks[b][q][part] for b in range(4)])):
                        at = (px * N_PY + 4 * q + i) * BACK_ROWS + 8 * part
                        out[at : at + 8, :] = block


def last_kernel(got, b_high, b_low, mean1, mean2, mean3, modulus_far, route, sums, sums2, sums3, modulus, left):
    copies = []
    table = b_high[...], b_low[...]
    turn = lax.axis_index("py") % 4
    first_row = lax.broadcasted_iota(jnp.int32, (128, 128), 0) == 0
    for pair in range(4):
        rows = []
        for at in range(2):
            xh = 2 * pair + at
            part0 = got[pl.ds(xh, DEVICES, stride=BACK_ROWS), :]
            part1 = got[pl.ds(8 + xh, DEVICES, stride=BACK_ROWS), :]
            new0, new1 = swapped_parts(part0, part1, turn)
            part0 = jnp.where(first_row, 0.5 * new0, part0)
            part1 = jnp.where(first_row, 0.5 * new1, part1)
            rows.append(jnp.concatenate([part0.T, part1.T], 1))
        values = jnp.exp(product3(split(jnp.concatenate(rows, 0)), table))
        for at in range(2):
            xh = 2 * pair + at
            cells = [values[at * 128 + p * 32 : at * 128 + p * 32 + 32] for p in range(4)]
            for p, base in enumerate(places(turn)):
                modulus[pl.ds(pl.multiple_of(base + xh * 64, 32), 32), :] = cells[p]
            for p in range(2):
                both = cells[p] + cells[p + 2]
                rows = pl.ds(pl.multiple_of((p + turn) % 2 * 256 + xh * 32, 32), 32)
                sums[0, rows, :] = both[:, :128]
                sums[1, rows, :] = both[:, 128:]
        for f in range(2):
            rows = pl.ds(f * 512 + pair * 128, 128)
            copies.append(pltpu.make_async_copy(modulus.at[rows, :], modulus_far.at[rows, :], left.at[len(copies)]))
            copies[-1].start()
    one = jnp.zeros((256, 128), F32)
    for half in range(2):
        cells = sums[half, pl.ds(0, 256, stride=2), :] + sums[half, pl.ds(1, 256, stride=2), :]
        weights = mean1[half * 128 : half * 128 + 128, :]
        h, l = split(cells)
        one = one + (product(h, weights) + product(l, weights))
    for p in range(N_PY):
        route[p * ROUTE_ROWS : p * ROUTE_ROWS + 16, :] = one[p * 16 : p * 16 + 16]
    for k in range(8):
        sums2[k * 16 : k * 16 + 16, :] = one[k * 32 : k * 32 + 16] + one[k * 32 + 16 : k * 32 + 32]
    h, l = split(sums2[pl.ds(0, 64, stride=2), :] + sums2[pl.ds(1, 64, stride=2), :])
    two = product(h, mean2[...]) + product(l, mean2[...])
    sums2[0:64, :] = two
    for k in range(4):
        sums3[k * 8 : k * 8 + 8, :] = two[k * 16 : k * 16 + 8] + two[k * 16 + 8 : k * 16 + 16]
    h, l = split(sums3[pl.ds(0, 16, stride=2), :] + sums3[pl.ds(1, 16, stride=2), :])
    three = product(h, mean3[...]) + product(l, mean3[...])
    for i in range(4):
        row = sums2[pl.ds(i, N_PY, stride=4), :]
        route[pl.ds(16 + i, N_PY, stride=ROUTE_ROWS), :] = row if i else row + three
    for copy in copies:
        copy.wait()


def pick_kernel(table_row, got, out):
    table = table_row[...]
    low = lax.broadcasted_iota(jnp.int32, (4, 128), 1) < 64
    for g in range(N_PY):
        for k in range(4):
            out[g, k, :, :] = got[table[0, g], k, :, :]
        out[g, 4, :, :] = jnp.where(low, got[table[1, g], 4, :, :], got[table[2, g], 4, :, :])


def unpack_kernel(got, one_far, two_far, three_far, two, three, left):
    copies = [pltpu.make_async_copy(got.at[:, pl.ds(0, 4), :, :], one_far, left.at[0])]
    copies[0].start()
    for p in range(N_PY):
        last = got[p, 4, :, :]
        two[p * 4 : p * 4 + 4, :] = last[:, 0:64]
        three[p : p + 1, :] = last[0:1, 64:96]
    copies.append(pltpu.make_async_copy(two, two_far, left.at[1]))
    copies.append(pltpu.make_async_copy(three, three_far, left.at[2]))
    copies[1].start()
    copies[2].start()
    for copy in copies:
        copy.wait()


def on_chip(x):
    return pltpu.with_memory_space_constraint(x, pltpu.VMEM)


def off_chip(x):
    return pltpu.with_memory_space_constraint(x, pltpu.HBM)


def call(body, name, outs, *operands, scratch=(), **options):
    return pl.pallas_call(
        body,
        out_shape=outs,
        scratch_shapes=list(scratch),
        name=name,
        compiler_params=pltpu.CompilerParams(vmem_limit_bytes=VMEM_BYTES),
        **options,
    )(*operands)


def on_device(white_noise, spectrum, group_table):
    far = {k: tuple(jnp.asarray(t) for t in v) for k, v in make_tables().items()}
    tables = {k: tuple(on_chip(t) for t in v) for k, v in far.items()}
    noise = white_noise.reshape(1024, NZ)
    (sent,) = call(
        into_kernel,
        "into_z",
        [pltpu.VMEM((DEVICES * SEND_ROWS, 128), F32)],
        *(off_chip(a) for a in (noise, spectrum.reshape(512, NZ), *far["into"])),
        in_specs=[FAR] * 4,
        scratch=(
            pltpu.VMEM((1024, NZ), F32),
            pltpu.VMEM((2, 512, 128), F32),
            pltpu.VMEM((256, NZ), BF16),
            pltpu.VMEM((256, NZ), BF16),
            pltpu.SemaphoreType.DMA((8,)),
        ),
    )
    got = lax.all_to_all(sent.reshape(DEVICES, SEND_ROWS, 1, 128), ("px", "py"), 0, 0, tiled=True)
    (restored,) = call(
        middle_kernel,
        "planes",
        [pltpu.VMEM((DEVICES * BACK_ROWS, 128), F32)],
        on_chip(got.reshape(DEVICES * SEND_ROWS, 128)),
        *tables["along_y"],
        *tables["x_into"],
        *tables["x_back"],
        scratch=PLANE_SCRATCH,
    )
    back = lax.all_to_all(restored.reshape(DEVICES, BACK_ROWS, 128), ("px", "py"), 0, 0, tiled=True)
    modulus, route = call(
        last_kernel,
        "back_z",
        [jax.ShapeDtypeStruct((1024, NZ), F32), pltpu.VMEM((N_PY * ROUTE_ROWS, 128), F32)],
        on_chip(back.reshape(DEVICES * BACK_ROWS, 128)),
        *tables["into"],
        jnp.asarray(pair_mean(256)[:, :128]),
        jnp.asarray(pair_mean(128)),
        jnp.asarray(pair_mean(128, 64)),
        out_specs=[FAR, NEAR],
        scratch=(
            pltpu.VMEM((2, 512, 128), F32),
            pltpu.VMEM((128, 128), F32),
            pltpu.VMEM((32, 128), F32),
            pltpu.VMEM((1024, NZ), F32),
            pltpu.SemaphoreType.DMA((8,)),
        ),
    )
    spread = lax.all_to_all(route.reshape(ROUTE), "py", 0, 0, tiled=True)
    (picked,) = call(
        pick_kernel,
        "pick",
        [pltpu.VMEM(ROUTE, F32)],
        on_chip(group_table),
        on_chip(spread),
    )
    levels = lax.all_to_all(picked, "py", 0, 0, tiled=True)
    one, two, three = call(
        unpack_kernel,
        "unpack",
        [jax.ShapeDtypeStruct(s, F32) for s in ((16, 4, 4, 128), (64, 64), (16, 32))],
        on_chip(levels),
        out_specs=[FAR] * 3,
        scratch=(pltpu.VMEM((64, 64), F32), pltpu.VMEM((16, 32), F32), pltpu.SemaphoreType.DMA((3,))),
    )
    return (
        modulus.reshape(2, 16, 32, NZ),
        one.reshape(2, 8, 16, 128),
        two.reshape(2, 4, 8, 64),
        three.reshape(2, 2, 4, 32),
    )


def solution(mesh):
    block = P(None, "px", "py", None)
    return jax.shard_map(
        on_device,
        mesh=mesh,
        in_specs=(block, P("px", "py", None), P()),
        out_specs=(block, block, block, block),
        check_vma=False,
    )
```

```python
import math

import jax
import jax.numpy as jnp
import ml_dtypes
import numpy as np
from jax import lax
from jax.experimental import pallas as pl
from jax.experimental.pallas import tpu as pltpu
from jax.sharding import PartitionSpec as P

NX, NY, NZ = 128, 512, 256
N_PX, N_PY = 8, 16
DEVICES = N_PX * N_PY
SEND_ROWS = 21
BACK_ROWS = 16
ROUTE_ROWS = 20
SIDES = 1
SIDE_ROWS = NX // SIDES
VMEM_BYTES = 24 << 20
ROUTE = (N_PY, ROUTE_ROWS // 4, 4, 128)
F32 = jnp.float32
BF16 = jnp.bfloat16
PLANE_SCRATCH = (pltpu.VMEM((SIDES, 4, 4 * SIDE_ROWS, 256), BF16), pltpu.VMEM((1536, 128), F32))
NEAR = pl.BlockSpec(memory_space=pltpu.VMEM)
FAR = pl.BlockSpec(memory_space=pltpu.HBM)


def halves(table):
    high = table.astype(np.float32).astype(ml_dtypes.bfloat16)
    low = (table - high.astype(np.float64)).astype(np.float32).astype(ml_dtypes.bfloat16)
    return high, low


def angle_tables(rows, columns, length):
    angles = 2.0 * math.pi * ((rows[:, None] * columns[None, :]) % length) / length
    return np.cos(angles), np.sin(angles)


def make_tables():
    d, z = np.arange(NZ // 2), np.arange(NZ)
    cos_z, sin_z = angle_tables(d, z, NZ)
    alternating = (1.0 - 2.0 * (z % 2))[None, :]
    into = np.concatenate([cos_z, alternating, -sin_z[1:]], 0)
    y, m = np.arange(NY // 4), np.arange(NY // 4)
    along_y = []
    for r in range(4):
        cos_y, sin_y = angle_tables(y, 4 * m + r, NY)
        along_y.append(np.block([[cos_y, -sin_y], [sin_y, cos_y]]))
    row = np.arange(NX)
    x_of = (row // 16) * 16 + (row % 8) * 2 + row // 8 % 2
    j_of = (row % 8) * 16 + row // 8
    cos_x, sin_x = angle_tables(j_of, x_of, NX)
    x_into = np.block([[cos_x, sin_x], [-sin_x, cos_x]])
    return dict(
        into=halves(into),
        along_y=halves(np.concatenate(along_y, 0)),
        x_into=(np.concatenate(halves(x_into), 0),),
        x_back=(np.concatenate(halves(x_into.T), 0),),
    )


def pair_mean(size, first=0):
    rows, columns = np.arange(size), np.arange(128) - first
    return (0.125 * (rows[:, None] // 2 == columns[None, :])).astype(ml_dtypes.bfloat16)


def split(values):
    high = values.astype(BF16)
    return high, (values - high.astype(F32)).astype(BF16)


def product(a, b, dims=(((1,), (0,)), ((), ()))):
    return lax.dot_general(a, b, dims, preferred_element_type=F32)


def product3(a, b, dims=(((1,), (0,)), ((), ()))):
    return product(a[0], b[0], dims) + product(a[1], b[0], dims) + product(a[0], b[1], dims)


def places(turn):
    numbers = [(p + 4 - turn) % 4 for p in range(4)]
    return [b % 2 * 512 + b // 2 * 32 for b in numbers]


def swapped_parts(part0, part1, turn):
    first = (lax.broadcasted_iota(jnp.int32, part0.shape, 1) // 32 + turn) % 2 == 0
    new0 = jnp.where(first, part0, pltpu.roll(part1, 32, 1))
    new1 = jnp.where(first, pltpu.roll(part0, 96, 1), part1)
    return new0, new1


def blocks_transposed(parts):
    parts = list(parts)
    width = 128 // len(parts)
    lane = lax.broadcasted_iota(jnp.int32, parts[0].shape, 1) // width
    step = len(parts) // 2
    while step:
        stays = lane // step % 2 == 0
        for i in range(len(parts)):
            if i // step % 2 == 0:
                a, b = parts[i], parts[i + step]
                parts[i] = jnp.where(stays, a, pltpu.roll(b, step * width, 1))
                parts[i + step] = jnp.where(stays, pltpu.roll(a, 128 - step * width, 1), b)
        step //= 2
    return parts


def picked_blocks(parts):
    block = lax.broadcasted_iota(jnp.int32, parts[0].shape, 1) // 32
    picked = []
    for k in range(4):
        value = parts[-k % 4]
        for p in range(1, 4):
            value = jnp.where(block == p, parts[(p - k) % 4], value)
        picked.append(value)
    return picked


def gathered_blocks(parts):
    return [pltpu.roll(v, 128 - 32 * b, 1) if b else v for b, v in enumerate(picked_blocks(parts))]


def scattered_blocks(parts):
    return picked_blocks([pltpu.roll(v, 32 * b, 1) if b else v for b, v in enumerate(parts)])


def quarters(values, sign):
    (ar, ai), (br, bi), (cr, ci), (dr, di) = values
    sr, si, tr, ti = ar + cr, ai + ci, br + dr, bi + di
    ur, ui, vr, vi = ar - cr, ai - ci, sign * (br - dr), sign * (bi - di)
    return [(sr + tr, si + ti), (ur - vi, ui + vr), (sr - tr, si - ti), (ur + vi, ui - vr)]


def left_product(table, values):
    high, low = split(values)
    count = table.shape[0] // 2
    both = product(table, high)
    return both[:count] + both[count:] + product(table[:count], low)


def right_product(values, table_high, table_low, dims):
    count = values.shape[0] // 2
    both = product(values, table_high, dims)
    return both[:count] + both[count:] + product(values[:count], table_low, dims)


def into_kernel(noise_far, spectrum_far, high_far, low_far, out, noise, spectrum, t_high, t_low, arrived):
    moves = [(high_far, t_high, 0, 256), (low_far, t_low, 0, 256)]
    moves += [(noise_far, noise, quarter * 256, 256) for quarter in range(4)]
    copies = []
    for far, near, at, count in moves:
        rows = pl.ds(at, count)
        copies.append(pltpu.make_async_copy(far.at[rows, :], near.at[rows, :], arrived.at[len(copies)]))
    for half in range(2):
        columns = spectrum_far.at[:, pl.ds(half * 128, 128)]
        copies.append(pltpu.make_async_copy(columns, spectrum.at[half], arrived.at[len(copies)]))
    for copy in copies[6:] + copies[:6]:
        copy.start()
    for copy in copies[6:]:
        copy.wait()
    lower = lax.axis_index("py") < N_PY // 2
    for r in range(4):
        plane = spectrum[0, pl.ds(r, 128, stride=4), :].T
        other = spectrum[1, pl.ds(r, 128, stride=4), :].T[:1]
        out[pl.ds(16 + r, DEVICES, stride=SEND_ROWS), :] = plane
        out[16 + r : 17 + r, :] = jnp.where(lower, plane[:1], other)
        if r == 0:
            out[pl.ds(20, DEVICES, stride=SEND_ROWS), :] = plane
            out[20:21, :] = jnp.where(lower, other, plane[:1])
    for copy in copies[:6]:
        copy.wait()
    table = t_high[...], t_low[...]
    nt = (((1,), (1,)), ((), ()))
    turn = lax.axis_index("py") % 4
    for pair in range(4):
        starts = [pl.multiple_of(base + (2 * pair + at) * 64, 32) for at in range(2) for base in places(turn)]
        block = jnp.concatenate([noise[pl.ds(s, 32), :] for s in starts], 0)
        made = product3(table, split(block), nt)
        for at in range(2):
            xh = 2 * pair + at
            part0 = made[:128, at * 128 : at * 128 + 128]
            part1 = made[128:, at * 128 : at * 128 + 128]
            out[pl.ds(xh, DEVICES, stride=SEND_ROWS), :] = part0
            out[pl.ds(8 + xh, DEVICES, stride=SEND_ROWS), :] = part1
            new0, new1 = swapped_parts(part0[:8], part1[:8], turn)
            out[xh : xh + 1, :] = new0[:1]
            out[8 + xh : 9 + xh, :] = new1[:1]


def unfold(got, scale, first):
    row = lax.broadcasted_iota(jnp.int32, (128, 128), 0)
    lane = lax.broadcasted_iota(jnp.int32, (128, 128), 1)
    j_sum = row % 8 * 16 + row // 8 + lane % 8 * 16 + lane // 8
    rows_turned = jnp.where(j_sum % 128 == 0, 1.0, 0.0).astype(BF16)
    around = jnp.where((row + lane) % 128 == 0, 1.0, 0.0).astype(BF16)
    mirrored = jnp.where(row + lane == 127, 1.0, 0.0).astype(BF16)
    columns = []
    for py in (8, 0):
        v = got[pl.ds(py * SEND_ROWS + 20, N_PX, stride=N_PY * SEND_ROWS), :]
        columns.append(jnp.concatenate([jnp.broadcast_to(v[:, 8 * j : 8 * j + 1], (8, 128)) for j in range(16)], 0))
    for r in range(4):
        own = scale[r * 128 : r * 128 + 128, :]
        at = (4 - r) % 4 * 128
        high, low = split(scale[at : at + 128, :])
        turn = mirrored if r else around
        sides = [product(product(rows_turned, part).astype(BF16), turn) for part in (high, low)]
        partner = sides[0] + sides[1]
        zero = jnp.where(lane < 64, own, partner)
        half = jnp.where(lane < 64, partner, own)
        if r == 0:
            zero = jnp.where(lane == 64, columns[0], zero)
            half = jnp.where(lane == 0, columns[1], half)
        scale[512 + r * 128 : 640 + r * 128, :] = jnp.where(first, zero, own)
        scale[1024 + r * 128 : 1152 + r * 128, :] = jnp.where(first, half, own)


def middle_kernel(got, y_high, y_low, x_into, x_back, out, left, scale):
    plain, turned = (((1,), (0,)), ((), ())), (((1,), (1,)), ((), ()))
    along_y = []
    for side in range(SIDES):
        for at_px in range(N_PX // SIDES):
            px = side * (N_PX // SIDES) + at_px
            blocks = []
            for q in range(4):
                at = [(px * N_PY + 4 * q + i) * SEND_ROWS for i in range(4)]
                parts = [gathered_blocks([got[pl.ds(s + 8 * part, 8), :] for s in at]) for part in range(2)]
                blocks.append(parts)
            for f in range(2):
                pair = []
                for xl in range(2):
                    b = 2 * xl + f
                    pair.append(quarters([(blocks[q][0][b], blocks[q][1][b]) for q in range(4)], -1.0))
                row = f * SIDE_ROWS + at_px * 16
                for r in range(4):
                    for part in range(2):
                        lanes = slice(part * 128, part * 128 + 128)
                        high, low = split(jnp.concatenate([pair[0][r][part], pair[1][r][part]], 0))
                        left[side, r, row : row + 16, lanes] = high
                        left[side, r, 2 * SIDE_ROWS + row : 2 * SIDE_ROWS + row + 16, lanes] = low
        made = []
        for r in range(4):
            rows = slice(r * 256, r * 256 + 256)
            made.append(right_product(left[side, r], y_high[rows, :], y_low[rows, :], plain))
        along_y.append(made)
    for r in range(4):
        step = N_PY * SEND_ROWS
        pieces = [got[pl.ds(py * SEND_ROWS + 16 + r, N_PX, stride=step), :] for py in range(N_PY)]
        for j, block in enumerate(blocks_transposed(pieces)):
            scale[r * 128 + j * 8 : r * 128 + j * 8 + 8, :] = block
    unfold(got, scale, (lax.axis_index("px") == 0) & (lax.axis_index("py") == 0))
    spectral = []
    for f in range(2):
        rows = slice(f * SIDE_ROWS, f * SIDE_ROWS + SIDE_ROWS)
        parts = []
        for part in range(2):
            lanes = slice(part * 128, part * 128 + 128)
            for made in along_y:
                parts.append(jnp.concatenate([a[rows, lanes] for a in made], 1))
        spectral.append(left_product(x_into[...], jnp.concatenate(parts, 0)))
    restored = []
    for f in range(2):
        at = [512 + (f * 4 + r) * 128 for r in range(4)]
        s = jnp.concatenate([scale[k : k + 128, :] for k in at], 1) * (1.0 / (NX * NY * NZ))
        scaled = jnp.concatenate([spectral[f][:128] * s, spectral[f][128:] * s], 0)
        restored.append(left_product(x_back[...], scaled))
    for side in range(SIDES):
        back = []
        for r in range(4):
            lanes = slice(r * 128, r * 128 + 128)
            at, end = side * SIDE_ROWS, side * SIDE_ROWS + SIDE_ROWS
            rows = [jnp.concatenate([z[at:end, lanes], z[128 + at : 128 + end, lanes]], 1) for z in restored]
            values = jnp.concatenate(split(jnp.concatenate(rows, 0)), 0)
            table = slice(r * 256, r * 256 + 256)
            back.append(right_product(values, y_high[table, :], y_low[table, :], turned))
        for at_px in range(N_PX // SIDES):
            px = side * (N_PX // SIDES) + at_px
            blocks = []
            for b in range(4):
                row = (b % 2) * SIDE_ROWS + at_px * 16 + (b // 2) * 8
                blocks.append(quarters([(u[row : row + 8, :128], u[row : row + 8, 128:]) for u in back], 1.0))
            for q in range(4):
                for part in range(2):
                    for i, block in enumerate(scattered_blocks([blocks[b][q][part] for b in range(4)])):
                        at = (px * N_PY + 4 * q + i) * BACK_ROWS + 8 * part
                        out[at : at + 8, :] = block


def last_kernel(got, b_high, b_low, mean1, mean2, mean3, modulus_far, route, sums, sums2, sums3, modulus, left):
    copies = []
    table = b_high[...], b_low[...]
    turn = lax.axis_index("py") % 4
    first_row = lax.broadcasted_iota(jnp.int32, (128, 128), 0) == 0
    for pair in range(4):
        rows = []
        for at in range(2):
            xh = 2 * pair + at
            part0 = got[pl.ds(xh, DEVICES, stride=BACK_ROWS), :]
            part1 = got[pl.ds(8 + xh, DEVICES, stride=BACK_ROWS), :]
            new0, new1 = swapped_parts(part0, part1, turn)
            part0 = jnp.where(first_row, 0.5 * new0, part0)
            part1 = jnp.where(first_row, 0.5 * new1, part1)
            rows.append(jnp.concatenate([part0.T, part1.T], 1))
        values = jnp.exp(product3(split(jnp.concatenate(rows, 0)), table))
        for at in range(2):
            xh = 2 * pair + at
            cells = [values[at * 128 + p * 32 : at * 128 + p * 32 + 32] for p in range(4)]
            for p, base in enumerate(places(turn)):
                modulus[pl.ds(pl.multiple_of(base + xh * 64, 32), 32), :] = cells[p]
            for p in range(2):
                both = cells[p] + cells[p + 2]
                rows = pl.ds(pl.multiple_of((p + turn) % 2 * 256 + xh * 32, 32), 32)
                sums[0, rows, :] = both[:, :128]
                sums[1, rows, :] = both[:, 128:]
        for f in range(2):
            rows = pl.ds(f * 512 + pair * 128, 128)
            copies.append(pltpu.make_async_copy(modulus.at[rows, :], modulus_far.at[rows, :], left.at[len(copies)]))
            copies[-1].start()
    one = jnp.zeros((256, 128), F32)
    for half in range(2):
        cells = sums[half, pl.ds(0, 256, stride=2), :] + sums[half, pl.ds(1, 256, stride=2), :]
        weights = mean1[half * 128 : half * 128 + 128, :]
        h, l = split(cells)
        one = one + (product(h, weights) + product(l, weights))
    for p in range(N_PY):
        route[p * ROUTE_ROWS : p * ROUTE_ROWS + 16, :] = one[p * 16 : p * 16 + 16]
    for k in range(8):
        sums2[k * 16 : k * 16 + 16, :] = one[k * 32 : k * 32 + 16] + one[k * 32 + 16 : k * 32 + 32]
    h, l = split(sums2[pl.ds(0, 64, stride=2), :] + sums2[pl.ds(1, 64, stride=2), :])
    two = product(h, mean2[...]) + product(l, mean2[...])
    sums2[0:64, :] = two
    for k in range(4):
        sums3[k * 8 : k * 8 + 8, :] = two[k * 16 : k * 16 + 8] + two[k * 16 + 8 : k * 16 + 16]
    h, l = split(sums3[pl.ds(0, 16, stride=2), :] + sums3[pl.ds(1, 16, stride=2), :])
    three = product(h, mean3[...]) + product(l, mean3[...])
    for i in range(4):
        row = sums2[pl.ds(i, N_PY, stride=4), :]
        route[pl.ds(16 + i, N_PY, stride=ROUTE_ROWS), :] = row if i else row + three
    for copy in copies:
        copy.wait()


def pick_kernel(table_row, got, out):
    table = table_row[...]
    low = lax.broadcasted_iota(jnp.int32, (4, 128), 1) < 64
    for g in range(N_PY):
        for k in range(4):
            out[g, k, :, :] = got[table[0, g], k, :, :]
        out[g, 4, :, :] = jnp.where(low, got[table[1, g], 4, :, :], got[table[2, g], 4, :, :])


def unpack_kernel(got, one_far, two_far, three_far, two, three, left):
    copies = [pltpu.make_async_copy(got.at[:, pl.ds(0, 4), :, :], one_far, left.at[0])]
    copies[0].start()
    for p in range(N_PY):
        last = got[p, 4, :, :]
        two[p * 4 : p * 4 + 4, :] = last[:, 0:64]
        three[p : p + 1, :] = last[0:1, 64:96]
    copies.append(pltpu.make_async_copy(two, two_far, left.at[1]))
    copies.append(pltpu.make_async_copy(three, three_far, left.at[2]))
    copies[1].start()
    copies[2].start()
    for copy in copies:
        copy.wait()


def on_chip(x):
    return pltpu.with_memory_space_constraint(x, pltpu.VMEM)


def off_chip(x):
    return pltpu.with_memory_space_constraint(x, pltpu.HBM)


def call(body, name, outs, *operands, scratch=(), **options):
    return pl.pallas_call(
        body,
        out_shape=outs,
        scratch_shapes=list(scratch),
        name=name,
        compiler_params=pltpu.CompilerParams(vmem_limit_bytes=VMEM_BYTES),
        **options,
    )(*operands)


def on_device(white_noise, spectrum, group_table):
    far = {k: tuple(jnp.asarray(t) for t in v) for k, v in make_tables().items()}
    tables = {k: tuple(on_chip(t) for t in v) for k, v in far.items()}
    noise = white_noise.reshape(1024, NZ)
    (sent,) = call(
        into_kernel,
        "into_z",
        [pltpu.VMEM((DEVICES * SEND_ROWS, 128), F32)],
        *(off_chip(a) for a in (noise, spectrum.reshape(512, NZ), *far["into"])),
        in_specs=[FAR] * 4,
        scratch=(
            pltpu.VMEM((1024, NZ), F32),
            pltpu.VMEM((2, 512, 128), F32),
            pltpu.VMEM((256, NZ), BF16),
            pltpu.VMEM((256, NZ), BF16),
            pltpu.SemaphoreType.DMA((8,)),
        ),
    )
    got = lax.all_to_all(sent.reshape(DEVICES, SEND_ROWS, 1, 128), ("px", "py"), 0, 0, tiled=True)
    (restored,) = call(
        middle_kernel,
        "planes",
        [pltpu.VMEM((DEVICES * BACK_ROWS, 128), F32)],
        on_chip(got.reshape(DEVICES * SEND_ROWS, 128)),
        *tables["along_y"],
        *tables["x_into"],
        *tables["x_back"],
        scratch=PLANE_SCRATCH,
    )
    back = lax.all_to_all(restored.reshape(DEVICES, BACK_ROWS, 128), ("px", "py"), 0, 0, tiled=True)
    modulus, route = call(
        last_kernel,
        "back_z",
        [jax.ShapeDtypeStruct((1024, NZ), F32), pltpu.VMEM((N_PY * ROUTE_ROWS, 128), F32)],
        on_chip(back.reshape(DEVICES * BACK_ROWS, 128)),
        *tables["into"],
        jnp.asarray(pair_mean(256)[:, :128]),
        jnp.asarray(pair_mean(128)),
        jnp.asarray(pair_mean(128, 64)),
        out_specs=[FAR, NEAR],
        scratch=(
            pltpu.VMEM((2, 512, 128), F32),
            pltpu.VMEM((128, 128), F32),
            pltpu.VMEM((32, 128), F32),
            pltpu.VMEM((1024, NZ), F32),
            pltpu.SemaphoreType.DMA((8,)),
        ),
    )
    spread = lax.all_to_all(route.reshape(ROUTE), "py", 0, 0, tiled=True)
    (picked,) = call(
        pick_kernel,
        "pick",
        [pltpu.VMEM(ROUTE, F32)],
        on_chip(group_table),
        on_chip(spread),
    )
    levels = lax.all_to_all(picked, "py", 0, 0, tiled=True)
    one, two, three = call(
        unpack_kernel,
        "unpack",
        [jax.ShapeDtypeStruct(s, F32) for s in ((16, 4, 4, 128), (64, 64), (16, 32))],
        on_chip(levels),
        out_specs=[FAR] * 3,
        scratch=(pltpu.VMEM((64, 64), F32), pltpu.VMEM((16, 32), F32), pltpu.SemaphoreType.DMA((3,))),
    )
    return (
        modulus.reshape(2, 16, 32, NZ),
        one.reshape(2, 8, 16, 128),
        two.reshape(2, 4, 8, 64),
        three.reshape(2, 2, 4, 32),
    )


def solution(mesh):
    block = P(None, "px", "py", None)
    return jax.shard_map(
        on_device,
        mesh=mesh,
        in_specs=(block, P("px", "py", None), P()),
        out_specs=(block, block, block, block),
        check_vma=False,
    )
```
